128 devices in a mesh: dp: 64 (over z, y, x), tp: 2 (over core).
Axes of the slice: x: 4, y: 4, z: 4, core: 2. Of those that a mesh axis runs over, the one named last changes fastest.
Arguments:
- hidden: bfloat16 [64, 1024, 576], P('dp')
- norm_w: bfloat16 [576], replicated
- embed_table: bfloat16 [49152, 576], P('tp')
- labels: int32 [64, 1024], P('dp')
- loss_mask: int32 [64, 1024], P('dp')
Outputs:
- output 1: float32 [], replicated
- output 2: bfloat16 [64, 1024, 576], P('dp')
- output 3: float32 [576], replicated
- output 4: float32 [49152, 576], P('tp')
All inputs are finite; a program needn't handle non-finite values.
Results may differ from the reference program's by a relative error of at most 0.001.
Values sent between devices are 32-bit elements.
A program may use at most 1 GiB of HBM per device.

```python
import math
import jax
import jax.numpy as jnp
from jax import lax

BATCH_ROWS = 64
SEQ_LEN = 1024
MODEL_DIM = 576
VOCAB_SIZE = 49152
TOKEN_BLOCK = 128
SOFT_CAP = 30.0


def draw_labels(root_key):
    key_pick, key_common, key_any = jax.random.split(root_key, 3)
    label_shape = (BATCH_ROWS, SEQ_LEN)
    pick_val = jax.random.randint(key_pick, label_shape, 0, 4)
    common_id = jax.random.randint(key_common, label_shape, 0, VOCAB_SIZE // 32)
    any_id = jax.random.randint(key_any, label_shape, 0, VOCAB_SIZE)
    return jnp.where(pick_val == 0, any_id, common_id).astype(jnp.int32)


def draw_mask(root_key):
    key_rate, key_roll = jax.random.split(root_key, 2)
    drop_pct = jax.random.randint(key_rate, (BATCH_ROWS, 1), 5, 40)
    roll_val = jax.random.randint(key_roll, (BATCH_ROWS, SEQ_LEN), 0, 100)
    return (roll_val >= drop_pct).astype(jnp.int32)


def norm_apply(hid_rows, gain32):
    h32 = hid_rows.astype(jnp.float32)
    inv_rms = lax.rsqrt(jnp.mean(h32 * h32, axis=-1, keepdims=True) + 1e-6)
    return h32 * inv_rms * (1.0 + gain32)


def setup_inputs(seed: int = 0) -> dict:
    root_key = jax.random.key(seed)
    key_noise, key_gain, key_table, key_str, key_lab, key_mask, key_top = jax.random.split(root_key, 7)
    table_scale = 3.0 / math.sqrt(MODEL_DIM)
    table32 = jax.random.normal(key_table, (VOCAB_SIZE, MODEL_DIM), jnp.float32) * table_scale
    labels = draw_labels(key_lab)
    top_str = jax.random.uniform(key_top, (), jnp.float32, minval=3.0, maxval=6.5)
    strength = jax.random.uniform(key_str, (BATCH_ROWS, SEQ_LEN, 1), jnp.float32) * top_str
    noise_val = jax.random.normal(key_noise, (BATCH_ROWS, SEQ_LEN, MODEL_DIM), jnp.float32)
    hidden = noise_val + strength * jnp.take(table32, labels, axis=0)
    gain_vec = 0.3 * jax.random.normal(key_gain, (MODEL_DIM,), jnp.float32)
    return {'hidden': hidden.astype(jnp.bfloat16), 'norm_w': gain_vec.astype(jnp.bfloat16), 'embed_table': table32.astype(jnp.bfloat16), 'labels': labels, 'loss_mask': draw_mask(key_mask)}


def reference(hidden, norm_w, embed_table, labels, loss_mask):
    tokens = BATCH_ROWS * SEQ_LEN
    n_blocks = tokens // TOKEN_BLOCK
    hid_blocks = hidden.reshape(n_blocks, TOKEN_BLOCK, MODEL_DIM)
    lab_blocks = labels.reshape(n_blocks, TOKEN_BLOCK)
    mask_blocks = loss_mask.reshape(n_blocks, TOKEN_BLOCK).astype(jnp.float32)
    tok_count = jnp.maximum(jnp.sum(mask_blocks), 1.0)
    gain32 = norm_w.astype(jnp.float32)
    vocab_ids = jnp.arange(VOCAB_SIZE, dtype=jnp.int32)

    def block_step(carry_in, block_in):
        loss_sum, grad_gain, grad_table = carry_in
        hid_rows, lab_rows, mask_rows = block_in
        normed, norm_back = jax.vjp(norm_apply, hid_rows, gain32)
        normed_bf = normed.astype(jnp.bfloat16)
        logits = jnp.dot(normed_bf, embed_table.T, preferred_element_type=jnp.float32)
        capped = SOFT_CAP * jnp.tanh(logits / SOFT_CAP)
        row_max = jnp.max(capped, axis=-1, keepdims=True)
        exp_shift = jnp.exp(capped - row_max)
        row_sum = jnp.sum(exp_shift, axis=-1, keepdims=True)
        onehot = vocab_ids[None, :] == lab_rows[:, None]
        picked = jnp.sum(jnp.where(onehot, capped, 0.0), axis=-1)
        tok_loss = jnp.log(row_sum[:, 0]) + row_max[:, 0] - picked
        tok_scale = mask_rows / tok_count
        cap_ratio = capped / SOFT_CAP
        grad_logit = ((exp_shift / row_sum - onehot.astype(jnp.float32)) * tok_scale[:, None] * (1.0 - cap_ratio * cap_ratio)).astype(jnp.bfloat16)
        grad_x = jnp.dot(grad_logit, embed_table, preferred_element_type=jnp.float32)
        grad_rows, grad_g = norm_back(grad_x)
        table_part = jnp.dot(grad_logit.T, normed_bf, preferred_element_type=jnp.float32)
        new_carry = (loss_sum + jnp.sum(mask_rows * tok_loss), grad_gain + grad_g, grad_table + table_part)
        return new_carry, grad_rows

    init_carry = (jnp.zeros((), jnp.float32), jnp.zeros((MODEL_DIM,), jnp.float32), jnp.zeros((VOCAB_SIZE, MODEL_DIM), jnp.float32))
    final_carry, grad_rows = lax.scan(block_step, init_carry, (hid_blocks, lab_blocks, mask_blocks))
    loss_sum, grad_gain, grad_table = final_carry
    return loss_sum / tok_count, grad_rows.reshape(BATCH_ROWS, SEQ_LEN, MODEL_DIM), grad_gain, grad_table
```

```python
import jax
import jax.numpy as jnp
import numpy as np
from jax import lax
from jax.experimental import pallas as pl
from jax.experimental.pallas import tpu as pltpu
from jax.sharding import Mesh, PartitionSpec as P

SOFT_CAP = 30.0
INV_CAP = 1.0 / SOFT_CAP
CAP_LOG2E = SOFT_CAP * 1.4426950408889634
LANES = 128
NCHUNK = 3
VMEM_LIMIT = 60 * 1024 * 1024
F32 = jnp.float32
BF16 = jnp.bfloat16
FAR = -(2 ** 24)


def norm_body(ht_ref, w1_ref, xt_ref, xb_ref):
    h = ht_ref[...].astype(F32)
    inv_rms = lax.rsqrt(jnp.mean(h * h, axis=0, keepdims=True) + 1e-6)
    xt = h * inv_rms * jnp.broadcast_to(w1_ref[:, :1], h.shape)
    xt_ref[...] = xt
    xb_ref[...] = xt.T.astype(BF16)


def norm_rows(ht, w1):
    dim, tokens = ht.shape
    tb = min(512, tokens)
    return pl.pallas_call(
        norm_body,
        grid=(tokens // tb,),
        in_specs=[
            pl.BlockSpec((dim, tb), lambda i: (0, i)),
            pl.BlockSpec((dim, LANES), lambda i: (0, 0)),
        ],
        out_specs=[
            pl.BlockSpec((dim, tb), lambda i: (0, i)),
            pl.BlockSpec((tb, dim), lambda i: (i, 0)),
        ],
        out_shape=[
            jax.ShapeDtypeStruct((dim, tokens), F32),
            jax.ShapeDtypeStruct((tokens, dim), BF16),
        ],
        compiler_params=pltpu.CompilerParams(
            dimension_semantics=("arbitrary",), vmem_limit_bytes=VMEM_LIMIT),
        cost_estimate=pl.CostEstimate(
            flops=10 * dim * tokens, bytes_accessed=8 * dim * tokens, transcendentals=0),
        name="norm",
    )(ht, w1)


def norm_back_body(ht_ref, w1_ref, g0_ref, g1_ref, dh_ref, dw_ref):
    h = ht_ref[...].astype(F32)
    inv_rms = lax.rsqrt(jnp.mean(h * h, axis=0, keepdims=True) + 1e-6)
    n = h * inv_rms
    g = g0_ref[...] + g1_ref[...]
    gn = g * n

    @pl.when(pl.program_id(0) == 0)
    def _():
        dw_ref[...] = jnp.zeros_like(dw_ref)

    part = dw_ref[...]
    for j in range(h.shape[1] // LANES):
        part = part + gn[:, j * LANES:(j + 1) * LANES]
    dw_ref[...] = part
    w1 = jnp.broadcast_to(w1_ref[:, :1], h.shape)
    inner = jnp.mean(gn * w1, axis=0, keepdims=True)
    dh_ref[...] = ((g * w1 - n * inner) * inv_rms).astype(BF16)


def norm_back(ht, w1, g0, g1):
    dim, tokens = ht.shape
    tb = min(512, tokens)
    return pl.pallas_call(
        norm_back_body,
        grid=(tokens // tb,),
        in_specs=[
            pl.BlockSpec((dim, tb), lambda i: (0, i)),
            pl.BlockSpec((dim, LANES), lambda i: (0, 0)),
            pl.BlockSpec((dim, tb), lambda i: (0, i)),
            pl.BlockSpec((dim, tb), lambda i: (0, i)),
        ],
        out_specs=[
            pl.BlockSpec((dim, tb), lambda i: (0, i)),
            pl.BlockSpec((dim, LANES), lambda i: (0, 0)),
        ],
        out_shape=[
            jax.ShapeDtypeStruct((dim, tokens), BF16),
            jax.ShapeDtypeStruct((dim, LANES), F32),
        ],
        compiler_params=pltpu.CompilerParams(
            dimension_semantics=("arbitrary",), vmem_limit_bytes=VMEM_LIMIT),
        cost_estimate=pl.CostEstimate(
            flops=20 * dim * tokens, bytes_accessed=12 * dim * tokens, transcendentals=0),
        name="norm_back",
    )(ht, w1, g0, g1)


def dot_f32(a, b, dims):
    return lax.dot_general(a, b, (dims, ((), ())), preferred_element_type=F32)


def fwd_body(tb, x_ref, lab_ref, e_ref, z_ref, p_ref):
    step = pl.program_id(0)
    tokens = x_ref.shape[0]
    bv = e_ref.shape[1]

    @pl.when(step == 0)
    def _():
        z_ref[...] = jnp.zeros_like(z_ref)
        p_ref[...] = jnp.zeros_like(p_ref)

    lane = lax.broadcasted_iota(jnp.int32, (tb, LANES), 1)

    def block(i, carry):
        rows = pl.ds(pl.multiple_of(i * tb, tb), tb)
        z = dot_f32(x_ref[rows, :], e_ref[...], ((1,), (0,)))
        lab = lab_ref[rows, :] - step * bv
        zsum = z_ref[rows, :]
        psum = p_ref[rows, :]
        for j in range(bv // LANES):
            t = jnp.tanh(z[:, j * LANES:(j + 1) * LANES] * INV_CAP)
            zsum = zsum + jnp.exp2(t * CAP_LOG2E)
            psum = jnp.where(lab == lane + j * LANES, t, psum)
        z_ref[rows, :] = zsum
        p_ref[rows, :] = psum
        return carry

    lax.fori_loop(0, tokens // tb, block, 0, unroll=True)


def forward(x, lab_rep, et, bv=512, tb=256):
    tokens, dim = x.shape
    vocab = et.shape[1]
    tb = min(tb, tokens)
    return pl.pallas_call(
        lambda *refs: fwd_body(tb, *refs),
        grid=(vocab // bv,),
        in_specs=[
            pl.BlockSpec((tokens, dim), lambda i: (0, 0)),
            pl.BlockSpec((tokens, LANES), lambda i: (0, 0)),
            pl.BlockSpec((dim, bv), lambda i: (0, i)),
        ],
        out_specs=[
            pl.BlockSpec((tokens, LANES), lambda i: (0, 0)),
            pl.BlockSpec((tokens, LANES), lambda i: (0, 0)),
        ],
        out_shape=[jax.ShapeDtypeStruct((tokens, LANES), F32)] * 2,
        compiler_params=pltpu.CompilerParams(
            dimension_semantics=("arbitrary",), vmem_limit_bytes=VMEM_LIMIT),
        cost_estimate=pl.CostEstimate(
            flops=2 * tokens * dim * vocab, bytes_accessed=2 * dim * vocab,
            transcendentals=2 * tokens * vocab),
        name="fwd",
    )(x, lab_rep, et)


def prep_body(xt_ref, xtb_ref, xb_ref):
    xt = xt_ref[0]
    xtb_ref[...] = xt.astype(BF16)
    xb_ref[...] = xt.T.astype(BF16)


def prep(xgt):
    group, dim, tokens = xgt.shape
    return pl.pallas_call(
        prep_body,
        grid=(group,),
        in_specs=[pl.BlockSpec((1, dim, tokens), lambda i: (i, 0, 0))],
        out_specs=[
            pl.BlockSpec((dim, tokens), lambda i: (0, i)),
            pl.BlockSpec((tokens, dim), lambda i: (i, 0)),
        ],
        out_shape=[
            jax.ShapeDtypeStruct((dim, group * tokens), BF16),
            jax.ShapeDtypeStruct((group * tokens, dim), BF16),
        ],
        compiler_params=pltpu.CompilerParams(
            dimension_semantics=("arbitrary",), vmem_limit_bytes=VMEM_LIMIT),
        cost_estimate=pl.CostEstimate(
            flops=10 * group * dim * tokens, bytes_accessed=8 * group * dim * tokens,
            transcendentals=0),
        name="prep",
    )(xgt)


def grad_tile(z, scale, lab, vid, inv_count):
    t = jnp.tanh(z * INV_CAP)
    p = jnp.exp2(t * CAP_LOG2E) * scale
    p = jnp.where(lab == vid, p - inv_count, p)
    return (p * (1.0 - t * t)).astype(BF16)


def table_body(chunk, stride, tb, idx_ref, cnt_ref, xb_ref, xtb_ref, scale_ref, lab_ref,
               e0_ref, e1_ref, out_ref, ga_ref, gb_ref, et_ref, acc_ref):
    step = pl.program_id(0)
    blocks = xb_ref.shape[0] // tb
    inv_count = cnt_ref[0]
    et_ref[:, :LANES] = e0_ref[...]
    et_ref[:, LANES:] = e1_ref[...]
    lane = lax.broadcasted_iota(jnp.int32, (tb, LANES), 1)
    base = chunk + step * 2 * stride

    def rows_of(i):
        return pl.ds(pl.multiple_of(i * tb, tb), tb)

    def grads(i, g_ref):
        rows = rows_of(i)
        z = dot_f32(xb_ref[rows, :], et_ref[...], ((1,), (0,)))
        lab = lab_ref[rows, :] - base
        scale = scale_ref[rows, :]
        for j in range(2):
            g_ref[:, j * LANES:(j + 1) * LANES] = grad_tile(
                z[:, j * LANES:(j + 1) * LANES], scale, lab, lane + j * stride, inv_count)

    def product(i, g_ref):
        return dot_f32(xtb_ref[:, rows_of(i)], g_ref[...], ((1,), (0,)))

    grads(0, ga_ref)
    grads(1, gb_ref)
    acc_ref[...] = product(0, ga_ref)

    def pair(k, carry):
        grads(2 * k, ga_ref)
        acc_ref[...] += product(2 * k - 1, gb_ref)
        grads(2 * k + 1, gb_ref)
        acc_ref[...] += product(2 * k, ga_ref)
        return carry

    lax.fori_loop(1, blocks // 2, pair, 0)
    last = product(blocks - 1, gb_ref)
    out_ref[0] = acc_ref[:, :LANES] + last[:, :LANES]
    out_ref[1] = acc_ref[:, LANES:] + last[:, LANES:]


def table_chunk(c, idx, inv_count, xb, xtb, scale_rep, lab_rep, et, n_dest, group, tb=512):
    tokens, dim = xb.shape
    tb = min(tb, tokens // 2)
    first = c * n_dest * group

    def whole(shape):
        return pl.BlockSpec(shape, lambda i, idx: (0, 0), pipeline_mode=pl.Buffered(1))

    def e_spec(k):
        return pl.BlockSpec((dim, LANES), lambda i, idx: (0, first + (2 * i + k) * group + idx[0]))

    return pl.pallas_call(
        lambda *refs: table_body(first * LANES, group * LANES, tb, *refs),
        grid_spec=pltpu.PrefetchScalarGridSpec(
            num_scalar_prefetch=1,
            grid=(n_dest // 2,),
            in_specs=[
                pl.BlockSpec(memory_space=pltpu.SMEM),
                whole((tokens, dim)),
                whole((dim, tokens)),
                whole((tokens, LANES)),
                whole((tokens, LANES)),
                e_spec(0),
                e_spec(1),
            ],
            out_specs=[pl.BlockSpec((2, dim, LANES), lambda i, idx: (i, 0, 0))],
            scratch_shapes=[
                pltpu.VMEM((tb, 2 * LANES), BF16),
                pltpu.VMEM((tb, 2 * LANES), BF16),
                pltpu.VMEM((dim, 2 * LANES), BF16),
                pltpu.VMEM((dim, 2 * LANES), F32),
            ],
        ),
        out_shape=[jax.ShapeDtypeStruct((n_dest, dim, LANES), F32)],
        compiler_params=pltpu.CompilerParams(
            dimension_semantics=("arbitrary",), vmem_limit_bytes=VMEM_LIMIT),
        cost_estimate=pl.CostEstimate(
            flops=4 * tokens * dim * n_dest * LANES,
            bytes_accessed=6 * dim * n_dest * LANES + 4 * tokens * dim,
            transcendentals=2 * tokens * n_dest * LANES),
        name="table_grad",
    )(idx, inv_count, xb, xtb, scale_rep, lab_rep, et, et)[0]


def rows_body(tb, cnt_ref, x_ref, scale_ref, lab_ref, e_ref, out_ref, g_ref):
    step = pl.program_id(0)
    tokens = x_ref.shape[0]
    bv = e_ref.shape[1]
    inv_count = cnt_ref[0]

    @pl.when(step == 0)
    def _():
        out_ref[...] = jnp.zeros_like(out_ref)

    lane = lax.broadcasted_iota(jnp.int32, (tb, LANES), 1)

    def block(i, carry):
        rows = pl.ds(pl.multiple_of(i * tb, tb), tb)
        z = dot_f32(x_ref[rows, :], e_ref[...], ((1,), (0,)))
        lab = lab_ref[rows, :] - step * bv
        scale = scale_ref[rows, :]
        for j in range(bv // LANES):
            g_ref[:, j * LANES:(j + 1) * LANES] = grad_tile(
                z[:, j * LANES:(j + 1) * LANES], scale, lab, lane + j * LANES, inv_count)
        out_ref[:, rows] += dot_f32(e_ref[...], g_ref[...], ((1,), (1,)))
        return carry

    lax.fori_loop(0, tokens // tb, block, 0)


def rows_grad(inv_count, x, scale_rep, lab_rep, et, bv=1024, tb=256):
    tokens, dim = x.shape
    vocab = et.shape[1]
    tb = min(tb, tokens)
    return pl.pallas_call(
        lambda *refs: rows_body(tb, *refs),
        grid=(vocab // bv,),
        in_specs=[
            pl.BlockSpec(memory_space=pltpu.SMEM),
            pl.BlockSpec((tokens, dim), lambda i: (0, 0)),
            pl.BlockSpec((tokens, LANES), lambda i: (0, 0)),
            pl.BlockSpec((tokens, LANES), lambda i: (0, 0)),
            pl.BlockSpec((dim, bv), lambda i: (0, i)),
        ],
        out_specs=[pl.BlockSpec((dim, tokens), lambda i: (0, 0))],
        out_shape=[jax.ShapeDtypeStruct((dim, tokens), F32)],
        scratch_shapes=[pltpu.VMEM((tb, bv), BF16)],
        compiler_params=pltpu.CompilerParams(
            dimension_semantics=("arbitrary",), vmem_limit_bytes=VMEM_LIMIT),
        cost_estimate=pl.CostEstimate(
            flops=4 * tokens * dim * vocab, bytes_accessed=2 * dim * vocab,
            transcendentals=2 * tokens * vocab),
        name="rows_grad",
    )(inv_count, x, scale_rep, lab_rep, et)[0]


def place_body(n, src_ref, *refs):
    out_ref = refs[-1]
    for k in range(n):
        out_ref[:, k * LANES:(k + 1) * LANES] = src_ref[k]


def place_chunk(c, gathered, table, vocab):
    n_dev, dim, _ = gathered.shape
    rows = 96 if dim % 96 == 0 else dim
    out_shape = jax.ShapeDtypeStruct((dim, vocab), F32)
    in_specs = [pl.BlockSpec((n_dev, rows, LANES), lambda i: (0, i, 0))]
    args = [gathered]
    alias = {}
    if table is not None:
        in_specs.append(pl.BlockSpec(memory_space=pl.ANY))
        args.append(table)
        alias = {1: 0}
    return pl.pallas_call(
        lambda *refs: place_body(n_dev, *refs),
        grid=(dim // rows,),
        in_specs=in_specs,
        out_specs=pl.BlockSpec((rows, n_dev * LANES), lambda i: (i, c)),
        out_shape=out_shape,
        input_output_aliases=alias,
        compiler_params=pltpu.CompilerParams(
            dimension_semantics=("arbitrary",), vmem_limit_bytes=VMEM_LIMIT),
        cost_estimate=pl.CostEstimate(
            flops=n_dev * dim * LANES, bytes_accessed=8 * n_dev * dim * LANES, transcendentals=0),
        name="place",
    )(*args)


def solution(mesh, dims=(4, 4, 4)):
    nz, ny, nx = dims
    grid_mesh = Mesh(mesh.devices.reshape(nz, ny, nx, 2), ('z', 'y', 'x', 'core'))
    every = ('z', 'y', 'x', 'core')

    def local_step(hidden, norm_w, embed_table, labels, loss_mask):
        batch_rows, seq_len, dim = hidden.shape
        vocab = embed_table.shape[0]
        tokens = batch_rows * seq_len
        n_dest = nz * ny
        et = embed_table.T
        ht = hidden.reshape(tokens, dim).T
        w1 = jnp.broadcast_to((1.0 + norm_w.astype(F32))[:, None], (dim, LANES))
        mask_rows = loss_mask.reshape(tokens).astype(F32)
        core = lax.axis_index('core')
        x_idx = lax.axis_index('x')

        count = jnp.maximum(lax.psum(jnp.sum(mask_rows), every) * 0.5, 1.0)
        xt_own, xb_own = norm_rows(ht, w1)
        xgt = lax.all_gather(xt_own, 'x', axis=0)

        lab_own = labels.reshape(tokens)
        lab_local = lab_own - core * vocab
        zpart, ppart = forward(
            xb_own, jnp.broadcast_to(lab_local[:, None], (tokens, LANES)), et)

        lab_masked = jnp.where(mask_rows > 0.0, lab_own, FAR).astype(F32)
        stats = lax.all_gather(
            jnp.stack([jnp.sum(zpart, axis=1), jnp.sum(ppart, axis=1), lab_masked]),
            ('x', 'core'), axis=0).reshape(nx, 2, 3, tokens)
        row_sum = stats[:, 0, 0] + stats[:, 1, 0]
        lab_group = stats[:, 0, 2].astype(jnp.int32)
        picked = lax.dynamic_index_in_dim(stats[:, 0, 1] + stats[:, 1, 1], x_idx, 0, False) * SOFT_CAP
        own_sum = lax.dynamic_index_in_dim(row_sum, x_idx, 0, False)
        tok_loss = jnp.log(own_sum) - picked
        loss_part = jnp.sum(mask_rows * tok_loss)

        inv_count = 1.0 / count
        scale_group = jnp.where(lab_group >= 0, inv_count, 0.0) / row_sum
        scale_own = (mask_rows * inv_count) / own_sum
        cnt = inv_count.reshape(1)
        group_tokens = nx * tokens
        scale_rep = jnp.broadcast_to(scale_group.reshape(group_tokens, 1), (group_tokens, LANES))
        lab_rep = jnp.broadcast_to(
            (lab_group - core * vocab - x_idx * LANES).reshape(group_tokens, 1), (group_tokens, LANES))

        xtb, xb = prep(xgt)
        idx = x_idx.astype(jnp.int32).reshape(1)
        table = None
        for c in range(NCHUNK):
            part = table_chunk(c, idx, cnt, xb, xtb, scale_rep, lab_rep, et, n_dest, nx)
            mine = lax.psum_scatter(part, ('z', 'y'), scatter_dimension=0, tiled=False)
            gathered = lax.all_gather(mine, ('z', 'y', 'x'), axis=0)
            table = place_chunk(c, gathered, table, vocab)

        xb_late, _ = lax.optimization_barrier((xb_own, part))
        lab_mine = jnp.where(mask_rows > 0.0, lab_local, FAR)
        gxt = rows_grad(
            cnt, xb_late, jnp.broadcast_to(scale_own[:, None], (tokens, LANES)),
            jnp.broadcast_to(lab_mine[:, None], (tokens, LANES)), et)
        dht, dw = norm_back(ht, w1, gxt, lax.ppermute(gxt, 'core', [(0, 1), (1, 0)]))
        grad_rows = dht.T
        loss_sum, grad_gain = lax.psum((loss_part, jnp.sum(dw, axis=1)), every)
        return (loss_sum * 0.5 / count, grad_rows.reshape(batch_rows, seq_len, dim),
                grad_gain * 0.5, table.T)

    dp = ('z', 'y', 'x')
    return jax.shard_map(
        local_step, mesh=grid_mesh,
        in_specs=(P(dp, None, None), P(None), P('core', None), P(dp, None), P(dp, None)),
        out_specs=(P(), P(dp, None, None), P(None), P('core', None)), check_vma=False)
```

```python
import jax
import jax.numpy as jnp
from jax import lax
from jax.experimental import pallas as pl
from jax.experimental.pallas import tpu as pltpu
from jax.sharding import Mesh, PartitionSpec as P

SOFT_CAP = 30.0
INV_CAP = 1.0 / SOFT_CAP
CAP_LOG2E = SOFT_CAP * 1.4426950408889634
LANES = 128
RING = 4
VMEM_LIMIT = 60 * 1024 * 1024
F32 = jnp.float32
BF16 = jnp.bfloat16
FAR = -(2 ** 22)
MESH_ID = pl.DeviceIdType.MESH
AXES = ('z', 'y', 'x', 'core')
SIZES = {'z': RING, 'y': RING, 'x': RING, 'core': 2}


def dot_f32(a, b, dims):
    return lax.dot_general(a, b, (dims, ((), ())), preferred_element_type=F32)


def grid_params(**kw):
    return pltpu.CompilerParams(
        dimension_semantics=("arbitrary",), vmem_limit_bytes=VMEM_LIMIT, **kw)


def peer(**shift):
    place = []
    for axis in AXES:
        here = lax.axis_index(axis)
        if axis in shift:
            here = lax.rem(here + shift[axis], SIZES[axis])
        place.append(here)
    return tuple(place)


def send(src, dst, send_sem, recv_sem, where):
    return pltpu.make_async_remote_copy(
        src, dst, send_sem, recv_sem, device_id=where, device_id_type=MESH_ID)


def meet(peers):
    barrier = pltpu.get_barrier_semaphore()
    for where in peers:
        pl.semaphore_signal(barrier, inc=1, device_id=where, device_id_type=MESH_ID)
    pl.semaphore_wait(barrier, len(peers))


def sum_slots(slot_ref, k, axis):
    total = slot_ref[k, 0]
    for i in range(1, SIZES[axis]):
        total = total + slot_ref[k, i]
    return total


def norm_body(ht_ref, w1_ref, xt_ref, xb_ref):
    h = ht_ref[...].astype(F32)
    inv_rms = lax.rsqrt(jnp.mean(h * h, axis=0, keepdims=True) + 1e-6)
    xt = h * inv_rms * jnp.broadcast_to(w1_ref[:, :1], h.shape)
    xt_ref[0] = xt
    xb_ref[...] = xt.T.astype(BF16)


def norm_rows(ht, w1):
    dim, tokens = ht.shape
    tb = tokens // 2
    return pl.pallas_call(
        norm_body,
        grid=(2,),
        in_specs=[
            pl.BlockSpec((dim, tb), lambda i: (0, i)),
            pl.BlockSpec((dim, LANES), lambda i: (0, 0)),
        ],
        out_specs=[
            pl.BlockSpec((1, dim, tb), lambda i: (i, 0, 0)),
            pl.BlockSpec((tb, dim), lambda i: (i, 0)),
        ],
        out_shape=[
            jax.ShapeDtypeStruct((2, dim, tb), F32),
            jax.ShapeDtypeStruct((tokens, dim), BF16),
        ],
        compiler_params=grid_params(),
        cost_estimate=pl.CostEstimate(
            flops=10 * dim * tokens, bytes_accessed=8 * dim * tokens, transcendentals=0),
        name="norm",
    )(ht, w1)


def norm_back_body(ht_ref, w1_ref, g0_ref, g1_ref, loss_ref, dh_ref, sum_ref,
                   dw_ref, cur_ref, slot_ref, send_sem, recv_sem):
    step = pl.program_id(0)
    dim, tb = ht_ref.shape
    h = ht_ref[...].astype(F32)
    inv_rms = lax.rsqrt(jnp.mean(h * h, axis=0, keepdims=True) + 1e-6)
    n = h * inv_rms
    g = g0_ref[...] + g1_ref[...]
    gn = g * n

    @pl.when(step == 0)
    def _():
        dw_ref[...] = jnp.zeros_like(dw_ref)

    part = dw_ref[...]
    for j in range(tb // LANES):
        part = part + gn[:, j * LANES:(j + 1) * LANES]
    dw_ref[...] = part
    w1 = jnp.broadcast_to(w1_ref[:, :1], h.shape)
    inner = jnp.mean(gn * w1, axis=0, keepdims=True)
    dh_ref[...] = ((g * w1 - n * inner) * inv_rms).astype(BF16)

    @pl.when(step == pl.num_programs(0) - 1)
    def _():
        cur_ref[0] = jnp.zeros_like(cur_ref[0])
        cur_ref[0, 0:1, 0:dim] = jnp.sum(dw_ref[...].T, axis=0, keepdims=True)
        cur_ref[0, 1:2, 0:LANES] = loss_ref[0:1, :]
        meet([peer(**{axis: r}) for axis in ('x', 'y', 'z') for r in range(1, SIZES[axis])])
        for k, axis in enumerate(('x', 'y', 'z')):
            me = lax.axis_index(axis)
            copies = []
            for r in range(1, SIZES[axis]):
                copies.append(send(cur_ref.at[k], slot_ref.at[k, me], send_sem.at[k, r - 1],
                                   recv_sem.at[k, r - 1], peer(**{axis: r})))
                copies[-1].start()
            slot_ref[k, me] = cur_ref[k]
            for copy in copies:
                copy.wait()
            cur_ref[k + 1] = sum_slots(slot_ref, k, axis)
        sum_ref[...] = cur_ref[3]


def norm_back(ht, w1, g0, g1, loss_tile):
    dim, tokens = ht.shape
    tb = tokens // 2
    width = -(-dim // LANES) * LANES
    return pl.pallas_call(
        norm_back_body,
        grid=(2,),
        in_specs=[
            pl.BlockSpec((dim, tb), lambda i: (0, i)),
            pl.BlockSpec((dim, LANES), lambda i: (0, 0)),
            pl.BlockSpec((dim, tb), lambda i: (0, i)),
            pl.BlockSpec((dim, tb), lambda i: (0, i)),
            pl.BlockSpec((8, LANES), lambda i: (0, 0)),
        ],
        out_specs=[
            pl.BlockSpec((dim, tb), lambda i: (0, i)),
            pl.BlockSpec((8, width), lambda i: (0, 0)),
        ],
        out_shape=[
            jax.ShapeDtypeStruct((dim, tokens), BF16),
            jax.ShapeDtypeStruct((8, width), F32),
        ],
        scratch_shapes=[
            pltpu.VMEM((dim, LANES), F32),
            pltpu.VMEM((4, 8, width), F32),
            pltpu.VMEM((3, RING, 8, width), F32),
            pltpu.SemaphoreType.DMA((3, 3)),
            pltpu.SemaphoreType.DMA((3, 3)),
        ],
        compiler_params=grid_params(collective_id=3, has_side_effects=True),
        cost_estimate=pl.CostEstimate(
            flops=20 * dim * tokens, bytes_accessed=12 * dim * tokens, transcendentals=0),
        name="norm_back",
    )(ht, w1, g0, g1, loss_tile)


def fwd_body(tb, early, late, x_ref, lab_ref, mask_ref, row_ref, e_ref, xt_ref,
             xg_ref, stat_ref, count_ref,
             z_ref, p_ref, pay_ref, cnt_ref, slot_ref,
             ring_send, ring_recv, half_send, half_recv, die_send, die_recv,
             cnt_send, cnt_recv, stat_send, stat_recv, own_sem):
    step = pl.program_id(0)
    last = pl.num_programs(0) - 1
    tokens = x_ref.shape[0]
    bv = e_ref.shape[1]
    dim = e_ref.shape[0]
    cut = dim // 16 * 8
    core = lax.axis_index('core')
    right, left, across = peer(x=1), peer(x=RING - 1), peer(core=1)

    to_right = send(xt_ref.at[core], xg_ref.at[0, core], ring_send.at[0], ring_recv.at[0], right)
    to_left = send(xt_ref.at[core], xg_ref.at[2, core], ring_send.at[1], ring_recv.at[1], left)
    on_right = send(xg_ref.at[0, core, pl.ds(0, cut)], xg_ref.at[1, core, pl.ds(0, cut)],
                    half_send.at[0], half_recv.at[0], right)
    on_left = send(xg_ref.at[2, core, pl.ds(cut, dim - cut)],
                   xg_ref.at[1, core, pl.ds(cut, dim - cut)],
                   half_send.at[1], half_recv.at[1], left)
    over = [send(xg_ref.at[r, core], xg_ref.at[r, core], die_send.at[r], die_recv.at[r], across)
            for r in range(3)]

    def count_copies(k, axis):
        me = lax.axis_index(axis)
        return [send(cnt_ref.at[k], slot_ref.at[k, me], cnt_send.at[k, r - 1],
                     cnt_recv.at[k, r - 1], peer(**{axis: r})) for r in range(1, SIZES[axis])]

    def count_sum(k, axis):
        for copy in count_copies(k, axis):
            copy.wait()
        slot_ref[k, lax.axis_index(axis)] = cnt_ref[k]
        cnt_ref[k + 1] = sum_slots(slot_ref, k, axis)

    @pl.when(step == 0)
    def _():
        z_ref[...] = jnp.zeros_like(z_ref)
        p_ref[...] = jnp.zeros_like(p_ref)
        cnt_ref[0] = jnp.full(cnt_ref.shape[1:], jnp.sum(mask_ref[...]), F32)
        meet([peer(**{axis: r}) for axis in ('y', 'z') for r in range(1, SIZES[axis])]
             + [peer(x=r, core=c) for r in (1, 2, 3) for c in (0, 1)] + [across])
        to_right.start()
        to_left.start()
        for copy in count_copies(0, 'x'):
            copy.start()

    @pl.when(step == 4)
    def _():
        count_sum(0, 'x')
        for copy in count_copies(1, 'y'):
            copy.start()

    @pl.when(step == 8)
    def _():
        count_sum(1, 'y')
        for copy in count_copies(2, 'z'):
            copy.start()

    @pl.when(step == 12)
    def _():
        count_sum(2, 'z')
        count_ref[...] = cnt_ref[3]

    @pl.when(step == early)
    def _():
        to_right.wait()
        to_left.wait()
        on_right.start()
        on_left.start()
        over[0].start()
        over[2].start()

    @pl.when(step == late)
    def _():
        on_right.wait()
        on_left.wait()
        over[1].start()

    lane = lax.broadcasted_iota(jnp.int32, (tb, LANES), 1)

    def block(i, carry):
        rows = pl.ds(pl.multiple_of(i * tb, tb), tb)
        z = dot_f32(x_ref[rows, :], e_ref[...], ((1,), (0,)))
        lab = lab_ref[rows, :] - step * bv
        zsum = z_ref[rows, :]
        psum = p_ref[rows, :]
        for j in range(bv // LANES):
            t = jnp.tanh(z[:, j * LANES:(j + 1) * LANES] * INV_CAP)
            zsum = zsum + jnp.exp2(t * CAP_LOG2E)
            psum = jnp.where(lab == lane + j * LANES, t, psum)
        z_ref[rows, :] = zsum
        p_ref[rows, :] = psum
        return carry

    lax.fori_loop(0, tokens // tb, block, 0, unroll=True)

    @pl.when(step == last)
    def _():
        pay_ref[0:1, :] = jnp.sum(z_ref[...].T, axis=0, keepdims=True)
        pay_ref[1:2, :] = jnp.sum(p_ref[...].T, axis=0, keepdims=True)
        pay_ref[2:3, :] = row_ref[...]
        pay_ref[3:8, :] = jnp.zeros((5, tokens), F32)
        own = pltpu.make_async_copy(pay_ref, stat_ref.at[0, core], own_sem)
        own.start()
        copies = [send(pay_ref, stat_ref.at[0, core], stat_send.at[0], stat_recv.at[0], across)]
        for r in (1, 2, 3):
            for c in (0, 1):
                k = 2 * r - 1 + c
                copies.append(send(pay_ref, stat_ref.at[r, core], stat_send.at[k],
                                   stat_recv.at[k], peer(x=r, core=c)))
        for copy in copies:
            copy.start()
        for copy in over:
            copy.wait()
        own.wait()
        for copy in copies:
            copy.wait()


def forward(x, lab_rep, mask_tile, lab_row, et, xt, bv=512, tb=256):
    tokens, dim = x.shape
    vocab = et.shape[1]
    tb = min(tb, tokens)
    steps = vocab // bv
    early, late = max(13, steps * 25 // 48), max(14, steps * 38 // 48)
    anyspace = pl.BlockSpec(memory_space=pl.ANY)
    sem = pltpu.SemaphoreType.DMA
    return pl.pallas_call(
        lambda *refs: fwd_body(tb, early, late, *refs),
        grid=(steps,),
        in_specs=[
            pl.BlockSpec((tokens, dim), lambda i: (0, 0)),
            pl.BlockSpec((tokens, LANES), lambda i: (0, 0)),
            pl.BlockSpec((8, tokens // 8), lambda i: (0, 0)),
            pl.BlockSpec((1, tokens), lambda i: (0, 0)),
            pl.BlockSpec((dim, bv), lambda i: (0, i)),
            anyspace,
        ],
        out_specs=[anyspace, anyspace, pl.BlockSpec((8, LANES), lambda i: (0, 0))],
        out_shape=[
            jax.ShapeDtypeStruct((RING - 1, 2, dim, tokens // 2), F32),
            jax.ShapeDtypeStruct((RING, 2, 8, tokens), F32),
            jax.ShapeDtypeStruct((8, LANES), F32),
        ],
        scratch_shapes=[
            pltpu.VMEM((tokens, LANES), F32),
            pltpu.VMEM((tokens, LANES), F32),
            pltpu.VMEM((8, tokens), F32),
            pltpu.VMEM((4, 8, LANES), F32),
            pltpu.VMEM((3, RING, 8, LANES), F32),
            sem((2,)), sem((2,)), sem((2,)), sem((2,)), sem((3,)), sem((3,)),
            sem((3, 3)), sem((3, 3)), sem((7,)), sem((7,)), sem,
        ],
        compiler_params=grid_params(collective_id=1, has_side_effects=True),
        cost_estimate=pl.CostEstimate(
            flops=2 * tokens * dim * vocab, bytes_accessed=2 * dim * vocab,
            transcendentals=2 * tokens * vocab),
        name="fwd",
    )(x, lab_rep, mask_tile, lab_row, et, xt)


def prep_body(cnt_ref, own_ref, xg_ref, stat_ref, xb_ref, xt_ref, scale_ref, lab_ref, loss_ref):
    r = pl.program_id(0)
    _, dim, half = own_ref.shape
    inv_count = cnt_ref[0]
    tail = dim % LANES

    def store(x_ref):
        for side in range(2):
            v = (own_ref[side] if x_ref is own_ref else x_ref[0, side])
            vt = v.T.astype(BF16)
            vb = v.astype(BF16)
            rows = pl.ds(side * half, half)
            for k in range(dim // LANES):
                xb_ref[k, rows, :] = vt[:, k * LANES:(k + 1) * LANES]
            if tail:
                xb_ref[dim // LANES, rows, :] = jnp.concatenate(
                    [vt[:, dim - tail:], jnp.zeros((half, LANES - tail), BF16)], axis=1)
            for k in range(half // LANES):
                xt_ref[side * (half // LANES) + k] = vb[:, k * LANES:(k + 1) * LANES]

    @pl.when(r == 0)
    def _():
        store(own_ref)

    @pl.when(r != 0)
    def _():
        store(xg_ref)

    row_sum = stat_ref[0, 0, 0:1, :] + stat_ref[0, 1, 0:1, :]
    label = stat_ref[0, 0, 2:3, :]
    live = label >= 0.0
    scale = jnp.where(live, inv_count, 0.0) / row_sum
    for k in range(2 * half // LANES):
        cols = slice(k * LANES, (k + 1) * LANES)
        scale_ref[cols, :] = jnp.broadcast_to(scale[:, cols], (LANES, LANES)).T
        lab_ref[cols, :] = jnp.broadcast_to(label[:, cols], (LANES, LANES)).T.astype(jnp.int32)

    @pl.when(r == 0)
    def _():
        picked = (stat_ref[0, 0, 1:2, :] + stat_ref[0, 1, 1:2, :]) * SOFT_CAP
        loss = jnp.where(live, jnp.log(row_sum) - picked, 0.0)
        loss_ref[...] = jnp.full((8, LANES), jnp.sum(loss), F32)


def prep(inv_count, xt_own, xg, stat):
    _, dim, half = xt_own.shape
    tokens = 2 * half
    slabs = -(-dim // LANES)
    per = tokens // LANES
    return pl.pallas_call(
        prep_body,
        grid=(RING,),
        in_specs=[
            pl.BlockSpec(memory_space=pltpu.SMEM),
            pl.BlockSpec((2, dim, half), lambda i: (0, 0, 0)),
            pl.BlockSpec((1, 2, dim, half), lambda i: (jnp.maximum(i - 1, 0), 0, 0, 0)),
            pl.BlockSpec((1, 2, 8, tokens), lambda i: (i, 0, 0, 0)),
        ],
        out_specs=[
            pl.BlockSpec((slabs, tokens, LANES), lambda i: (0, i, 0)),
            pl.BlockSpec((per, dim, LANES), lambda i: (i, 0, 0)),
            pl.BlockSpec((tokens, LANES), lambda i: (i, 0)),
            pl.BlockSpec((tokens, LANES), lambda i: (i, 0)),
            pl.BlockSpec((8, LANES), lambda i: (0, 0)),
        ],
        out_shape=[
            jax.ShapeDtypeStruct((slabs, RING * tokens, LANES), BF16),
            jax.ShapeDtypeStruct((RING * per, dim, LANES), BF16),
            jax.ShapeDtypeStruct((RING * tokens, LANES), F32),
            jax.ShapeDtypeStruct((RING * tokens, LANES), jnp.int32),
            jax.ShapeDtypeStruct((8, LANES), F32),
        ],
        compiler_params=grid_params(),
        cost_estimate=pl.CostEstimate(
            flops=40 * dim * tokens, bytes_accessed=32 * dim * tokens, transcendentals=0),
        name="prep",
    )(inv_count, xt_own, xg, stat)


def grad_tile(z, scale, lab, vid, inv_count):
    t = jnp.tanh(z * INV_CAP)
    p = jnp.exp2(t * CAP_LOG2E) * scale
    p = jnp.where(lab == vid, p - inv_count, p)
    return (p * (1.0 - t * t)).astype(BF16)


def table_body(first, n_chunks, tb, cnt_ref, off_ref, xb_ref, xt_ref, scale_ref, lab_ref, et_ref,
               out_ref, ebuf, ga_ref, gb_ref, tiles, part_in, tile_in, bpart_in, btile_in,
               esem, psend, precv, tsend, trecv, bpsend, bprecv, btsend, btrecv):
    slabs, group_tokens, _ = xb_ref.shape
    dim = xt_ref.shape[1]
    blocks = group_tokens // tb
    cut = dim // 16 * 8
    rest = dim - cut
    units = 8 * n_chunks
    inv_count = cnt_ref[0]
    vocab_off = off_ref[0]
    zi, yi, xi = (lax.axis_index(a) for a in ('z', 'y', 'x'))
    lane = lax.broadcasted_iota(jnp.int32, (tb, LANES), 1)

    def shifted(odd, da, db):
        return peer(z=db + odd * (da - db), y=da + odd * (db - da))

    def tile_index(u, j):
        k = u // 8
        odd = lax.rem(first + k, 2)
        s = lax.rem(u, 8) // 2
        half = lax.rem(u, 2)
        rb = lax.rem(2 + 3 * s + 3 * (s * (s - 1) // 2), 4)
        ra = 2 + half - j * (1 + 2 * half)
        dz, dy = rb + odd * (ra - rb), ra + odd * (rb - ra)
        return (((first + k) * 4 + lax.rem(zi + dz, 4)) * 4 + lax.rem(yi + dy, 4)) * 4 + xi

    def fetch(u, j):
        cols = pl.ds(pl.multiple_of(tile_index(u, j) * LANES, LANES), LANES)
        slot = lax.rem(u, 2)
        return pltpu.make_async_copy(
            et_ref.at[:, cols], ebuf.at[slot, j, pl.ds(0, dim)], esem.at[slot, j])

    def part_copies(q):
        odd = lax.rem(first + q // 4, 2)
        return (send(tiles.at[q, 0, pl.ds(0, cut)], part_in.at[q, 0, pl.ds(0, cut)],
                     psend.at[q, 0], precv.at[q, 0], shifted(odd, 1, 0)),
                send(tiles.at[q, 0, pl.ds(cut, rest)], part_in.at[q, 1, pl.ds(0, rest)],
                     psend.at[q, 1], precv.at[q, 1], shifted(odd, 3, 0)))

    def tile_copies(q):
        odd = lax.rem(first + q // 4, 2)
        return (send(tiles.at[q, 1], tile_in.at[q, 0], tsend.at[q, 0], trecv.at[q, 0],
                     shifted(odd, 1, 0)),
                send(tiles.at[q, 2], tile_in.at[q, 1], tsend.at[q, 1], trecv.at[q, 1],
                     shifted(odd, 3, 0)))

    def bpart_copies(k):
        odd = lax.rem(first + k, 2)
        return (send(tiles.at[4 * k, 3, pl.ds(0, cut)], bpart_in.at[k, 0, pl.ds(0, cut)],
                     bpsend.at[k, 0], bprecv.at[k, 0], shifted(odd, 0, 1)),
                send(tiles.at[4 * k, 3, pl.ds(cut, rest)], bpart_in.at[k, 1, pl.ds(0, rest)],
                     bpsend.at[k, 1], bprecv.at[k, 1], shifted(odd, 0, 3)))

    def btile_copies(k):
        odd = lax.rem(first + k, 2)
        return (send(tiles.at[4 * k + 1, 3], btile_in.at[k, 0], btsend.at[k, 0], btrecv.at[k, 0],
                     shifted(odd, 0, 1)),
                send(tiles.at[4 * k + 2, 3], btile_in.at[k, 1], btsend.at[k, 1], btrecv.at[k, 1],
                     shifted(odd, 0, 3)))

    def start(copies):
        for copy in copies:
            copy.start()

    def arrive(copies):
        for copy in copies:
            copy.wait_recv()

    def close_slab(q):
        arrive(tile_copies(q))
        tiles[q, 3] = tiles[q, 3] + (tile_in[q, 0] + tile_in[q, 1])

    def close_chunk(k):
        close_slab(4 * k + 3)
        arrive(btile_copies(k))
        out_ref[k] = tiles[4 * k + 3, 3] + (btile_in[k, 0] + btile_in[k, 1])

    if slabs * LANES > dim:
        for slot in range(2):
            for j in range(2):
                ebuf[slot, j, dim:, :] = jnp.zeros((slabs * LANES - dim, LANES), BF16)
    for j in range(2):
        fetch(0, j).start()
    meet([peer(y=1), peer(y=3), peer(z=1), peer(z=3)])

    def unit(u, carry):
        slot = lax.rem(u, 2)
        q = u // 2
        k = u // 8
        s = lax.rem(q, 4)
        half = lax.rem(u, 2)
        for j in range(2):
            fetch(u, j).wait()

        @pl.when(u + 1 < units)
        def _():
            for j in range(2):
                fetch(u + 1, j).start()

        bases = [tile_index(u, j) * LANES + vocab_off for j in range(2)]

        def rows_of(i):
            return pl.ds(pl.multiple_of(i * tb, tb), tb)

        def grads(i, g_ref):
            rows = rows_of(i)
            x = jnp.concatenate([xb_ref[n, rows, :] for n in range(slabs)], axis=1)
            e = jnp.concatenate([ebuf[slot, 0], ebuf[slot, 1]], axis=1)
            z = dot_f32(x, e, ((1,), (0,)))
            lab = lab_ref[rows, :]
            scale = scale_ref[rows, :]
            for j in range(2):
                g_ref[j] = grad_tile(z[:, j * LANES:(j + 1) * LANES], scale, lab - bases[j], lane,
                                     inv_count)

        def product(i, g_ref):
            n = tb // LANES
            x = jnp.concatenate([xt_ref[i * n + m] for m in range(n)], axis=1)
            g = jnp.concatenate([g_ref[0], g_ref[1]], axis=1)
            return dot_f32(x, g, ((1,), (0,)))

        def add(i, g_ref):
            part = product(i, g_ref)
            for j in range(2):
                tiles[q, 2 * half + j] += part[:, j * LANES:(j + 1) * LANES]

        grads(0, ga_ref)
        grads(1, gb_ref)
        part = product(0, ga_ref)
        for j in range(2):
            tiles[q, 2 * half + j] = part[:, j * LANES:(j + 1) * LANES]

        def pair(i, c):
            grads(2 * i, ga_ref)
            add(2 * i - 1, gb_ref)
            grads(2 * i + 1, gb_ref)
            add(2 * i, ga_ref)
            return c

        lax.fori_loop(1, blocks // 2, pair, 0)
        add(blocks - 1, gb_ref)

        @pl.when(half == 0)
        def _():
            @pl.when((s == 1) & (k > 0))
            def _():
                close_chunk(k - 1)

            start(part_copies(q))

        @pl.when(half == 1)
        def _():
            arrive(part_copies(q))
            tiles[q, 1, 0:cut, :] += part_in[q, 0, 0:cut, :]
            tiles[q, 2, cut:dim, :] += part_in[q, 1, 0:rest, :]

            @pl.when(s >= 1)
            def _():
                close_slab(q - 1)

            start(tile_copies(q))

            @pl.when(s == 1)
            def _():
                start(bpart_copies(k))

            @pl.when(s == 3)
            def _():
                arrive(bpart_copies(k))
                tiles[4 * k + 1, 3, 0:cut, :] += bpart_in[k, 0, 0:cut, :]
                tiles[4 * k + 2, 3, cut:dim, :] += bpart_in[k, 1, 0:rest, :]
                start(btile_copies(k))
        return carry

    lax.fori_loop(0, units, unit, 0)
    close_chunk(n_chunks - 1)

    def sent(q, carry):
        for copy in part_copies(q) + tile_copies(q):
            copy.wait_send()
        return carry

    lax.fori_loop(0, 4 * n_chunks, sent, 0)
    for k in range(n_chunks):
        for copy in bpart_copies(k) + btile_copies(k):
            copy.wait_send()


def table_chunks(first, n_chunks, inv_count, vocab_off, xb, xt, scale, lab, et, ident, tb=512):
    slabs, group_tokens, _ = xb.shape
    dim = xt.shape[1]
    tb = min(tb, group_tokens // 4)
    part = max(dim // 16 * 8, dim - dim // 16 * 8)
    smem = pl.BlockSpec(memory_space=pltpu.SMEM)
    vmem = pl.BlockSpec(memory_space=pltpu.VMEM)
    n_slabs = 4 * n_chunks
    sem = pltpu.SemaphoreType.DMA
    tokens = n_chunks * 16 * LANES * group_tokens
    return pl.pallas_call(
        lambda *refs: table_body(first, n_chunks, tb, *refs),
        in_specs=[smem, smem, vmem, vmem, vmem, vmem, pl.BlockSpec(memory_space=pl.ANY)],
        out_specs=vmem,
        out_shape=jax.ShapeDtypeStruct((n_chunks, dim, LANES), F32),
        scratch_shapes=[
            pltpu.VMEM((2, 2, slabs * LANES, LANES), BF16),
            pltpu.VMEM((2, tb, LANES), BF16),
            pltpu.VMEM((2, tb, LANES), BF16),
            pltpu.VMEM((n_slabs, 4, dim, LANES), F32),
            pltpu.VMEM((n_slabs, 2, part, LANES), F32),
            pltpu.VMEM((n_slabs, 2, dim, LANES), F32),
            pltpu.VMEM((n_chunks, 2, part, LANES), F32),
            pltpu.VMEM((n_chunks, 2, dim, LANES), F32),
            sem((2, 2)), sem((n_slabs, 2)), sem((n_slabs, 2)), sem((n_slabs, 2)),
            sem((n_slabs, 2)), sem((n_chunks, 2)), sem((n_chunks, 2)), sem((n_chunks, 2)),
            sem((n_chunks, 2)),
        ],
        compiler_params=pltpu.CompilerParams(
            collective_id=ident, has_side_effects=True, vmem_limit_bytes=VMEM_LIMIT),
        cost_estimate=pl.CostEstimate(
            flops=4 * dim * tokens, bytes_accessed=4 * dim * group_tokens,
            transcendentals=2 * tokens),
        name="table_grad",
    )(inv_count, vocab_off, xb, xt, scale, lab, et)


def rows_body(tb, cnt_ref, off_ref, x_ref, scale_ref, lab_ref, e_ref, out_ref, g_ref):
    step = pl.program_id(0)
    tokens = x_ref.shape[0]
    bv = e_ref.shape[1]
    inv_count = cnt_ref[0]
    base = step * bv + off_ref[0]

    @pl.when(step == 0)
    def _():
        out_ref[...] = jnp.zeros_like(out_ref)

    lane = lax.broadcasted_iota(jnp.int32, (tb, LANES), 1)

    def block(i, carry):
        rows = pl.ds(pl.multiple_of(i * tb, tb), tb)
        z = dot_f32(x_ref[rows, :], e_ref[...], ((1,), (0,)))
        lab = lab_ref[rows, :] - base
        scale = scale_ref[rows, :]
        for j in range(bv // LANES):
            g_ref[:, j * LANES:(j + 1) * LANES] = grad_tile(
                z[:, j * LANES:(j + 1) * LANES], scale, lab, lane + j * LANES, inv_count)
        out_ref[:, rows] += dot_f32(e_ref[...], g_ref[...], ((1,), (1,)))
        return carry

    lax.fori_loop(0, tokens // tb, block, 0)


def rows_grad(inv_count, vocab_off, x, scale, lab, et, bv=1024, tb=256):
    tokens, dim = x.shape
    vocab = et.shape[1]
    tb = min(tb, tokens)
    smem = pl.BlockSpec(memory_space=pltpu.SMEM)
    return pl.pallas_call(
        lambda *refs: rows_body(tb, *refs),
        grid=(vocab // bv,),
        in_specs=[
            smem,
            smem,
            pl.BlockSpec((tokens, dim), lambda i: (0, 0)),
            pl.BlockSpec((tokens, LANES), lambda i: (0, 0)),
            pl.BlockSpec((tokens, LANES), lambda i: (0, 0)),
            pl.BlockSpec((dim, bv), lambda i: (0, i)),
        ],
        out_specs=pl.BlockSpec((dim, tokens), lambda i: (0, 0)),
        out_shape=jax.ShapeDtypeStruct((dim, tokens), F32),
        scratch_shapes=[pltpu.VMEM((tb, bv), BF16)],
        compiler_params=grid_params(),
        cost_estimate=pl.CostEstimate(
            flops=4 * tokens * dim * vocab, bytes_accessed=2 * dim * vocab,
            transcendentals=2 * tokens * vocab),
        name="rows_grad",
    )(inv_count, vocab_off, x, scale, lab, et)


def place_body(n, src_ref, *refs):
    out_ref = refs[-1]
    for k in range(n):
        out_ref[:, k * LANES:(k + 1) * LANES] = src_ref[k]


def place_chunk(c, gathered, table, vocab):
    n_dev, dim, _ = gathered.shape
    rows = 96 if dim % 96 == 0 else dim
    in_specs = [pl.BlockSpec((n_dev, rows, LANES), lambda i: (0, i, 0))]
    args = [gathered]
    alias = {}
    if table is not None:
        in_specs.append(pl.BlockSpec(memory_space=pl.ANY))
        args.append(table)
        alias = {1: 0}
    return pl.pallas_call(
        lambda *refs: place_body(n_dev, *refs),
        grid=(dim // rows,),
        in_specs=in_specs,
        out_specs=pl.BlockSpec((rows, n_dev * LANES), lambda i: (i, c)),
        out_shape=jax.ShapeDtypeStruct((dim, vocab), F32),
        input_output_aliases=alias,
        compiler_params=grid_params(),
        cost_estimate=pl.CostEstimate(
            flops=n_dev * dim * LANES, bytes_accessed=8 * n_dev * dim * LANES, transcendentals=0),
        name="place",
    )(*args)


def solution(mesh):
    grid_mesh = Mesh(mesh.devices.reshape(RING, RING, RING, 2), AXES)
    dp = ('z', 'y', 'x')

    def local_step(hidden, norm_w, embed_table, labels, loss_mask):
        batch_rows, seq_len, dim = hidden.shape
        vocab = embed_table.shape[0]
        tokens = batch_rows * seq_len
        et = embed_table.T
        ht = hidden.reshape(tokens, dim).T
        w1 = jnp.broadcast_to((1.0 + norm_w.astype(F32))[:, None], (dim, LANES))
        mask_row = loss_mask.reshape(1, tokens)
        lab_row = labels.reshape(1, tokens)
        core = lax.axis_index('core')

        xt_own, xb_own = norm_rows(ht, w1)
        lab_rep = jnp.broadcast_to((lab_row.reshape(tokens) - core * vocab)[:, None], (tokens, LANES))
        lab_live = jnp.where(mask_row > 0, lab_row, FAR).astype(F32)
        xg, stat, count = forward(
            xb_own, lab_rep, mask_row.reshape(8, tokens // 8).astype(F32), lab_live, et, xt_own)
        inv_count = (1.0 / jnp.maximum(count[0, 0], 1.0)).reshape(1)
        vocab_off = (core * vocab).astype(jnp.int32).reshape(1)
        xb, xt, scale, lab, loss_tile = prep(inv_count, xt_own, xg, stat)

        n_chunks = vocab // (64 * LANES)
        runs = [(0, 1), (1, n_chunks - 1)] if n_chunks > 1 else [(0, 1)]
        mine = []
        for n, (first, many) in enumerate(runs):
            got = table_chunks(first, many, inv_count, vocab_off, xb, xt, scale, lab, et, 4 + n)
            mine += [got[k] for k in range(many)]
        table = None
        for c in range(n_chunks):
            gathered = lax.all_gather(mine[c], dp, axis=0)
            table = place_chunk(c, gathered, table, vocab)

        xb_late, _ = lax.optimization_barrier((xb_own, mine[-1]))
        gxt = rows_grad(inv_count, vocab_off, xb_late, scale[:tokens], lab[:tokens], et)
        dht, sums = norm_back(
            ht, w1, gxt, lax.ppermute(gxt, 'core', [(0, 1), (1, 0)]), loss_tile)
        return (sums[1, 0] * inv_count[0], dht.T.reshape(batch_rows, seq_len, dim),
                sums[0, :dim], table.T)

    return jax.shard_map(
        local_step, mesh=grid_mesh,
        in_specs=(P(dp, None, None), P(None), P('core', None), P(dp, None), P(dp, None)),
        out_specs=(P(), P(dp, None, None), P(None), P('core', None)), check_vma=False)
```

```python
import jax
import jax.numpy as jnp
from jax import lax
from jax.experimental import pallas as pl
from jax.experimental.pallas import tpu as pltpu
from jax.sharding import Mesh, PartitionSpec as P

SOFT_CAP = 30.0
INV_CAP = 1.0 / SOFT_CAP
CAP_LOG2E = SOFT_CAP * 1.4426950408889634
LANES = 128
SUB = 8
RING = 4
WAYS = (1, RING - 1)
PAIR = range(2)
VMEM_LIMIT = 60 * 1024 * 1024
F32 = jnp.float32
BF16 = jnp.bfloat16
FAR = -(2 ** 22)
MESH_ID = pl.DeviceIdType.MESH
AXES = ('z', 'y', 'x', 'core')
CUBE = ('x', 'y', 'z')
SIZES = {'z': RING, 'y': RING, 'x': RING, 'core': 2}
SEM = pltpu.SemaphoreType.DMA
HBM = pl.BlockSpec(memory_space=pl.ANY)
SMEM = pl.BlockSpec(memory_space=pltpu.SMEM)
VMEM = pl.BlockSpec(memory_space=pltpu.VMEM)


def dot_f32(a, b, dims):
    return lax.dot_general(a, b, (dims, ((), ())), preferred_element_type=F32)


def f32(*shape):
    return jax.ShapeDtypeStruct(shape, F32)


def bf16(*shape):
    return jax.ShapeDtypeStruct(shape, BF16)


def block(axis, *shape):
    return pl.BlockSpec(shape, lambda i: tuple(i if n == axis else 0 for n in range(len(shape))))


def cost(flops, moved, exps=0):
    return pl.CostEstimate(flops=flops, bytes_accessed=moved, transcendentals=exps)


def params(**kw):
    return pltpu.CompilerParams(vmem_limit_bytes=VMEM_LIMIT, **kw)


def meeting(ident):
    return params(collective_id=ident, has_side_effects=True)


def lane_slice(j):
    return slice(j * LANES, (j + 1) * LANES)


def halved(n):
    return n // (2 * SUB) * SUB


def peer(**shift):
    place = []
    for axis in AXES:
        here = lax.axis_index(axis)
        if axis in shift:
            here = lax.rem(here + shift[axis], SIZES[axis])
        place.append(here)
    return tuple(place)


def send(src, dst, send_sem, recv_sem, where):
    return pltpu.make_async_remote_copy(
        src, dst, send_sem, recv_sem, device_id=where, device_id_type=MESH_ID)


def start(copies):
    for copy in copies:
        copy.start()


def finish(copies):
    for copy in copies:
        copy.wait()


def arrive(copies):
    for copy in copies:
        copy.wait_recv()


def meet(peers):
    barrier = pltpu.get_barrier_semaphore()
    for where in peers:
        pl.semaphore_signal(barrier, inc=1, device_id=where, device_id_type=MESH_ID)
    pl.semaphore_wait(barrier, len(peers))


def others(axis):
    return [peer(**{axis: r}) for r in range(1, SIZES[axis])]


def swap_copies(k, cur_ref, slot_ref, sends, recvs):
    axis = CUBE[k]
    return [send(cur_ref.at[k], slot_ref.at[k, lax.axis_index(axis)], sends.at[k, n],
                 recvs.at[k, n], where) for n, where in enumerate(others(axis))]


def swap_sum(k, cur_ref, slot_ref, sends, recvs):
    finish(swap_copies(k, cur_ref, slot_ref, sends, recvs))
    axis = CUBE[k]
    slot_ref[k, lax.axis_index(axis)] = cur_ref[k]
    total = slot_ref[k, 0]
    for i in range(1, SIZES[axis]):
        total = total + slot_ref[k, i]
    cur_ref[k + 1] = total


def swap_scratch(width):
    n = len(CUBE)
    return [pltpu.VMEM((n + 1, SUB, width), F32), pltpu.VMEM((n, RING, SUB, width), F32),
            SEM((n, n)), SEM((n, n))]


def norm_body(ht_ref, w1_ref, xt_ref, xb_ref):
    h = ht_ref[...].astype(F32)
    inv_rms = lax.rsqrt(jnp.mean(h * h, axis=0, keepdims=True) + 1e-6)
    xt = h * inv_rms * jnp.broadcast_to(w1_ref[:, :1], h.shape)
    xt_ref[0] = xt
    xb_ref[...] = xt.T.astype(BF16)


def norm_rows(ht, w1):
    dim, tokens = ht.shape
    tb = tokens // 2
    return pl.pallas_call(
        norm_body,
        grid=(2,),
        in_specs=[block(1, dim, tb), block(None, dim, LANES)],
        out_specs=[block(0, 1, dim, tb), block(0, tb, dim)],
        out_shape=[f32(2, dim, tb), bf16(tokens, dim)],
        compiler_params=params(),
        cost_estimate=cost(10 * ht.size, 8 * ht.size),
        name="norm",
    )(ht, w1)


def norm_back_body(ht_ref, w1_ref, g0_ref, g1_ref, loss_ref, dh_ref, sum_ref, dw_ref, *swap):
    step = pl.program_id(0)
    dim, tb = ht_ref.shape
    h = ht_ref[...].astype(F32)
    inv_rms = lax.rsqrt(jnp.mean(h * h, axis=0, keepdims=True) + 1e-6)
    n = h * inv_rms
    g = g0_ref[...] + g1_ref[...]
    gn = g * n

    @pl.when(step == 0)
    def _():
        dw_ref[...] = jnp.zeros_like(dw_ref)

    part = dw_ref[...]
    for j in range(tb // LANES):
        part = part + gn[:, lane_slice(j)]
    dw_ref[...] = part
    w1 = jnp.broadcast_to(w1_ref[:, :1], h.shape)
    inner = jnp.mean(gn * w1, axis=0, keepdims=True)
    dh_ref[...] = ((g * w1 - n * inner) * inv_rms).astype(BF16)

    @pl.when(step == pl.num_programs(0) - 1)
    def _():
        cur_ref = swap[0]
        cur_ref[0] = jnp.zeros_like(cur_ref[0])
        cur_ref[0, 0:1, 0:dim] = jnp.sum(dw_ref[...].T, axis=0, keepdims=True)
        cur_ref[0, 1:2, 0:LANES] = loss_ref[0:1, :]
        meet([where for axis in CUBE for where in others(axis)])
        for k in range(len(CUBE)):
            start(swap_copies(k, *swap))
            swap_sum(k, *swap)
        sum_ref[...] = cur_ref[len(CUBE)]


def norm_back(ht, w1, g0, g1, loss_tile):
    dim, tokens = ht.shape
    tb = tokens // 2
    width = -(-dim // LANES) * LANES
    cols = block(1, dim, tb)
    return pl.pallas_call(
        norm_back_body,
        grid=(2,),
        in_specs=[cols, block(None, dim, LANES), cols, cols, block(None, SUB, LANES)],
        out_specs=[cols, block(None, SUB, width)],
        out_shape=[bf16(dim, tokens), f32(SUB, width)],
        scratch_shapes=[pltpu.VMEM((dim, LANES), F32), *swap_scratch(width)],
        compiler_params=meeting(3),
        cost_estimate=cost(20 * ht.size, 12 * ht.size),
        name="norm_back",
    )(ht, w1, g0, g1, loss_tile)


GAP = 4


def fwd_body(tb, early, late, x_ref, lab_ref, mask_ref, row_ref, e_ref, xt_ref,
             xg_ref, stat_ref, count_ref, z_ref, p_ref, pay_ref, ring_sem, half_sem, die_sem,
             stat_sem, own_sem, *swap):
    step = pl.program_id(0)
    tokens = x_ref.shape[0]
    dim, bv = e_ref.shape
    cut = halved(dim)
    spans = (pl.ds(0, cut), pl.ds(cut, dim - cut))
    core = lax.axis_index('core')
    across = peer(core=1)
    group = [peer(x=r, core=c) for r in range(1, RING) for c in PAIR]
    ring = [send(xt_ref.at[core], xg_ref.at[2 * w, core], ring_sem.at[0, w], ring_sem.at[1, w],
                 peer(x=WAYS[w])) for w in PAIR]
    on = [send(xg_ref.at[2 * w, core, spans[w]], xg_ref.at[1, core, spans[w]],
               half_sem.at[0, w], half_sem.at[1, w], peer(x=WAYS[w])) for w in PAIR]
    over = [send(xg_ref.at[r, core], xg_ref.at[r, core], die_sem.at[0, r], die_sem.at[1, r],
                 across) for r in range(RING - 1)]

    @pl.when(step == 0)
    def _():
        z_ref[...] = jnp.zeros_like(z_ref)
        p_ref[...] = jnp.zeros_like(p_ref)
        cur_ref = swap[0]
        cur_ref[0] = jnp.full(cur_ref.shape[1:], jnp.sum(mask_ref[...]), F32)
        meet(others('y') + others('z') + group + [across])

    for k in range(len(CUBE) + 1):
        @pl.when(step == k * GAP)
        def _(k=k):
            if k:
                swap_sum(k - 1, *swap)
            if k < len(CUBE):
                start(swap_copies(k, *swap))
            else:
                count_ref[...] = swap[0][k]
            if not k:
                start(ring)

    @pl.when(step == early)
    def _():
        finish(ring)
        start(on)
        start(over[::2])

    @pl.when(step == late)
    def _():
        finish(on)
        over[1].start()

    lane = lax.broadcasted_iota(jnp.int32, (tb, LANES), 1)

    def rows_part(i, carry):
        rows = pl.ds(pl.multiple_of(i * tb, tb), tb)
        z = dot_f32(x_ref[rows, :], e_ref[...], ((1,), (0,)))
        lab = lab_ref[rows, :] - step * bv
        zsum = z_ref[rows, :]
        psum = p_ref[rows, :]
        for j in range(bv // LANES):
            t = jnp.tanh(z[:, lane_slice(j)] * INV_CAP)
            zsum = zsum + jnp.exp2(t * CAP_LOG2E)
            psum = jnp.where(lab == lane + j * LANES, t, psum)
        z_ref[rows, :] = zsum
        p_ref[rows, :] = psum
        return carry

    lax.fori_loop(0, tokens // tb, rows_part, 0, unroll=True)

    @pl.when(step == pl.num_programs(0) - 1)
    def _():
        pay_ref[...] = jnp.concatenate(
            [jnp.sum(z_ref[...].T, axis=0, keepdims=True),
             jnp.sum(p_ref[...].T, axis=0, keepdims=True), row_ref[...]], axis=0)
        own = pltpu.make_async_copy(pay_ref, stat_ref.at[0, core], own_sem)
        own.start()
        copies = [send(pay_ref, stat_ref.at[(n + 1) // 2, core], stat_sem.at[0, n],
                       stat_sem.at[1, n], where) for n, where in enumerate([across] + group)]
        start(copies)
        finish(over)
        own.wait()
        finish(copies)


def forward(x, lab_rep, mask_tile, lab_row, et, xt, bv=512, tb=256):
    tokens, dim = x.shape
    vocab = et.shape[1]
    tb = min(tb, tokens)
    steps = vocab // bv
    after = len(CUBE) * GAP + 1
    early, late = max(after, steps * 9 // 16), max(after + 1, steps * 5 // 6)
    per_lane = pltpu.VMEM((tokens, LANES), F32)
    return pl.pallas_call(
        lambda *refs: fwd_body(tb, early, late, *refs),
        grid=(steps,),
        in_specs=[block(None, tokens, dim), block(None, tokens, LANES),
                  block(None, SUB, tokens // SUB), block(None, 1, tokens), block(1, dim, bv), HBM],
        out_specs=[HBM, HBM, block(None, SUB, LANES)],
        out_shape=[f32(RING - 1, 2, dim, tokens // 2), f32(RING, 2, 3, tokens), f32(SUB, LANES)],
        scratch_shapes=[
            per_lane, per_lane, pltpu.VMEM((3, tokens), F32),
            SEM((2, 2)), SEM((2, 2)), SEM((2, RING)), SEM((2, SUB)), SEM, *swap_scratch(LANES)],
        compiler_params=meeting(1),
        cost_estimate=cost(2 * x.size * vocab, 2 * et.size, 2 * tokens * vocab),
        name="fwd",
    )(x, lab_rep, mask_tile, lab_row, et, xt)


def prep_body(cnt_ref, own_ref, xg_ref, stat_ref, xb_ref, xt_ref, scale_ref, lab_ref, loss_ref):
    r = pl.program_id(0)
    _, dim, half = own_ref.shape
    inv_count = cnt_ref[0]
    whole, tail = divmod(dim, LANES)

    def store(x_ref):
        for side in PAIR:
            v = x_ref[side]
            vt = v.T.astype(BF16)
            vb = v.astype(BF16)
            rows = pl.ds(side * half, half)
            for k in range(whole):
                xb_ref[k, rows, :] = vt[:, lane_slice(k)]
            if tail:
                xb_ref[whole, rows, :] = jnp.concatenate(
                    [vt[:, dim - tail:], jnp.zeros((half, LANES - tail), BF16)], axis=1)
            for k in range(half // LANES):
                xt_ref[side * (half // LANES) + k] = vb[:, lane_slice(k)]

    @pl.when(r == 0)
    def _():
        store(own_ref)

    @pl.when(r != 0)
    def _():
        store(xg_ref.at[0])

    def stat(n):
        return stat_ref[0, 0, pl.ds(n, 1), :], stat_ref[0, 1, pl.ds(n, 1), :]

    row_sum = sum(stat(0))
    label = stat(2)[0]
    live = label >= 0.0
    scale = jnp.where(live, inv_count, 0.0) / row_sum
    for k in range(2 * half // LANES):
        cols = lane_slice(k)
        scale_ref[cols, :] = jnp.broadcast_to(scale[:, cols], (LANES, LANES)).T
        lab_ref[cols, :] = jnp.broadcast_to(label[:, cols], (LANES, LANES)).T.astype(jnp.int32)

    @pl.when(r == 0)
    def _():
        picked = sum(stat(1)) * SOFT_CAP
        loss = jnp.where(live, jnp.log(row_sum) - picked, 0.0)
        loss_ref[...] = jnp.full(loss_ref.shape, jnp.sum(loss), F32)


def prep(inv_count, xt_own, xg, stat):
    _, dim, half = xt_own.shape
    tokens = 2 * half
    slabs = -(-dim // LANES)
    per = tokens // LANES
    group = RING * tokens
    return pl.pallas_call(
        prep_body,
        grid=(RING,),
        in_specs=[
            SMEM,
            block(None, 2, dim, half),
            pl.BlockSpec((1, 2, dim, half), lambda i: (jnp.maximum(i - 1, 0), 0, 0, 0)),
            block(0, 1, *stat.shape[1:]),
        ],
        out_specs=[
            block(1, slabs, tokens, LANES),
            block(0, per, dim, LANES),
            block(0, tokens, LANES),
            block(0, tokens, LANES),
            block(None, SUB, LANES),
        ],
        out_shape=[
            bf16(slabs, group, LANES), bf16(group // LANES, dim, LANES), f32(group, LANES),
            jax.ShapeDtypeStruct((group, LANES), jnp.int32), f32(SUB, LANES),
        ],
        compiler_params=params(),
        cost_estimate=cost(40 * xg.size, 8 * xg.size),
        name="prep",
    )(inv_count, xt_own, xg, stat)


def grad_tile(z, scale, lab, vid, inv_count):
    t = jnp.tanh(z * INV_CAP)
    p = jnp.exp2(t * CAP_LOG2E) * scale
    p = jnp.where(lab == vid, p - inv_count, p)
    return (p * (1.0 - t * t)).astype(BF16)


GATHERS = ('xyz', 'yzx', 'zxy')
STEPS = (' a', 'a A', 'A bc', 'b Bdf', 'Bc eC', 'df DF', 'e E', 'CDFE ')
LETTERS = 'abcdef'
WHEN = (10, 11, 12, 15, 18, 20, 22, 25)


def main_body(n_chunks, tb, rb, cnt_ref, off_ref, xb_ref, xt_ref, scale_ref, lab_ref, et_ref,
              ag_ref, gx_ref, ebuf, rbuf, ga_ref, gb_ref, gr_ref, shard, tiles, part_in, tile_in,
              bpart_in, btile_in, esem, fsem, own_sem, psend, precv, tsend, trecv,
              bpsend, bprecv, btsend, btrecv, agsend, agrecv):
    slabs, group_tokens, _ = xb_ref.shape
    dim, tokens = gx_ref.shape
    deep = slabs * LANES
    wide = rbuf.shape[1]
    blocks = group_tokens // tb
    cut = halved(dim)
    rest = dim - cut
    units = 8 * n_chunks
    row_units = et_ref.shape[1] // (wide * LANES)
    inv_count = cnt_ref[0]
    vocab_off = off_ref[0]
    me = {axis: lax.axis_index(axis) for axis in AXES}
    lane = lax.broadcasted_iota(jnp.int32, (tb, LANES), 1)
    side = 7 * dim // 24 // SUB * SUB
    ranges = ((0, side), (side, dim - 2 * side), (dim - side, side))

    def shifted(q, da, db):
        odd = lax.rem(q // 4, 2)
        return peer(z=db + odd * (da - db), y=da + odd * (db - da))

    def tile_index(u, j):
        k = u // 8
        odd = lax.rem(k, 2)
        s = lax.rem(u, 8) // 2
        half = lax.rem(u, 2)
        db = lax.rem(2 + 3 * s + 3 * (s * (s - 1) // 2), RING)
        da = 2 + half - j * (1 + 2 * half)
        dz, dy = db + odd * (da - db), da + odd * (db - da)
        return ((k * RING + lax.rem(me['z'] + dz, RING)) * RING
                + lax.rem(me['y'] + dy, RING)) * SIZES['x'] + me['x']

    def fetch(u, j):
        cols = pl.ds(pl.multiple_of(tile_index(u, j) * LANES, LANES), LANES)
        slot = lax.rem(u, 2)
        return pltpu.make_async_copy(
            et_ref.at[:, cols], ebuf.at[slot, j, pl.ds(0, dim)], esem.at[slot, j])

    def fetch_wide(v, j):
        cols = pl.ds(pl.multiple_of((v * wide + j) * LANES, LANES), LANES)
        slot = lax.rem(v, 2)
        return pltpu.make_async_copy(
            et_ref.at[:, cols], rbuf.at[slot, j, pl.ds(0, dim)], fsem.at[slot, j])

    def parts(src, dst, sends, recvs, q, da, db):
        return (send(src.at[pl.ds(0, cut)], dst.at[0, pl.ds(0, cut)], sends.at[0], recvs.at[0],
                     shifted(q, da, db)),
                send(src.at[pl.ds(cut, rest)], dst.at[1, pl.ds(0, rest)], sends.at[1],
                     recvs.at[1], shifted(q, 3 * da, 3 * db)))

    def part_copies(q):
        return parts(tiles.at[q, 0], part_in.at[q], psend.at[q], precv.at[q], q, 1, 0)

    def bpart_copies(k):
        return parts(tiles.at[4 * k, 3], bpart_in.at[k], bpsend.at[k], bprecv.at[k], 4 * k, 0, 1)

    def tile_copies(q):
        return [send(tiles.at[q, 1 + w], tile_in.at[q, w], tsend.at[q, w], trecv.at[q, w],
                     shifted(q, WAYS[w], 0)) for w in PAIR]

    def btile_copies(k):
        return [send(tiles.at[4 * k + 1 + w, 3], btile_in.at[k, w], btsend.at[k, w],
                     btrecv.at[k, w], shifted(4 * k, 0, WAYS[w])) for w in PAIR]

    def add_parts(first, second, got):
        first[0:cut, :] += got[0, 0:cut, :]
        second[cut:dim, :] += got[1, 0:rest, :]

    def close_slab(q):
        arrive(tile_copies(q))
        tiles[q, 3] = tiles[q, 3] + (tile_in[q, 0] + tile_in[q, 1])

    def close_chunk(k):
        close_slab(4 * k + 3)
        arrive(btile_copies(k))
        shard[k] = tiles[4 * k + 3, 3] + (btile_in[k, 0] + btile_in[k, 1])

    def own_copy(k):
        return pltpu.make_async_copy(
            shard.at[k], ag_ref.at[k, me['z'], me['y'], me['x']], own_sem.at[k])

    def hops(k, letter):
        block = LETTERS.index(letter.lower())
        passed = int(letter.isupper())
        out = []
        for p, order in enumerate(GATHERS):
            phase = min(block, 2)
            axis = order[phase]
            if SIZES[axis] == 1 or (phase == 2 and block - 2 >= SIZES[order[1]]):
                continue
            for w in PAIR:
                at = dict(me)
                for done in order[:phase]:
                    at[done] = pl.ds(0, SIZES[done])
                if phase == 2:
                    at[order[1]] = lax.rem(me[order[1]] + block - 2, SIZES[order[1]])
                low, high = ranges[p]
                if passed:
                    at[axis] = lax.rem(me[axis] + RING - WAYS[w], RING)
                    mid = halved(high)
                    low, high = (low + mid, high - mid) if w else (low, mid)
                there = ag_ref.at[k, at['z'], at['y'], at['x'], pl.ds(low, high)]
                here = there if block + passed else shard.at[k, pl.ds(low, high)]
                sems = (k, p, block, passed, w)
                out.append(send(here, there, agsend.at[sems], agrecv.at[sems],
                                peer(**{axis: WAYS[w]})))
        return out

    def gather_step(k, n):
        waits, starts = STEPS[n].split(' ')
        for letter in waits:
            arrive(hops(k, letter))
        if n == 0:
            own_copy(k).start()
        if n == 2:
            own_copy(k).wait()
        for letter in starts:
            start(hops(k, letter))

    def gather_ticks(u, low, high):
        for n, due in enumerate(WHEN):
            if due < high and due + units > low:
                k = (u - due) // 8

                @pl.when((u >= due) & (k < n_chunks) & (lax.rem(u - due + 8, 8) == 0))
                def _(k=k, n=n):
                    gather_step(k, n)

    if deep > dim:
        zeros = jnp.zeros((deep - dim, LANES), BF16)
        for slot in PAIR:
            for j in PAIR:
                ebuf[slot, j, dim:, :] = zeros
            for j in range(wide):
                rbuf[slot, j, dim:, :] = zeros
    start([fetch(0, j) for j in PAIR])
    meet([peer(**{axis: w}) for axis in CUBE if SIZES[axis] > 1 for w in WAYS])

    def table_unit(u, carry):
        slot = lax.rem(u, 2)
        q = u // 2
        k = u // 8
        s = lax.rem(q, 4)
        half = slot
        for j in PAIR:
            fetch(u, j).wait()

        @pl.when(u + 1 < units)
        def _():
            start([fetch(u + 1, j) for j in PAIR])

        bases = [tile_index(u, j) * LANES + vocab_off for j in PAIR]

        def grads(i, g_ref):
            rows = pl.ds(pl.multiple_of(i * tb, tb), tb)
            x = jnp.concatenate([xb_ref[n, rows, :] for n in range(slabs)], axis=1)
            e = jnp.concatenate([ebuf[slot, 0], ebuf[slot, 1]], axis=1)
            z = dot_f32(x, e, ((1,), (0,)))
            lab = lab_ref[rows, :]
            scale = scale_ref[rows, :]
            for j in PAIR:
                g_ref[j] = grad_tile(z[:, lane_slice(j)], scale, lab - bases[j], lane,
                                     inv_count)

        def product(i, g_ref, store):
            n = tb // LANES
            x = jnp.concatenate([xt_ref[i * n + m] for m in range(n)], axis=1)
            g = jnp.concatenate([g_ref[0], g_ref[1]], axis=1)
            part = dot_f32(x, g, ((1,), (0,)))
            for j in PAIR:
                store(2 * half + j, part[:, lane_slice(j)])

        def put(t, part):
            tiles[q, t] = part

        def add(t, part):
            tiles[q, t] += part

        grads(0, ga_ref)
        grads(1, gb_ref)
        product(0, ga_ref, put)

        def both(i, c):
            grads(2 * i, ga_ref)
            product(2 * i - 1, gb_ref, add)
            grads(2 * i + 1, gb_ref)
            product(2 * i, ga_ref, add)
            return c

        lax.fori_loop(1, blocks // 2, both, 0)
        product(blocks - 1, gb_ref, add)

        @pl.when(half == 0)
        def _():
            @pl.when((s == 1) & (k > 0))
            def _():
                close_chunk(k - 1)

            start(part_copies(q))

        @pl.when(half == 1)
        def _():
            arrive(part_copies(q))
            add_parts(tiles.at[q, 1], tiles.at[q, 2], part_in.at[q])

            @pl.when(s >= 1)
            def _():
                close_slab(q - 1)

            start(tile_copies(q))

            @pl.when(s == 1)
            def _():
                start(bpart_copies(k))

            @pl.when(s == 3)
            def _():
                arrive(bpart_copies(k))
                add_parts(tiles.at[4 * k + 1, 3], tiles.at[4 * k + 2, 3], bpart_in.at[k])
                start(btile_copies(k))

        gather_ticks(u, 0, units)
        return carry

    lax.fori_loop(0, units, table_unit, 0)

    row_lane = lax.broadcasted_iota(jnp.int32, (rb, LANES), 1)
    start([fetch_wide(0, j) for j in range(wide)])
    gx_ref[...] = jnp.zeros_like(gx_ref)

    def row_unit(v, carry):
        slot = lax.rem(v, 2)
        for j in range(wide):
            fetch_wide(v, j).wait()

        @pl.when(v + 1 < row_units)
        def _():
            start([fetch_wide(v + 1, j) for j in range(wide)])

        base = v * wide * LANES + vocab_off

        def block(i, c):
            rows = pl.ds(pl.multiple_of(i * rb, rb), rb)
            x = jnp.concatenate([xb_ref[n, rows, :] for n in range(slabs)], axis=1)
            e = jnp.concatenate([rbuf[slot, j] for j in range(wide)], axis=1)
            z = dot_f32(x, e, ((1,), (0,)))
            lab = lab_ref[rows, :] - base
            scale = scale_ref[rows, :]
            for j in range(wide):
                gr_ref[:, lane_slice(j)] = grad_tile(
                    z[:, lane_slice(j)], scale, lab, row_lane + j * LANES, inv_count)
            e = jnp.concatenate([rbuf[slot, j, 0:dim, :] for j in range(wide)], axis=1)
            gx_ref[:, rows] += dot_f32(e, gr_ref[...], ((1,), (1,)))
            return c

        lax.fori_loop(0, tokens // rb, block, 0)

        @pl.when(v == 2)
        def _():
            close_chunk(n_chunks - 1)

        gather_ticks(v + units, units, units + row_units)
        return carry

    lax.fori_loop(0, row_units, row_unit, 0)

    def sent(q, carry):
        for copy in (*part_copies(q), *tile_copies(q)):
            copy.wait_send()
        return carry

    lax.fori_loop(0, 4 * n_chunks, sent, 0)

    def sent_chunk(k, carry):
        for copy in (*bpart_copies(k), *btile_copies(k)):
            copy.wait_send()
        for letter in LETTERS + LETTERS.upper():
            for copy in hops(k, letter):
                copy.wait_send()
        return carry

    lax.fori_loop(0, n_chunks, sent_chunk, 0)


def backward(inv_count, vocab_off, xb, xt, scale, lab, et, tb=512, rb=256, wide=8):
    slabs, group_tokens, _ = xb.shape
    dim = xt.shape[1]
    vocab = et.shape[1]
    tokens = group_tokens // SIZES['x']
    cube = tuple(SIZES[axis] for axis in AXES[:3])
    n_chunks = vocab // (LANES * cube[0] * cube[1] * cube[2])
    tb, rb = min(tb, group_tokens // 4), min(rb, tokens)
    part = dim - halved(dim)
    q = RING * n_chunks
    tile = (dim, LANES)
    held = (slabs * LANES, LANES)

    def vmem(dtype, *shape):
        return pltpu.VMEM(shape, dtype)

    return pl.pallas_call(
        lambda *refs: main_body(n_chunks, tb, rb, *refs),
        in_specs=[SMEM, SMEM, VMEM, VMEM, VMEM, VMEM, HBM],
        out_specs=[HBM, VMEM],
        out_shape=[f32(n_chunks, *cube, *tile), f32(dim, tokens)],
        scratch_shapes=[
            vmem(BF16, 2, 2, *held), vmem(BF16, 2, wide, *held),
            vmem(BF16, 2, tb, LANES), vmem(BF16, 2, tb, LANES), vmem(BF16, rb, wide * LANES),
            vmem(F32, n_chunks, *tile), vmem(F32, q, RING, *tile),
            vmem(F32, q, 2, part, LANES), vmem(F32, q, 2, *tile),
            vmem(F32, n_chunks, 2, part, LANES), vmem(F32, n_chunks, 2, *tile),
            SEM((2, 2)), SEM((2, wide)), SEM((n_chunks,)),
            *[SEM((q, 2))] * 4,
            *[SEM((n_chunks, 2))] * 4,
            *[SEM((n_chunks, len(GATHERS), len(LETTERS), 2, 2))] * 2,
        ],
        compiler_params=meeting(2),
        cost_estimate=cost(8 * xt.size * vocab, 4 * et.size),
        name="backward",
    )(inv_count, vocab_off, xb, xt, scale, lab, et)


def place_body(n, src_ref, out_ref):
    for k in range(n):
        out_ref[:, lane_slice(k)] = src_ref[0, k]


def place(gathered):
    n_chunks, n_dev, dim, _ = gathered.shape
    rows = dim // 6 if dim % 48 == 0 else dim
    return pl.pallas_call(
        lambda *refs: place_body(n_dev, *refs),
        grid=(n_chunks, dim // rows),
        in_specs=[pl.BlockSpec((1, n_dev, rows, LANES), lambda c, i: (c, 0, i, 0))],
        out_specs=pl.BlockSpec((rows, n_dev * LANES), lambda c, i: (i, c)),
        out_shape=f32(dim, n_chunks * n_dev * LANES),
        compiler_params=params(),
        cost_estimate=cost(gathered.size, 8 * gathered.size),
        name="place",
    )(gathered)


def solution(mesh):
    grid_mesh = Mesh(mesh.devices.reshape(RING, RING, RING, 2), AXES)
    dp = AXES[:3]

    def local_step(hidden, norm_w, embed_table, labels, loss_mask):
        batch_rows, seq_len, dim = hidden.shape
        vocab = embed_table.shape[0]
        tokens = batch_rows * seq_len
        et = embed_table.T
        ht = hidden.reshape(tokens, dim).T
        w1 = jnp.broadcast_to((1.0 + norm_w.astype(F32))[:, None], (dim, LANES))
        mask_row = loss_mask.reshape(1, tokens)
        lab_row = labels.reshape(1, tokens)
        core = lax.axis_index('core')

        xt_own, xb_own = norm_rows(ht, w1)
        lab_rep = jnp.broadcast_to((lab_row.reshape(tokens) - core * vocab)[:, None], (tokens, LANES))
        lab_live = jnp.where(mask_row > 0, lab_row, FAR).astype(F32)
        xg, stat, count = forward(
            xb_own, lab_rep, mask_row.reshape(SUB, tokens // SUB).astype(F32), lab_live, et, xt_own)
        inv_count = (1.0 / jnp.maximum(count[0, 0], 1.0)).reshape(1)
        vocab_off = (core * vocab).astype(jnp.int32).reshape(1)
        xb, xt, scale, lab, loss_tile = prep(inv_count, xt_own, xg, stat)

        gathered, gxt = backward(inv_count, vocab_off, xb, xt, scale, lab, et)
        table = place(gathered.reshape(-1, RING ** 3, dim, LANES))
        dht, sums = norm_back(
            ht, w1, gxt, lax.ppermute(gxt, 'core', [(0, 1), (1, 0)]), loss_tile)
        return (sums[1, 0] * inv_count[0], dht.T.reshape(batch_rows, seq_len, dim),
                sums[0, :dim], table.T)

    return jax.shard_map(
        local_step, mesh=grid_mesh,
        in_specs=(P(dp, None, None), P(None), P('core', None), P(dp, None), P(dp, None)),
        out_specs=(P(), P(dp, None, None), P(None), P('core', None)), check_vma=False)
```

```python
import jax
import jax.numpy as jnp
from jax import lax
from jax.experimental import pallas as pl
from jax.experimental.pallas import tpu as pltpu
from jax.sharding import Mesh, PartitionSpec as P

SOFT_CAP = 30.0
INV_CAP = 1.0 / SOFT_CAP
CAP_LOG2E = SOFT_CAP * 1.4426950408889634
LANES = 128
SUB = 8
RING = 4
WAYS = (1, RING - 1)
PAIR = range(2)
VMEM_LIMIT = 60 * 1024 * 1024
F32 = jnp.float32
BF16 = jnp.bfloat16
FAR = -(2 ** 22)
MESH_ID = pl.DeviceIdType.MESH
AXES = ('z', 'y', 'x', 'core')
CUBE = ('x', 'y', 'z')
SIZES = {'z': RING, 'y': RING, 'x': RING, 'core': 2}
SEM = pltpu.SemaphoreType.DMA
HBM = pl.BlockSpec(memory_space=pl.ANY)
SMEM = pl.BlockSpec(memory_space=pltpu.SMEM)
VMEM = pl.BlockSpec(memory_space=pltpu.VMEM)


def dot_f32(a, b, dims):
    return lax.dot_general(a, b, (dims, ((), ())), preferred_element_type=F32)


def f32(*shape):
    return jax.ShapeDtypeStruct(shape, F32)


def bf16(*shape):
    return jax.ShapeDtypeStruct(shape, BF16)


def block(axis, *shape):
    return pl.BlockSpec(shape, lambda i: tuple(i if n == axis else 0 for n in range(len(shape))))


def cost(flops, moved, exps=0):
    return pl.CostEstimate(flops=flops, bytes_accessed=moved, transcendentals=exps)


def params(**kw):
    return pltpu.CompilerParams(vmem_limit_bytes=VMEM_LIMIT, **kw)


def meeting(ident):
    return params(collective_id=ident, has_side_effects=True)


def lane_slice(j):
    return slice(j * LANES, (j + 1) * LANES)


def halved(n):
    return n // (2 * SUB) * SUB


def peer(**shift):
    place = []
    for axis in AXES:
        here = lax.axis_index(axis)
        if axis in shift:
            here = lax.rem(here + shift[axis], SIZES[axis])
        place.append(here)
    return tuple(place)


def send(src, dst, send_sem, recv_sem, where):
    return pltpu.make_async_remote_copy(
        src, dst, send_sem, recv_sem, device_id=where, device_id_type=MESH_ID)


def start(copies):
    for copy in copies:
        copy.start()


def finish(copies):
    for copy in copies:
        copy.wait()


def arrive(copies):
    for copy in copies:
        copy.wait_recv()


def meet(peers):
    barrier = pltpu.get_barrier_semaphore()
    for where in peers:
        pl.semaphore_signal(barrier, inc=1, device_id=where, device_id_type=MESH_ID)
    pl.semaphore_wait(barrier, len(peers))


def others(axis):
    return [peer(**{axis: r}) for r in range(1, SIZES[axis])]


def swap_copies(k, cur_ref, slot_ref, sends, recvs):
    axis = CUBE[k]
    return [send(cur_ref.at[k], slot_ref.at[k, lax.axis_index(axis)], sends.at[k, n],
                 recvs.at[k, n], where) for n, where in enumerate(others(axis))]


def swap_sum(k, cur_ref, slot_ref, sends, recvs):
    finish(swap_copies(k, cur_ref, slot_ref, sends, recvs))
    axis = CUBE[k]
    slot_ref[k, lax.axis_index(axis)] = cur_ref[k]
    total = slot_ref[k, 0]
    for i in range(1, SIZES[axis]):
        total = total + slot_ref[k, i]
    cur_ref[k + 1] = total


def swap_scratch(width):
    n = len(CUBE)
    return [pltpu.VMEM((n + 1, SUB, width), F32), pltpu.VMEM((n, RING, SUB, width), F32),
            SEM((n, n)), SEM((n, n))]


def norm_body(ht_ref, w1_ref, xt_ref, xb_ref):
    h = ht_ref[...].astype(F32)
    inv_rms = lax.rsqrt(jnp.mean(h * h, axis=0, keepdims=True) + 1e-6)
    xt = h * inv_rms * jnp.broadcast_to(w1_ref[:, :1], h.shape)
    xt_ref[0] = xt
    xb_ref[...] = xt.T.astype(BF16)


def norm_rows(ht, w1):
    dim, tokens = ht.shape
    tb = tokens // 2
    return pl.pallas_call(
        norm_body,
        grid=(2,),
        in_specs=[block(1, dim, tb), block(None, dim, LANES)],
        out_specs=[block(0, 1, dim, tb), block(0, tb, dim)],
        out_shape=[f32(2, dim, tb), bf16(tokens, dim)],
        compiler_params=params(),
        cost_estimate=cost(10 * ht.size, 8 * ht.size),
        name="norm",
    )(ht, w1)


GAP = 4


def fwd_body(tb, early, late, x_ref, lab_ref, mask_ref, row_ref, e_ref, xt_ref,
             xg_ref, stat_ref, count_ref, z_ref, p_ref, pay_ref, ring_sem, half_sem, die_sem,
             stat_sem, own_sem, *swap):
    step = pl.program_id(0)
    tokens = x_ref.shape[0]
    dim, bv = e_ref.shape
    cut = halved(dim)
    spans = (pl.ds(0, cut), pl.ds(cut, dim - cut))
    core = lax.axis_index('core')
    across = peer(core=1)
    group = [peer(x=r, core=c) for r in range(1, RING) for c in PAIR]
    ring = [send(xt_ref.at[core], xg_ref.at[2 * w, core], ring_sem.at[0, w], ring_sem.at[1, w],
                 peer(x=WAYS[w])) for w in PAIR]
    on = [send(xg_ref.at[2 * w, core, spans[w]], xg_ref.at[1, core, spans[w]],
               half_sem.at[0, w], half_sem.at[1, w], peer(x=WAYS[w])) for w in PAIR]
    over = [send(xg_ref.at[r, core], xg_ref.at[r, core], die_sem.at[0, r], die_sem.at[1, r],
                 across) for r in range(RING - 1)]

    @pl.when(step == 0)
    def _():
        z_ref[...] = jnp.zeros_like(z_ref)
        p_ref[...] = jnp.zeros_like(p_ref)
        cur_ref = swap[0]
        cur_ref[0] = jnp.full(cur_ref.shape[1:], jnp.sum(mask_ref[...]), F32)
        with jax.named_scope('f_meet'):
            meet(others('y') + others('z') + group + [across])

    for k in range(len(CUBE) + 1):
        @pl.when(step == k * GAP)
        def _(k=k):
            if k:
                swap_sum(k - 1, *swap)
            if k < len(CUBE):
                start(swap_copies(k, *swap))
            else:
                count_ref[...] = swap[0][k]
            if not k:
                start(ring)

    @pl.when(step == early)
    def _():
        with jax.named_scope('f_ring'):
            finish(ring)
        start(on)
        start(over[::2])

    @pl.when(step == late)
    def _():
        with jax.named_scope('f_on'):
            finish(on)
        over[1].start()

    lane = lax.broadcasted_iota(jnp.int32, (tb, LANES), 1)

    def rows_part(i, carry):
        rows = pl.ds(pl.multiple_of(i * tb, tb), tb)
        z = dot_f32(x_ref[rows, :], e_ref[...], ((1,), (0,)))
        lab = lab_ref[rows, :] - step * bv
        zsum = z_ref[rows, :]
        psum = p_ref[rows, :]
        for j in range(bv // LANES):
            t = jnp.tanh(z[:, lane_slice(j)] * INV_CAP)
            zsum = zsum + jnp.exp2(t * CAP_LOG2E)
            psum = jnp.where(lab == lane + j * LANES, t, psum)
        z_ref[rows, :] = zsum
        p_ref[rows, :] = psum
        return carry

    lax.fori_loop(0, tokens // tb, rows_part, 0, unroll=True)

    @pl.when(step == pl.num_programs(0) - 1)
    def _():
        pay_ref[...] = jnp.concatenate(
            [jnp.sum(z_ref[...].T, axis=0, keepdims=True),
             jnp.sum(p_ref[...].T, axis=0, keepdims=True), row_ref[...]], axis=0)
        own = pltpu.make_async_copy(pay_ref, stat_ref.at[0, core], own_sem)
        own.start()
        copies = [send(pay_ref, stat_ref.at[(n + 1) // 2, core], stat_sem.at[0, n],
                       stat_sem.at[1, n], where) for n, where in enumerate([across] + group)]
        start(copies)
        with jax.named_scope('f_end'):
            finish(over)
            own.wait()
            finish(copies)


def forward(x, lab_rep, mask_tile, lab_row, et, xt, bv=512, tb=256):
    tokens, dim = x.shape
    vocab = et.shape[1]
    tb = min(tb, tokens)
    steps = vocab // bv
    after = len(CUBE) * GAP + 1
    early, late = max(after, steps * 9 // 16), max(after + 1, steps * 5 // 6)
    per_lane = pltpu.VMEM((tokens, LANES), F32)
    return pl.pallas_call(
        lambda *refs: fwd_body(tb, early, late, *refs),
        grid=(steps,),
        in_specs=[block(None, tokens, dim), block(None, tokens, LANES),
                  block(None, SUB, tokens // SUB), block(None, 1, tokens), block(1, dim, bv), HBM],
        out_specs=[HBM, HBM, block(None, SUB, LANES)],
        out_shape=[f32(RING - 1, 2, dim, tokens // 2), f32(RING, 2, 3, tokens), f32(SUB, LANES)],
        scratch_shapes=[
            per_lane, per_lane, pltpu.VMEM((3, tokens), F32),
            SEM((2, 2)), SEM((2, 2)), SEM((2, RING)), SEM((2, SUB)), SEM, *swap_scratch(LANES)],
        compiler_params=meeting(1),
        cost_estimate=cost(2 * x.size * vocab, 2 * et.size, 2 * tokens * vocab),
        name="fwd",
    )(x, lab_rep, mask_tile, lab_row, et, xt)


def prep_body(cnt_ref, own_ref, xg_ref, stat_ref, xb_ref, xt_ref, scale_ref, lab_ref, loss_ref):
    r = pl.program_id(0)
    _, dim, half = own_ref.shape
    inv_count = cnt_ref[0]
    whole, tail = divmod(dim, LANES)

    def store(x_ref):
        for side in PAIR:
            vb = x_ref[side].astype(BF16)
            vt = vb.T
            rows = pl.ds(side * half, half)
            for k in range(whole):
                xb_ref[k, rows, :] = vt[:, lane_slice(k)]
            if tail:
                xb_ref[whole, rows, :] = jnp.concatenate(
                    [vt[:, dim - tail:], jnp.zeros((half, LANES - tail), BF16)], axis=1)
            for k in range(half // LANES):
                xt_ref[side * (half // LANES) + k] = vb[:, lane_slice(k)]

    @pl.when(r == 0)
    def _():
        store(own_ref)

    @pl.when(r != 0)
    def _():
        store(xg_ref.at[0])

    def stat(n):
        return stat_ref[0, 0, pl.ds(n, 1), :], stat_ref[0, 1, pl.ds(n, 1), :]

    row_sum = sum(stat(0))
    label = stat(2)[0]
    live = label >= 0.0
    scale = jnp.where(live, inv_count, 0.0) / row_sum
    for k in range(2 * half // LANES):
        cols = lane_slice(k)
        scale_ref[cols, :] = jnp.broadcast_to(scale[:, cols], (LANES, LANES)).T
        lab_ref[cols, :] = jnp.broadcast_to(label[:, cols], (LANES, LANES)).T.astype(jnp.int32)

    @pl.when(r == 0)
    def _():
        picked = sum(stat(1)) * SOFT_CAP
        loss = jnp.where(live, jnp.log(row_sum) - picked, 0.0)
        loss_ref[...] = jnp.full(loss_ref.shape, jnp.sum(loss), F32)


def prep(inv_count, xt_own, xg, stat):
    _, dim, half = xt_own.shape
    tokens = 2 * half
    slabs = -(-dim // LANES)
    per = tokens // LANES
    group = RING * tokens
    return pl.pallas_call(
        prep_body,
        grid=(RING,),
        in_specs=[
            SMEM,
            block(None, 2, dim, half),
            pl.BlockSpec((1, 2, dim, half), lambda i: (jnp.maximum(i - 1, 0), 0, 0, 0)),
            block(0, 1, *stat.shape[1:]),
        ],
        out_specs=[
            block(1, slabs, tokens, LANES),
            block(0, per, dim, LANES),
            block(0, tokens, LANES),
            block(0, tokens, LANES),
            block(None, SUB, LANES),
        ],
        out_shape=[
            bf16(slabs, group, LANES), bf16(group // LANES, dim, LANES), f32(group, LANES),
            jax.ShapeDtypeStruct((group, LANES), jnp.int32), f32(SUB, LANES),
        ],
        compiler_params=params(),
        cost_estimate=cost(40 * xg.size, 8 * xg.size),
        name="prep",
    )(inv_count, xt_own, xg, stat)


def grad_tile(z, scale, lab, vid, inv_count):
    t = jnp.tanh(z * INV_CAP)
    p = jnp.exp2(t * CAP_LOG2E) * scale
    p = jnp.where(lab == vid, p - inv_count, p)
    return (p * (1.0 - t * t)).astype(BF16)


GATHERS = ('xyz', 'yzx', 'zxy')
STEPS = (' a', 'a A', 'A bc', 'b Bdf', 'Bc eC', 'df DF', 'e E', 'CDFE ')
LETTERS = 'abcdef'
ADD_LAG = (1, 3, 3)
TILE_LAG = (2, 3, 3)
WHEN = ((9, 10, 12, 15, 19, 21, 22, 25), (12, 13, 16, 19, 21, 24, 26, 38),
        (13, 16, 17, 22, 23, 27, 29, 33))


def main_body(n_chunks, tb, rb, cnt_ref, off_ref, xb_ref, xt_ref, scale_ref, lab_ref, ht_ref,
              w1_ref, loss_ref, et_ref, ag_ref, dh_ref, sum_ref,
              gx_ref, gin_ref, dw_ref, ebuf, rbuf, ga_ref, gb_ref, gr_ref, shard, tiles, part_in,
              tile_in, bpart_in, btile_in, esem, fsem, gsem, own_sem, psend, precv, tsend, trecv,
              bpsend, bprecv, btsend, btrecv, agsend, agrecv, *swap):
    slabs, group_tokens, _ = xb_ref.shape
    dim, tokens = gx_ref.shape
    deep = slabs * LANES
    wide = rbuf.shape[1]
    blocks = group_tokens // tb
    cut = halved(dim)
    rest = dim - cut
    units = 8 * n_chunks
    row_units = et_ref.shape[1] // (wide * LANES)
    inv_count = cnt_ref[0]
    vocab_off = off_ref[0]
    me = {axis: lax.axis_index(axis) for axis in AXES}
    lane = lax.broadcasted_iota(jnp.int32, (tb, LANES), 1)
    side = 11 * dim // 36 // SUB * SUB
    ranges = ((0, side), (side, dim - 2 * side), (dim - side, side))

    def shifted(q, da, db):
        odd = lax.rem(q // 4, 2)
        return peer(z=db + odd * (da - db), y=da + odd * (db - da))

    def tile_index(u, j):
        k = u // 8
        odd = lax.rem(k, 2)
        s = lax.rem(u, 8) // 2
        half = lax.rem(u, 2)
        db = lax.rem(2 + 3 * s + 3 * (s * (s - 1) // 2), RING)
        da = 2 + half - j * (1 + 2 * half)
        dz, dy = db + odd * (da - db), da + odd * (db - da)
        return ((k * RING + lax.rem(me['z'] + dz, RING)) * RING
                + lax.rem(me['y'] + dy, RING)) * SIZES['x'] + me['x']

    def fetch(u, j):
        cols = pl.ds(pl.multiple_of(tile_index(u, j) * LANES, LANES), LANES)
        slot = lax.rem(u, 2)
        return pltpu.make_async_copy(
            et_ref.at[:, cols], ebuf.at[slot, j, pl.ds(0, dim)], esem.at[slot, j])

    def fetch_wide(v, j):
        cols = pl.ds(pl.multiple_of((v * wide + j) * LANES, LANES), LANES)
        slot = lax.rem(v, 2)
        return pltpu.make_async_copy(
            et_ref.at[:, cols], rbuf.at[slot, j, pl.ds(0, dim)], fsem.at[slot, j])

    def parts(src, dst, sends, recvs, q, da, db):
        return (send(src.at[pl.ds(0, cut)], dst.at[0, pl.ds(0, cut)], sends.at[0], recvs.at[0],
                     shifted(q, da, db)),
                send(src.at[pl.ds(cut, rest)], dst.at[1, pl.ds(0, rest)], sends.at[1],
                     recvs.at[1], shifted(q, 3 * da, 3 * db)))

    def part_copies(q):
        return parts(tiles.at[q, 0], part_in.at[q], psend.at[q], precv.at[q], q, 1, 0)

    def bpart_copies(k):
        return parts(tiles.at[4 * k, 3], bpart_in.at[k], bpsend.at[k], bprecv.at[k], 4 * k, 0, 1)

    def tile_copies(q):
        return [send(tiles.at[q, 1 + w], tile_in.at[q, w], tsend.at[q, w], trecv.at[q, w],
                     shifted(q, WAYS[w], 0)) for w in PAIR]

    def btile_copies(k):
        return [send(tiles.at[4 * k + 1 + w, 3], btile_in.at[k, w], btsend.at[k, w],
                     btrecv.at[k, w], shifted(4 * k, 0, WAYS[w])) for w in PAIR]

    def add_parts(first, second, got):
        first[0:cut, :] += got[0, 0:cut, :]
        second[cut:dim, :] += got[1, 0:rest, :]

    def close_slab(q):
        with jax.named_scope('w_tile'):
            arrive(tile_copies(q))
        tiles[q, 3] = tiles[q, 3] + (tile_in[q, 0] + tile_in[q, 1])

    def close_chunk(k):
        close_slab(4 * k + 3)
        with jax.named_scope('w_btile'):
            arrive(btile_copies(k))
        shard[k] = tiles[4 * k + 3, 3] + (btile_in[k, 0] + btile_in[k, 1])

    def own_copy(k):
        return pltpu.make_async_copy(
            shard.at[k], ag_ref.at[k, me['z'], me['y'], me['x']], own_sem.at[k])

    def hops(k, letter):
        block = LETTERS.index(letter.lower())
        passed = int(letter.isupper())
        out = []
        for p, order in enumerate(GATHERS):
            phase = min(block, 2)
            axis = order[phase]
            if SIZES[axis] == 1 or (phase == 2 and block - 2 >= SIZES[order[1]]):
                continue
            for w in PAIR:
                at = dict(me)
                for done in order[:phase]:
                    at[done] = pl.ds(0, SIZES[done])
                if phase == 2:
                    at[order[1]] = lax.rem(me[order[1]] + block - 2, SIZES[order[1]])
                low, high = ranges[p]
                if passed:
                    at[axis] = lax.rem(me[axis] + RING - WAYS[w], RING)
                    mid = halved(high)
                    low, high = (low + mid, high - mid) if w else (low, mid)
                there = ag_ref.at[k, at['z'], at['y'], at['x'], pl.ds(low, high)]
                here = there if block + passed else shard.at[k, pl.ds(low, high)]
                sems = (k, p, block, passed, w)
                out.append(send(here, there, agsend.at[sems], agrecv.at[sems],
                                peer(**{axis: WAYS[w]})))
        return out

    def gather_step(k, n):
        waits, starts = STEPS[n].split(' ')
        for letter in waits:
            with jax.named_scope(f'w_g{n}{letter}'):
                arrive(hops(k, letter))
        if n == 0:
            own_copy(k).start()
        if n == 2:
            own_copy(k).wait()
        for letter in starts:
            start(hops(k, letter))

    def ticks(u, low, high):
        def every_other(first, count):
            def run(act):
                if first < high and first + 2 * count > low:
                    @pl.when((u >= first) & (u < first + 2 * count) & (lax.rem(u + first, 2) == 0))
                    def _():
                        act((u - first) // 2)
            return run

        for k in range(n_chunks):
            added = 8 * k + ADD_LAG[min(k, 2)]
            closed = added + TILE_LAG[min(k, 2)]

            @every_other(added, RING)
            def _(s, k=k):
                q = 4 * k + s
                with jax.named_scope('w_part'):
                    arrive(part_copies(q))
                add_parts(tiles.at[q, 1], tiles.at[q, 2], part_in.at[q])
                start(tile_copies(q))

            @every_other(closed, RING - 1)
            def _(s, k=k):
                close_slab(4 * k + s)

                @pl.when(s == 0)
                def _():
                    start(bpart_copies(k))

                @pl.when(s == 2)
                def _():
                    with jax.named_scope('w_bpart'):
                        arrive(bpart_copies(k))
                    add_parts(tiles.at[4 * k + 1, 3], tiles.at[4 * k + 2, 3], bpart_in.at[k])
                    start(btile_copies(k))

            @every_other(closed + 2 * RING - 2, 1)
            def _(s, k=k):
                close_chunk(k)

        for k in range(n_chunks):
            for n, late in enumerate(WHEN[min(k, 2)]):
                due = 8 * k + late
                if low <= due < high:
                    @pl.when(u == due)
                    def _(k=k, n=n):
                        gather_step(k, n)

    if deep > dim:
        zeros = jnp.zeros((deep - dim, LANES), BF16)
        for slot in PAIR:
            for j in PAIR:
                ebuf[slot, j, dim:, :] = zeros
            for j in range(wide):
                rbuf[slot, j, dim:, :] = zeros
    start([fetch(0, j) for j in PAIR])
    with jax.named_scope('w_meet'):
        meet([where for axis in AXES for where in others(axis)])

    def table_unit(u, carry):
        slot = lax.rem(u, 2)
        q = u // 2
        half = slot
        for j in PAIR:
            fetch(u, j).wait()

        @pl.when(u + 1 < units)
        def _():
            start([fetch(u + 1, j) for j in PAIR])

        bases = [tile_index(u, j) * LANES + vocab_off for j in PAIR]

        def grads(i, g_ref):
            rows = pl.ds(pl.multiple_of(i * tb, tb), tb)
            x = jnp.concatenate([xb_ref[n, rows, :] for n in range(slabs)], axis=1)
            e = jnp.concatenate([ebuf[slot, 0], ebuf[slot, 1]], axis=1)
            z = dot_f32(x, e, ((1,), (0,)))
            lab = lab_ref[rows, :]
            scale = scale_ref[rows, :]
            for j in PAIR:
                g_ref[j] = grad_tile(z[:, lane_slice(j)], scale, lab - bases[j], lane,
                                     inv_count)

        def product(i, g_ref, store):
            n = tb // LANES
            x = jnp.concatenate([xt_ref[i * n + m] for m in range(n)], axis=1)
            g = jnp.concatenate([g_ref[0], g_ref[1]], axis=1)
            part = dot_f32(x, g, ((1,), (0,)))
            for j in PAIR:
                store(2 * half + j, part[:, lane_slice(j)])

        def put(t, part):
            tiles[q, t] = part

        def add(t, part):
            tiles[q, t] += part

        grads(0, ga_ref)
        grads(1, gb_ref)
        product(0, ga_ref, put)

        def both(i, c):
            grads(2 * i, ga_ref)
            product(2 * i - 1, gb_ref, add)
            grads(2 * i + 1, gb_ref)
            product(2 * i, ga_ref, add)
            return c

        with jax.named_scope('t_comp'):
            lax.fori_loop(1, blocks // 2, both, 0)
            product(blocks - 1, gb_ref, add)

        @pl.when(half == 0)
        def _():
            start(part_copies(q))

        ticks(u, 0, units)
        return carry

    lax.fori_loop(0, units, table_unit, 0)

    row_lane = lax.broadcasted_iota(jnp.int32, (rb, LANES), 1)
    start([fetch_wide(0, j) for j in range(wide)])
    gx_ref[...] = jnp.zeros_like(gx_ref)

    def row_unit(v, carry):
        slot = lax.rem(v, 2)
        for j in range(wide):
            fetch_wide(v, j).wait()

        @pl.when(v + 1 < row_units)
        def _():
            start([fetch_wide(v + 1, j) for j in range(wide)])

        base = v * wide * LANES + vocab_off

        def block(i, c):
            rows = pl.ds(pl.multiple_of(i * rb, rb), rb)
            x = jnp.concatenate([xb_ref[n, rows, :] for n in range(slabs)], axis=1)
            e = jnp.concatenate([rbuf[slot, j] for j in range(wide)], axis=1)
            z = dot_f32(x, e, ((1,), (0,)))
            lab = lab_ref[rows, :] - base
            scale = scale_ref[rows, :]
            for j in range(wide):
                gr_ref[:, lane_slice(j)] = grad_tile(
                    z[:, lane_slice(j)], scale, lab, row_lane + j * LANES, inv_count)
            e = jnp.concatenate([rbuf[slot, j, 0:dim, :] for j in range(wide)], axis=1)
            gx_ref[:, rows] += dot_f32(e, gr_ref[...], ((1,), (1,)))
            return c

        with jax.named_scope('r_comp'):
            lax.fori_loop(0, tokens // rb, block, 0)

        ticks(v + units, units, units + row_units)
        return carry

    lax.fori_loop(0, row_units, row_unit, 0)

    if SIZES['core'] > 1:
        swap_rows = send(gx_ref, gin_ref, gsem.at[0], gsem.at[1], peer(core=1))
        swap_rows.start()
        with jax.named_scope('w_rows'):
            swap_rows.wait()
    else:
        gin_ref[...] = jnp.zeros_like(gin_ref)
    dw_ref[...] = jnp.zeros_like(dw_ref)

    def norm_back(i, carry):
        cols = pl.ds(pl.multiple_of(i * rb, rb), rb)
        h = ht_ref[:, cols].astype(F32)
        inv_rms = lax.rsqrt(jnp.mean(h * h, axis=0, keepdims=True) + 1e-6)
        n = h * inv_rms
        g = gx_ref[:, cols] + gin_ref[:, cols]
        gn = g * n
        part = dw_ref[...]
        for j in range(rb // LANES):
            part = part + gn[:, lane_slice(j)]
        dw_ref[...] = part
        w1 = jnp.broadcast_to(w1_ref[:, :1], h.shape)
        inner = jnp.mean(gn * w1, axis=0, keepdims=True)
        dh_ref[:, cols] = ((g * w1 - n * inner) * inv_rms).astype(BF16)
        return carry

    with jax.named_scope('n_back'):
        lax.fori_loop(0, tokens // rb, norm_back, 0)
    cur_ref = swap[0]
    cur_ref[0] = jnp.zeros_like(cur_ref[0])
    cur_ref[0, 0:1, 0:dim] = jnp.sum(dw_ref[...].T, axis=0, keepdims=True)
    cur_ref[0, 1:2, 0:LANES] = loss_ref[0:1, :]
    for k in range(len(CUBE)):
        start(swap_copies(k, *swap))
        with jax.named_scope('w_swap'):
            swap_sum(k, *swap)
    sum_ref[...] = cur_ref[len(CUBE)]
    for k in range(n_chunks):
        for n, late in enumerate(WHEN[min(k, 2)]):
            if 8 * k + late >= units + row_units:
                gather_step(k, n)

    def sent(q, carry):
        for copy in (*part_copies(q), *tile_copies(q)):
            copy.wait_send()
        return carry

    lax.fori_loop(0, 4 * n_chunks, sent, 0)

    def sent_chunk(k, carry):
        for copy in (*bpart_copies(k), *btile_copies(k)):
            copy.wait_send()
        for letter in LETTERS + LETTERS.upper():
            for copy in hops(k, letter):
                copy.wait_send()
        return carry

    lax.fori_loop(0, n_chunks, sent_chunk, 0)


def backward(inv_count, vocab_off, xb, xt, scale, lab, ht, w1, loss, et, tb=512, rb=256, wide=8):
    slabs, group_tokens, _ = xb.shape
    dim = xt.shape[1]
    vocab = et.shape[1]
    tokens = group_tokens // SIZES['x']
    cube = tuple(SIZES[axis] for axis in AXES[:3])
    n_chunks = vocab // (LANES * cube[0] * cube[1] * cube[2])
    tb, rb = min(tb, group_tokens // 4), min(rb, tokens)
    part = dim - halved(dim)
    q = RING * n_chunks
    tile = (dim, LANES)
    held = (slabs * LANES, LANES)

    def vmem(dtype, *shape):
        return pltpu.VMEM(shape, dtype)

    return pl.pallas_call(
        lambda *refs: main_body(n_chunks, tb, rb, *refs),
        in_specs=[SMEM, SMEM] + [VMEM] * 7 + [HBM],
        out_specs=[HBM, VMEM, VMEM],
        out_shape=[f32(n_chunks, *cube, *tile), bf16(dim, tokens), f32(SUB, slabs * LANES)],
        scratch_shapes=[
            vmem(F32, dim, tokens), vmem(F32, dim, tokens), vmem(F32, *tile),
            vmem(BF16, 2, 2, *held), vmem(BF16, 2, wide, *held),
            vmem(BF16, 2, tb, LANES), vmem(BF16, 2, tb, LANES), vmem(BF16, rb, wide * LANES),
            vmem(F32, n_chunks, *tile), vmem(F32, q, RING, *tile),
            vmem(F32, q, 2, part, LANES), vmem(F32, q, 2, *tile),
            vmem(F32, n_chunks, 2, part, LANES), vmem(F32, n_chunks, 2, *tile),
            SEM((2, 2)), SEM((2, wide)), SEM((2,)), SEM((n_chunks,)),
            *[SEM((q, 2))] * 4,
            *[SEM((n_chunks, 2))] * 4,
            *[SEM((n_chunks, len(GATHERS), len(LETTERS), 2, 2))] * 2,
            *swap_scratch(slabs * LANES),
        ],
        compiler_params=meeting(2),
        cost_estimate=cost(8 * xt.size * vocab, 4 * et.size),
        name="backward",
    )(inv_count, vocab_off, xb, xt, scale, lab, ht, w1, loss, et)


def place_body(rows, deep, src_ref, out_ref, buf, in_sem, out_sem):
    n_chunks, n_dev, dim, _ = src_ref.shape
    per = dim // rows
    pieces = n_chunks * per

    def source(i):
        return src_ref.at[i // per, :, pl.ds(lax.rem(i, per) * rows, rows)]

    def read(i):
        slot = lax.rem(i, deep)
        return pltpu.make_async_copy(source(i), buf.at[slot], in_sem.at[slot])

    def written(i):
        slot = lax.rem(i, deep)
        return pltpu.make_async_copy(buf.at[slot], source(i), out_sem.at[slot])

    def piece(i, carry):
        @pl.when(i < pieces)
        def _():
            @pl.when(i >= deep)
            def _():
                written(i - deep).wait()

            read(i).start()

        j = i - deep // 2

        @pl.when(j >= 0)
        def _():
            read(j).wait()
            slot = lax.rem(j, deep)
            at = pl.ds(pl.multiple_of(lax.rem(j, per) * rows, rows), rows)
            for k in range(n_dev):
                cols = pl.ds(pl.multiple_of(((j // per) * n_dev + k) * LANES, LANES), LANES)
                pltpu.make_async_copy(buf.at[slot, k], out_ref.at[at, cols],
                                      out_sem.at[slot]).start()
        return carry

    lax.fori_loop(0, pieces + deep // 2, piece, 0)
    lax.fori_loop(max(pieces - deep, 0), pieces, lambda i, c: (written(i).wait(), c)[1], 0)


def place(gathered, rows=48, deep=12):
    n_chunks, n_dev, dim, _ = gathered.shape
    return pl.pallas_call(
        lambda *refs: place_body(rows, deep, *refs),
        in_specs=[HBM],
        out_specs=HBM,
        out_shape=f32(dim, n_chunks * n_dev * LANES),
        scratch_shapes=[pltpu.VMEM((deep, n_dev, rows, LANES), F32), SEM((deep,)), SEM((deep,))],
        compiler_params=params(),
        cost_estimate=cost(gathered.size, 8 * gathered.size),
        name="place",
    )(gathered)


def solution(mesh):
    grid_mesh = Mesh(mesh.devices.reshape(RING, RING, RING, 2), AXES)
    dp = AXES[:3]

    def local_step(hidden, norm_w, embed_table, labels, loss_mask):
        batch_rows, seq_len, dim = hidden.shape
        vocab = embed_table.shape[0]
        tokens = batch_rows * seq_len
        et = embed_table.T
        ht = hidden.reshape(tokens, dim).T
        w1 = jnp.broadcast_to((1.0 + norm_w.astype(F32))[:, None], (dim, LANES))
        mask_row = loss_mask.reshape(1, tokens)
        lab_row = labels.reshape(1, tokens)
        core = lax.axis_index('core')

        xt_own, xb_own = norm_rows(ht, w1)
        lab_rep = jnp.broadcast_to((lab_row.reshape(tokens) - core * vocab)[:, None], (tokens, LANES))
        lab_live = jnp.where(mask_row > 0, lab_row, FAR).astype(F32)
        xg, stat, count = forward(
            xb_own, lab_rep, mask_row.reshape(SUB, tokens // SUB).astype(F32), lab_live, et, xt_own)
        inv_count = (1.0 / jnp.maximum(count[0, 0], 1.0)).reshape(1)
        vocab_off = (core * vocab).astype(jnp.int32).reshape(1)
        xb, xt, scale, lab, loss_tile = prep(inv_count, xt_own, xg, stat)

        gathered, dht, sums = backward(
            inv_count, vocab_off, xb, xt, scale, lab, ht, w1, loss_tile, et)
        table = place(gathered.reshape(-1, RING ** 3, dim, LANES))
        return (sums[1, 0] * inv_count[0], dht.T.reshape(batch_rows, seq_len, dim),
                sums[0, :dim], table.T)

    return jax.shard_map(
        local_step, mesh=grid_mesh,
        in_specs=(P(dp, None, None), P(None), P('core', None), P(dp, None), P(dp, None)),
        out_specs=(P(), P(dp, None, None), P(None), P('core', None)), check_vma=False)
```

```python
import jax
import jax.numpy as jnp
from jax import lax
from jax.experimental import pallas as pl
from jax.experimental.pallas import tpu as pltpu
from jax.sharding import Mesh, PartitionSpec as P

SOFT_CAP = 30.0
INV_CAP = 1.0 / SOFT_CAP
CAP_LOG2E = SOFT_CAP * 1.4426950408889634
LANES = 128
SUB = 8
RING = 4
WAYS = (1, RING - 1)
PAIR = range(2)
VMEM_LIMIT = 60 * 1024 * 1024
F32 = jnp.float32
BF16 = jnp.bfloat16
FAR = -(2 ** 22)
MESH_ID = pl.DeviceIdType.MESH
AXES = ('z', 'y', 'x', 'core')
CUBE = ('x', 'y', 'z')
SIZES = {'z': RING, 'y': RING, 'x': RING, 'core': 2}
SEM = pltpu.SemaphoreType.DMA
HBM = pl.BlockSpec(memory_space=pl.ANY)
SMEM = pl.BlockSpec(memory_space=pltpu.SMEM)
VMEM = pl.BlockSpec(memory_space=pltpu.VMEM)


def dot_f32(a, b, dims):
    return lax.dot_general(a, b, (dims, ((), ())), preferred_element_type=F32)


def f32(*shape):
    return jax.ShapeDtypeStruct(shape, F32)


def bf16(*shape):
    return jax.ShapeDtypeStruct(shape, BF16)


def block(axis, *shape):
    return pl.BlockSpec(shape, lambda i: tuple(i if n == axis else 0 for n in range(len(shape))))


def cost(flops, moved, exps=0):
    return pl.CostEstimate(flops=flops, bytes_accessed=moved, transcendentals=exps)


def params(**kw):
    return pltpu.CompilerParams(vmem_limit_bytes=VMEM_LIMIT, **kw)


def meeting(ident):
    return params(collective_id=ident, has_side_effects=True)


def lane_slice(j):
    return slice(j * LANES, (j + 1) * LANES)


def in_lanes(row):
    return jnp.broadcast_to(row, (LANES, LANES)).T


def halved(n):
    return n // (2 * SUB) * SUB


def peer(**shift):
    place = []
    for axis in AXES:
        here = lax.axis_index(axis)
        if axis in shift:
            here = lax.rem(here + shift[axis], SIZES[axis])
        place.append(here)
    return tuple(place)


def send(src, dst, send_sem, recv_sem, where):
    return pltpu.make_async_remote_copy(
        src, dst, send_sem, recv_sem, device_id=where, device_id_type=MESH_ID)


def start(copies):
    for copy in copies:
        copy.start()


def finish(copies):
    for copy in copies:
        copy.wait()


def arrive(copies):
    for copy in copies:
        copy.wait_recv()


def meet(peers):
    barrier = pltpu.get_barrier_semaphore()
    for where in peers:
        pl.semaphore_signal(barrier, inc=1, device_id=where, device_id_type=MESH_ID)
    pl.semaphore_wait(barrier, len(peers))


def others(axis):
    return [peer(**{axis: r}) for r in range(1, SIZES[axis])]


def swap_copies(k, cur_ref, slot_ref, sends, recvs):
    axis = CUBE[k]
    return [send(cur_ref.at[k], slot_ref.at[k, lax.axis_index(axis)], sends.at[k, n],
                 recvs.at[k, n], where) for n, where in enumerate(others(axis))]


def swap_sum(k, cur_ref, slot_ref, sends, recvs):
    finish(swap_copies(k, cur_ref, slot_ref, sends, recvs))
    axis = CUBE[k]
    slot_ref[k, lax.axis_index(axis)] = cur_ref[k]
    total = slot_ref[k, 0]
    for i in range(1, SIZES[axis]):
        total = total + slot_ref[k, i]
    cur_ref[k + 1] = total


def swap_scratch(width):
    n = len(CUBE)
    return [pltpu.VMEM((n + 1, SUB, width), F32), pltpu.VMEM((n, RING, SUB, width), F32),
            SEM((n, n)), SEM((n, n))]


def norm_body(ht_ref, w1_ref, xt_ref, xb_ref):
    h = ht_ref[...].astype(F32)
    inv_rms = lax.rsqrt(jnp.mean(h * h, axis=0, keepdims=True) + 1e-6)
    xt = h * inv_rms * jnp.broadcast_to(w1_ref[:, :1], h.shape)
    xt_ref[0] = xt
    xb_ref[...] = xt.T.astype(BF16)


def norm_rows(ht, w1):
    dim, tokens = ht.shape
    tb = tokens // 2
    return pl.pallas_call(
        norm_body,
        grid=(2,),
        in_specs=[block(1, dim, tb), block(None, dim, LANES)],
        out_specs=[block(0, 1, dim, tb), block(0, tb, dim)],
        out_shape=[f32(2, dim, tb), bf16(tokens, dim)],
        compiler_params=params(),
        cost_estimate=cost(10 * ht.size, 8 * ht.size),
        name="norm",
    )(ht, w1)


GAP = 2


def fwd_body(tb, early, late, x_ref, row_ref, mask_ref, e_ref, xt_ref,
             xg_ref, stat_ref, count_ref, z_ref, p_ref, lab_ref, pay_ref, ring_sem, half_sem, die_sem,
             stat_sem, own_sem, *swap):
    step = pl.program_id(0)
    tokens = x_ref.shape[0]
    dim, bv = e_ref.shape
    cut = halved(dim)
    spans = (pl.ds(0, cut), pl.ds(cut, dim - cut))
    core = lax.axis_index('core')
    across = peer(core=1)
    group = [peer(x=r, core=c) for r in range(1, RING) for c in PAIR]
    ring = [send(xt_ref.at[core], xg_ref.at[2 * w, core], ring_sem.at[0, w], ring_sem.at[1, w],
                 peer(x=WAYS[w])) for w in PAIR]
    on = [send(xg_ref.at[2 * w, core, spans[w]], xg_ref.at[1, core, spans[w]],
               half_sem.at[0, w], half_sem.at[1, w], peer(x=WAYS[w])) for w in PAIR]
    over = [send(xg_ref.at[r, core], xg_ref.at[r, core], die_sem.at[0, r], die_sem.at[1, r],
                 across) for r in range(RING - 1)]

    @pl.when(step == 0)
    def _():
        cur_ref = swap[0]
        cur_ref[0] = jnp.full(cur_ref.shape[1:], jnp.sum(mask_ref[...].astype(F32)), F32)
        with jax.named_scope('f_meet'):
            meet(others('y') + others('z') + group + [across])

    @pl.when(step == 0)
    def _():
        z_ref[...] = jnp.zeros_like(z_ref)
        p_ref[...] = jnp.zeros_like(p_ref)
        local = (row_ref[...] - core * (bv * pl.num_programs(0))).astype(F32)
        for k in range(tokens // LANES):
            lab_ref[lane_slice(k), :] = in_lanes(local[:, lane_slice(k)]).astype(jnp.int32)

    for k in range(len(CUBE) + 1):
        @pl.when(step == k * GAP)
        def _(k=k):
            if k:
                swap_sum(k - 1, *swap)
            if k < len(CUBE):
                start(swap_copies(k, *swap))
            else:
                count_ref[...] = swap[0][k]
            if not k:
                start(ring)

    @pl.when(step == early)
    def _():
        with jax.named_scope('f_ring'):
            finish(ring)
        start(on)
        start(over[::2])

    @pl.when(step == late)
    def _():
        with jax.named_scope('f_on'):
            finish(on)
        over[1].start()

    lane = lax.broadcasted_iota(jnp.int32, (tb, LANES), 1)

    def rows_part(i, carry):
        rows = pl.ds(pl.multiple_of(i * tb, tb), tb)
        z = dot_f32(x_ref[rows, :], e_ref[...], ((1,), (0,)))
        lab = lab_ref[rows, :] - step * bv
        zsum = z_ref[rows, :]
        psum = p_ref[rows, :]
        for j in range(bv // LANES):
            t = jnp.tanh(z[:, lane_slice(j)] * INV_CAP)
            zsum = zsum + jnp.exp2(t * CAP_LOG2E)
            psum = jnp.where(lab == lane + j * LANES, t, psum)
        z_ref[rows, :] = zsum
        p_ref[rows, :] = psum
        return carry

    lax.fori_loop(0, tokens // tb, rows_part, 0, unroll=True)

    @pl.when(step == pl.num_programs(0) - 1)
    def _():
        pay_ref[...] = jnp.concatenate(
            [jnp.sum(z_ref[...].T, axis=0, keepdims=True),
             jnp.sum(p_ref[...].T, axis=0, keepdims=True),
             jnp.where(mask_ref[...] > 0, row_ref[...], FAR).astype(F32)], axis=0)
        own = pltpu.make_async_copy(pay_ref, stat_ref.at[0, core], own_sem)
        own.start()
        copies = [send(pay_ref, stat_ref.at[(n + 1) // 2, core], stat_sem.at[0, n],
                       stat_sem.at[1, n], where) for n, where in enumerate([across] + group)]
        start(copies)
        with jax.named_scope('f_end'):
            finish(over)
            own.wait()
            finish(copies)


def forward(x, lab_row, mask_row, et, xt, bv=1024, tb=256):
    tokens, dim = x.shape
    vocab = et.shape[1]
    tb = min(tb, tokens)
    steps = vocab // bv
    after = len(CUBE) * GAP + 1
    early, late = max(after, steps * 9 // 16), max(after + 1, steps * 5 // 6)
    per_lane = pltpu.VMEM((tokens, LANES), F32)
    return pl.pallas_call(
        lambda *refs: fwd_body(tb, early, late, *refs),
        grid=(steps,),
        in_specs=[block(None, tokens, dim), block(None, 1, tokens), block(None, 1, tokens),
                  block(1, dim, bv), HBM],
        out_specs=[HBM, HBM, block(None, SUB, LANES)],
        out_shape=[f32(RING - 1, 2, dim, tokens // 2), f32(RING, 2, 3, tokens), f32(SUB, LANES)],
        scratch_shapes=[
            per_lane, per_lane, pltpu.VMEM((tokens, LANES), jnp.int32),
            pltpu.VMEM((3, tokens), F32),
            SEM((2, 2)), SEM((2, 2)), SEM((2, RING)), SEM((2, SUB)), SEM, *swap_scratch(LANES)],
        compiler_params=meeting(1),
        cost_estimate=cost(2 * x.size * vocab, 2 * et.size, 2 * tokens * vocab),
        name="fwd",
    )(x, lab_row, mask_row, et, xt)


def grad_tile(z, scale, lab, vid, inv_count):
    t = jnp.tanh(z * INV_CAP)
    p = jnp.exp2(t * CAP_LOG2E) * scale
    p = jnp.where(lab == vid, p - inv_count, p)
    return (p * (1.0 - t * t)).astype(BF16)


GATHERS = ('xyz', 'yzx', 'zxy')
STEPS = (' a', 'a A', 'A bc', 'b Bdf', 'Bc eC', 'df DF', 'e E', 'CDFE ')
LETTERS = 'abcdef'
ADD_LAG = (1, 3, 3)
TILE_LAG = (2, 3, 3)
WHEN = ((9, 10, 12, 15, 18, 20, 22, 25), (12, 14, 15, 18, 21, 25, 26, 35),
        (12, 17, 20, 23, 26, 27, 29, 37))


def main_body(n_chunks, tb, rb, cnt_ref, stat_ref, ht_ref, w1_ref, own_ref, xg_ref, et_ref,
              ag_ref, dh_ref, sum_ref,
              xb_ref, xt_ref, scale_ref, lab_ref, pbuf,
              gx_ref, gin_ref, dw_ref, ebuf, rbuf, ga_ref, gb_ref, gc_ref, gd_ref, shard, tiles,
              part_in, tile_in, bpart_in, btile_in, psem,
              esem, fsem, gsem, own_sem, psend, precv, tsend, trecv,
              bpsend, bprecv, btsend, btrecv, agsend, agrecv, *swap):
    slabs, group_tokens, _ = xb_ref.shape
    dim, tokens = gx_ref.shape
    deep = slabs * LANES
    wide = rbuf.shape[1]
    blocks = group_tokens // tb
    row_blocks = tokens // rb
    cut = halved(dim)
    rest = dim - cut
    units = 8 * n_chunks
    row_units = et_ref.shape[1] // (wide * LANES)
    inv_count = 1.0 / jnp.maximum(cnt_ref[0:1, :], 1.0)
    vocab_off = lax.axis_index('core') * et_ref.shape[1]
    me = {axis: lax.axis_index(axis) for axis in AXES}
    lane = lax.broadcasted_iota(jnp.int32, (tb, LANES), 1)
    side = 11 * dim // 36 // SUB * SUB
    ranges = ((0, side), (side, dim - 2 * side), (dim - side, side))

    def shifted(q, da, db):
        odd = lax.rem(q // 4, 2)
        return peer(z=db + odd * (da - db), y=da + odd * (db - da))

    def tile_index(u, j):
        k = u // 8
        odd = lax.rem(k, 2)
        s = lax.rem(u, 8) // 2
        half = lax.rem(u, 2)
        db = lax.rem(2 + 3 * s + 3 * (s * (s - 1) // 2), RING)
        da = 2 + half - j * (1 + 2 * half)
        dz, dy = db + odd * (da - db), da + odd * (db - da)
        return ((k * RING + lax.rem(me['z'] + dz, RING)) * RING
                + lax.rem(me['y'] + dy, RING)) * SIZES['x'] + me['x']

    def fetch(u, j):
        cols = pl.ds(pl.multiple_of(tile_index(u, j) * LANES, LANES), LANES)
        slot = lax.rem(u, 2)
        return pltpu.make_async_copy(
            et_ref.at[:, cols], ebuf.at[slot, j, pl.ds(0, dim)], esem.at[slot, j])

    def fetch_wide(v, j):
        cols = pl.ds(pl.multiple_of((v * wide + j) * LANES, LANES), LANES)
        slot = lax.rem(v, 2)
        return pltpu.make_async_copy(
            et_ref.at[:, cols], rbuf.at[slot, j, pl.ds(0, dim)], fsem.at[slot, j])

    def parts(src, dst, sends, recvs, q, da, db):
        return (send(src.at[pl.ds(0, cut)], dst.at[0, pl.ds(0, cut)], sends.at[0], recvs.at[0],
                     shifted(q, da, db)),
                send(src.at[pl.ds(cut, rest)], dst.at[1, pl.ds(0, rest)], sends.at[1],
                     recvs.at[1], shifted(q, 3 * da, 3 * db)))

    def part_copies(q):
        return parts(tiles.at[q, 0], part_in.at[q], psend.at[q], precv.at[q], q, 1, 0)

    def bpart_copies(k):
        return parts(tiles.at[4 * k, 3], bpart_in.at[k], bpsend.at[k], bprecv.at[k], 4 * k, 0, 1)

    def tile_copies(q):
        return [send(tiles.at[q, 1 + w], tile_in.at[q, w], tsend.at[q, w], trecv.at[q, w],
                     shifted(q, WAYS[w], 0)) for w in PAIR]

    def btile_copies(k):
        return [send(tiles.at[4 * k + 1 + w, 3], btile_in.at[k, w], btsend.at[k, w],
                     btrecv.at[k, w], shifted(4 * k, 0, WAYS[w])) for w in PAIR]

    def add_parts(first, second, got):
        first[0:cut, :] += got[0, 0:cut, :]
        second[cut:dim, :] += got[1, 0:rest, :]

    def close_slab(q):
        with jax.named_scope('w_tile'):
            arrive(tile_copies(q))
        tiles[q, 3] = tiles[q, 3] + (tile_in[q, 0] + tile_in[q, 1])

    def close_chunk(k):
        close_slab(4 * k + 3)
        with jax.named_scope('w_btile'):
            arrive(btile_copies(k))
        shard[k] = tiles[4 * k + 3, 3] + (btile_in[k, 0] + btile_in[k, 1])

    def own_copy(k):
        return pltpu.make_async_copy(
            shard.at[k], ag_ref.at[k, me['z'], me['y'], me['x']], own_sem.at[k])

    def hops(k, letter):
        block = LETTERS.index(letter.lower())
        passed = int(letter.isupper())
        out = []
        for p, order in enumerate(GATHERS):
            phase = min(block, 2)
            axis = order[phase]
            if SIZES[axis] == 1 or (phase == 2 and block - 2 >= SIZES[order[1]]):
                continue
            for w in PAIR:
                at = dict(me)
                for done in order[:phase]:
                    at[done] = pl.ds(0, SIZES[done])
                if phase == 2:
                    at[order[1]] = lax.rem(me[order[1]] + block - 2, SIZES[order[1]])
                low, high = ranges[p]
                if passed:
                    at[axis] = lax.rem(me[axis] + RING - WAYS[w], RING)
                    mid = halved(high)
                    low, high = (low + mid, high - mid) if w else (low, mid)
                there = ag_ref.at[k, at['z'], at['y'], at['x'], pl.ds(low, high)]
                here = there if block + passed else shard.at[k, pl.ds(low, high)]
                sems = (k, p, block, passed, w)
                out.append(send(here, there, agsend.at[sems], agrecv.at[sems],
                                peer(**{axis: WAYS[w]})))
        return out

    def gather_step(k, n):
        waits, starts = STEPS[n].split(' ')
        for letter in waits:
            with jax.named_scope(f'w_g{n}{letter}'):
                arrive(hops(k, letter))
        if n == 0:
            own_copy(k).start()
        if n == 2:
            own_copy(k).wait()
        for letter in starts:
            start(hops(k, letter))

    def ticks(u, low, high):
        def every_other(first, count):
            def run(act):
                if first < high and first + 2 * count > low:
                    @pl.when((u >= first) & (u < first + 2 * count) & (lax.rem(u + first, 2) == 0))
                    def _():
                        act((u - first) // 2)
            return run

        for k in range(n_chunks):
            added = 8 * k + ADD_LAG[min(k, 2)]
            closed = added + TILE_LAG[min(k, 2)]

            @every_other(added, RING)
            def _(s, k=k):
                q = 4 * k + s
                with jax.named_scope('w_part'):
                    arrive(part_copies(q))
                add_parts(tiles.at[q, 1], tiles.at[q, 2], part_in.at[q])
                start(tile_copies(q))

            @every_other(closed, RING - 1)
            def _(s, k=k):
                close_slab(4 * k + s)

                @pl.when(s == 0)
                def _():
                    start(bpart_copies(k))

                @pl.when(s == 2)
                def _():
                    with jax.named_scope('w_bpart'):
                        arrive(bpart_copies(k))
                    add_parts(tiles.at[4 * k + 1, 3], tiles.at[4 * k + 2, 3], bpart_in.at[k])
                    start(btile_copies(k))

            @every_other(closed + 2 * RING - 2, 1)
            def _(s, k=k):
                close_chunk(k)

        for k in range(n_chunks):
            for n, late in enumerate(WHEN[min(k, 2)]):
                due = 8 * k + late
                if low <= due < high:
                    @pl.when(u == due)
                    def _(k=k, n=n):
                        gather_step(k, n)

    if deep > dim:
        zeros = jnp.zeros((deep - dim, LANES), BF16)
        for slot in PAIR:
            for j in PAIR:
                ebuf[slot, j, dim:, :] = zeros
            for j in range(wide):
                rbuf[slot, j, dim:, :] = zeros
    start([fetch(0, j) for j in PAIR])

    half = tokens // 2
    pieces = 2 * group_tokens // tokens
    whole, tail = divmod(dim, LANES)

    def bring(i, ref):
        return pltpu.make_async_copy(ref, pbuf.at[lax.rem(i, 2)], psem.at[lax.rem(i, 2)])

    def bring_far(i):
        return bring(i, xg_ref.at[i // 2 - 1, lax.rem(i, 2)])

    def label_rows(r, cols):
        return (stat_ref[r, 0, 0:1, cols] + stat_ref[r, 1, 0:1, cols], stat_ref[r, 0, 2:3, cols])

    start([bring(i, own_ref.at[i]) for i in PAIR])
    meet([where for axis in AXES for where in others(axis)])

    def piece(i, carry):
        bring(i, own_ref.at[0]).wait()
        v = pbuf[lax.rem(i, 2)].astype(BF16)
        vt = v.T
        rows = pl.ds(pl.multiple_of(i * half, half), half)
        for k in range(whole):
            xb_ref[k, rows, :] = vt[:, lane_slice(k)]
        if tail:
            xb_ref[whole, rows, :] = jnp.concatenate(
                [vt[:, dim - tail:], jnp.zeros((half, LANES - tail), BF16)], axis=1)
        for k in range(half // LANES):
            xt_ref[i * (half // LANES) + k] = v[:, lane_slice(k)]

        @pl.when(i + 2 < pieces)
        def _():
            bring_far(i + 2).start()

        row_sum, label = label_rows(
            i // 2, pl.ds(pl.multiple_of(lax.rem(i, 2) * half, half), half))
        scale = jnp.where(label >= 0.0, 1.0, 0.0) / row_sum
        for k in range(half // LANES):
            at = pl.ds(pl.multiple_of(i * half + k * LANES, LANES), LANES)
            scale_ref[at, :] = in_lanes(scale[:, lane_slice(k)]) * inv_count
            lab_ref[at, :] = in_lanes(label[:, lane_slice(k)]).astype(jnp.int32)
        return carry

    with jax.named_scope('prep'):
        lax.fori_loop(0, pieces, piece, 0)
    row_sum, label = label_rows(0, slice(None))
    picked = (stat_ref[0, 0, 1:2, :] + stat_ref[0, 1, 1:2, :]) * SOFT_CAP
    loss_part = jnp.sum(jnp.where(label >= 0.0, jnp.log(row_sum) - picked, 0.0))

    def table_product(i, g_ref, half, store):
        n = tb // LANES
        x = jnp.concatenate([xt_ref[i * n + m] for m in range(n)], axis=1)
        g = jnp.concatenate([g_ref[0], g_ref[1]], axis=1)
        part = dot_f32(x, g, ((1,), (0,)))
        for j in PAIR:
            store(2 * half + j, part[:, lane_slice(j)])

    def close_unit(u):
        before = lax.rem(u + units, units)
        q = before // 2

        def add(t, part):
            tiles[q, t] += part

        table_product(blocks - 1, gb_ref, lax.rem(before, 2), add)

        @pl.when((u >= 0) & (lax.rem(before, 2) == 0))
        def _():
            start(part_copies(q))

        ticks(u, 0, units)

    def table_unit(u, carry):
        slot = lax.rem(u, 2)
        q = u // 2
        half = slot
        for j in PAIR:
            fetch(u, j).wait()

        @pl.when(u + 1 < units)
        def _():
            start([fetch(u + 1, j) for j in PAIR])

        bases = [tile_index(u, j) * LANES + vocab_off for j in PAIR]

        def grads(i, g_ref):
            rows = pl.ds(pl.multiple_of(i * tb, tb), tb)
            x = jnp.concatenate([xb_ref[n, rows, :] for n in range(slabs)], axis=1)
            e = jnp.concatenate([ebuf[slot, 0], ebuf[slot, 1]], axis=1)
            z = dot_f32(x, e, ((1,), (0,)))
            lab = lab_ref[rows, :]
            scale = scale_ref[rows, :]
            for j in PAIR:
                g_ref[j] = grad_tile(z[:, lane_slice(j)], scale, lab - bases[j], lane,
                                     inv_count)

        def product(i, g_ref, store):
            table_product(i, g_ref, half, store)

        def put(t, part):
            tiles[q, t] = part

        def add(t, part):
            tiles[q, t] += part

        grads(0, ga_ref)
        close_unit(u - 1)
        grads(1, gb_ref)
        product(0, ga_ref, put)

        def both(i, c):
            grads(2 * i, ga_ref)
            product(2 * i - 1, gb_ref, add)
            grads(2 * i + 1, gb_ref)
            product(2 * i, ga_ref, add)
            return c

        with jax.named_scope('t_comp'):
            lax.fori_loop(1, blocks // 2, both, 0)
        return carry

    gb_ref[...] = jnp.zeros_like(gb_ref)
    tiles[RING * n_chunks - 1] = jnp.zeros_like(tiles[0])
    lax.fori_loop(0, units, table_unit, 0)
    close_unit(units - 1)

    row_lane = lax.broadcasted_iota(jnp.int32, (rb, LANES), 1)
    start([fetch_wide(0, j) for j in range(wide)])
    gx_ref[...] = jnp.zeros_like(gx_ref)

    def row_unit(v, carry):
        slot = lax.rem(v, 2)
        for j in range(wide):
            fetch_wide(v, j).wait()

        @pl.when(v + 1 < row_units)
        def _():
            start([fetch_wide(v + 1, j) for j in range(wide)])

        base = v * wide * LANES + vocab_off

        def grads(i, g_ref):
            rows = pl.ds(pl.multiple_of(i * rb, rb), rb)
            x = jnp.concatenate([xb_ref[n, rows, :] for n in range(slabs)], axis=1)
            e = jnp.concatenate([rbuf[slot, j] for j in range(wide)], axis=1)
            z = dot_f32(x, e, ((1,), (0,)))
            lab = lab_ref[rows, :] - base
            scale = scale_ref[rows, :]
            for j in range(wide):
                g_ref[:, lane_slice(j)] = grad_tile(
                    z[:, lane_slice(j)], scale, lab, row_lane + j * LANES, inv_count)

        def product(i, g_ref):
            rows = pl.ds(pl.multiple_of(i * rb, rb), rb)
            e = jnp.concatenate([rbuf[slot, j, 0:dim, :] for j in range(wide)], axis=1)
            gx_ref[:, rows] += dot_f32(e, g_ref[...], ((1,), (1,)))

        grads(0, gc_ref)
        grads(1, gd_ref)
        product(0, gc_ref)

        def both(i, c):
            grads(2 * i, gc_ref)
            product(2 * i - 1, gd_ref)
            grads(2 * i + 1, gd_ref)
            product(2 * i, gc_ref)
            return c

        with jax.named_scope('r_comp'):
            lax.fori_loop(1, row_blocks // 2, both, 0)
        product(row_blocks - 1, gd_ref)
        ticks(v + units, units, units + row_units)
        return carry

    lax.fori_loop(0, row_units, row_unit, 0)

    if SIZES['core'] > 1:
        swap_rows = send(gx_ref, gin_ref, gsem.at[0], gsem.at[1], peer(core=1))
        swap_rows.start()
        with jax.named_scope('w_rows'):
            swap_rows.wait()
    else:
        gin_ref[...] = jnp.zeros_like(gin_ref)
    dw_ref[...] = jnp.zeros_like(dw_ref)

    def norm_back(i, carry):
        cols = pl.ds(pl.multiple_of(i * rb, rb), rb)
        h = ht_ref[:, cols].astype(F32)
        inv_rms = lax.rsqrt(jnp.mean(h * h, axis=0, keepdims=True) + 1e-6)
        n = h * inv_rms
        g = gx_ref[:, cols] + gin_ref[:, cols]
        gn = g * n
        part = dw_ref[...]
        for j in range(rb // LANES):
            part = part + gn[:, lane_slice(j)]
        dw_ref[...] = part
        w1 = jnp.broadcast_to(w1_ref[:, :1], h.shape)
        inner = jnp.mean(gn * w1, axis=0, keepdims=True)
        dh_ref[:, cols] = ((g * w1 - n * inner) * inv_rms).astype(BF16)
        return carry

    with jax.named_scope('n_back'):
        lax.fori_loop(0, tokens // rb, norm_back, 0)
    cur_ref = swap[0]
    cur_ref[0] = jnp.zeros_like(cur_ref[0])
    cur_ref[0, 0:1, 0:dim] = jnp.sum(dw_ref[...].T, axis=0, keepdims=True)
    cur_ref[0, 1:2, 0:LANES] = loss_part * inv_count
    for k in range(len(CUBE)):
        start(swap_copies(k, *swap))
        with jax.named_scope('w_swap'):
            swap_sum(k, *swap)
    sum_ref[...] = cur_ref[len(CUBE)]
    for k in range(n_chunks):
        for n, late in enumerate(WHEN[min(k, 2)]):
            if 8 * k + late >= units + row_units:
                gather_step(k, n)

    def sent(q, carry):
        for copy in (*part_copies(q), *tile_copies(q)):
            copy.wait_send()
        return carry

    lax.fori_loop(0, 4 * n_chunks, sent, 0)

    def sent_chunk(k, carry):
        for copy in (*bpart_copies(k), *btile_copies(k)):
            copy.wait_send()
        for letter in LETTERS + LETTERS.upper():
            for copy in hops(k, letter):
                copy.wait_send()
        return carry

    lax.fori_loop(0, n_chunks, sent_chunk, 0)


def backward(count, stat, ht, w1, xt_own, xg, et, tb=512, rb=256, wide=8):
    dim, tokens = ht.shape
    vocab = et.shape[1]
    slabs = -(-dim // LANES)
    group_tokens = SIZES['x'] * tokens
    cube = tuple(SIZES[axis] for axis in AXES[:3])
    n_chunks = vocab // (LANES * cube[0] * cube[1] * cube[2])
    tb, rb = min(tb, group_tokens // 4), min(rb, tokens // 2)
    part = dim - halved(dim)
    q = RING * n_chunks
    tile = (dim, LANES)
    held = (slabs * LANES, LANES)

    def vmem(dtype, *shape):
        return pltpu.VMEM(shape, dtype)

    return pl.pallas_call(
        lambda *refs: main_body(n_chunks, tb, rb, *refs),
        in_specs=[VMEM] * 4 + [HBM] * 3,
        out_specs=[HBM, VMEM, VMEM],
        out_shape=[f32(n_chunks, *cube, *tile), bf16(dim, tokens), f32(SUB, slabs * LANES)],
        scratch_shapes=[
            vmem(BF16, slabs, group_tokens, LANES), vmem(BF16, group_tokens // LANES, *tile),
            vmem(F32, group_tokens, LANES), vmem(jnp.int32, group_tokens, LANES),
            vmem(F32, 2, dim, tokens // 2),
            vmem(F32, dim, tokens), vmem(F32, dim, tokens), vmem(F32, *tile),
            vmem(BF16, 2, 2, *held), vmem(BF16, 2, wide, *held),
            *[vmem(BF16, 2, tb, LANES)] * 2, *[vmem(BF16, rb, wide * LANES)] * 2,
            vmem(F32, n_chunks, *tile), vmem(F32, q, RING, *tile),
            vmem(F32, q, 2, part, LANES), vmem(F32, q, 2, *tile),
            vmem(F32, n_chunks, 2, part, LANES), vmem(F32, n_chunks, 2, *tile),
            SEM((2,)), SEM((2, 2)), SEM((2, wide)), SEM((2,)), SEM((n_chunks,)),
            *[SEM((q, 2))] * 4,
            *[SEM((n_chunks, 2))] * 4,
            *[SEM((n_chunks, len(GATHERS), len(LETTERS), 2, 2))] * 2,
            *swap_scratch(slabs * LANES),
        ],
        compiler_params=meeting(2),
        cost_estimate=cost(16 * ht.size * vocab, 4 * et.size),
        name="backward",
    )(count, stat, ht, w1, xt_own, xg, et)


def place_body(rows, deep, src_ref, out_ref, buf, in_sem, out_sem):
    n_chunks, n_dev, dim, _ = src_ref.shape
    per = dim // rows
    pieces = n_chunks * per

    def source(i):
        return src_ref.at[i // per, :, pl.ds(lax.rem(i, per) * rows, rows)]

    def read(i):
        slot = lax.rem(i, deep)
        return pltpu.make_async_copy(source(i), buf.at[slot], in_sem.at[slot])

    def written(i):
        slot = lax.rem(i, deep)
        return pltpu.make_async_copy(buf.at[slot], source(i), out_sem.at[slot])

    def piece(i, carry):
        @pl.when(i < pieces)
        def _():
            @pl.when(i >= deep)
            def _():
                written(i - deep).wait()

            read(i).start()

        j = i - deep // 2

        @pl.when(j >= 0)
        def _():
            read(j).wait()
            slot = lax.rem(j, deep)
            at = pl.ds(pl.multiple_of(lax.rem(j, per) * rows, rows), rows)
            for k in range(n_dev):
                cols = pl.ds(pl.multiple_of(((j // per) * n_dev + k) * LANES, LANES), LANES)
                pltpu.make_async_copy(buf.at[slot, k], out_ref.at[at, cols],
                                      out_sem.at[slot]).start()
        return carry

    lax.fori_loop(0, pieces + deep // 2, piece, 0)
    lax.fori_loop(max(pieces - deep, 0), pieces, lambda i, c: (written(i).wait(), c)[1], 0)


def place(gathered, rows=48, deep=12):
    n_chunks, n_dev, dim, _ = gathered.shape
    return pl.pallas_call(
        lambda *refs: place_body(rows, deep, *refs),
        in_specs=[HBM],
        out_specs=HBM,
        out_shape=f32(dim, n_chunks * n_dev * LANES),
        scratch_shapes=[pltpu.VMEM((deep, n_dev, rows, LANES), F32), SEM((deep,)), SEM((deep,))],
        compiler_params=params(),
        cost_estimate=cost(gathered.size, 8 * gathered.size),
        name="place",
    )(gathered)


def solution(mesh):
    grid_mesh = Mesh(mesh.devices.reshape(RING, RING, RING, 2), AXES)
    dp = AXES[:3]

    def local_step(hidden, norm_w, embed_table, labels, loss_mask):
        batch_rows, seq_len, dim = hidden.shape
        vocab = embed_table.shape[0]
        tokens = batch_rows * seq_len
        et = embed_table.T
        ht = hidden.reshape(tokens, dim).T
        w1 = jnp.broadcast_to((1.0 + norm_w.astype(F32))[:, None], (dim, LANES))
        mask_row = loss_mask.reshape(1, tokens)
        lab_row = labels.reshape(1, tokens)
        xt_own, xb_own = norm_rows(ht, w1)
        xg, stat, count = forward(xb_own, lab_row, mask_row, et, xt_own)
        gathered, dht, sums = backward(count, stat, ht, w1, xt_own, xg, et)
        table = place(gathered.reshape(-1, RING ** 3, dim, LANES))
        return (sums[1, 0], dht.T.reshape(batch_rows, seq_len, dim),
                sums[0, :dim], table.T)

    return jax.shard_map(
        local_step, mesh=grid_mesh,
        in_specs=(P(dp, None, None), P(None), P('core', None), P(dp, None), P(dp, None)),
        out_specs=(P(), P(dp, None, None), P(None), P('core', None)), check_vma=False)
```

```python
import jax
import jax.numpy as jnp
from jax import lax
from jax.experimental import pallas as pl
from jax.experimental.pallas import tpu as pltpu
from jax.sharding import Mesh, PartitionSpec as P

SOFT_CAP = 30.0
INV_CAP = 1.0 / SOFT_CAP
CAP_LOG2E = SOFT_CAP * 1.4426950408889634
LANES = 128
SUB = 8
RING = 4
WAYS = (1, RING - 1)
PAIR = range(2)
VMEM_LIMIT = 60 * 1024 * 1024
F32 = jnp.float32
BF16 = jnp.bfloat16
FAR = -(2 ** 22)
MESH_ID = pl.DeviceIdType.MESH
AXES = ('z', 'y', 'x', 'core')
CUBE = ('x', 'y', 'z')
SIZES = {'z': RING, 'y': RING, 'x': RING, 'core': 2}
SEM = pltpu.SemaphoreType.DMA
HBM = pl.BlockSpec(memory_space=pl.ANY)
SMEM = pl.BlockSpec(memory_space=pltpu.SMEM)
VMEM = pl.BlockSpec(memory_space=pltpu.VMEM)


def dot_f32(a, b, dims):
    return lax.dot_general(a, b, (dims, ((), ())), preferred_element_type=F32)


def f32(*shape):
    return jax.ShapeDtypeStruct(shape, F32)


def bf16(*shape):
    return jax.ShapeDtypeStruct(shape, BF16)


def block(axis, *shape):
    return pl.BlockSpec(shape, lambda i: tuple(i if n == axis else 0 for n in range(len(shape))))


def cost(flops, moved, exps=0):
    return pl.CostEstimate(flops=flops, bytes_accessed=moved, transcendentals=exps)


def params(**kw):
    return pltpu.CompilerParams(vmem_limit_bytes=VMEM_LIMIT, **kw)


def meeting(ident):
    return params(collective_id=ident, has_side_effects=True)


def lane_slice(j):
    return slice(j * LANES, (j + 1) * LANES)


def in_lanes(row):
    return jnp.broadcast_to(row, (LANES, LANES)).T


def halved(n):
    return n // (2 * SUB) * SUB


def peer(**shift):
    place = []
    for axis in AXES:
        here = lax.axis_index(axis)
        if axis in shift:
            here = lax.rem(here + shift[axis], SIZES[axis])
        place.append(here)
    return tuple(place)


def send(src, dst, send_sem, recv_sem, where):
    return pltpu.make_async_remote_copy(
        src, dst, send_sem, recv_sem, device_id=where, device_id_type=MESH_ID)


def start(copies):
    for copy in copies:
        copy.start()


def finish(copies):
    for copy in copies:
        copy.wait()


def arrive(copies):
    for copy in copies:
        copy.wait_recv()


def call(peers):
    for where in peers:
        pl.semaphore_signal(pltpu.get_barrier_semaphore(), inc=1, device_id=where,
                            device_id_type=MESH_ID)


def meet(peers):
    pl.semaphore_wait(pltpu.get_barrier_semaphore(), len(peers))


def others(axis):
    return [peer(**{axis: r}) for r in range(1, SIZES[axis])]


def swap_copies(k, cur_ref, slot_ref, sends, recvs):
    axis = CUBE[k]
    return [send(cur_ref.at[k], slot_ref.at[k, lax.axis_index(axis)], sends.at[k, n],
                 recvs.at[k, n], where) for n, where in enumerate(others(axis))]


def swap_sum(k, cur_ref, slot_ref, sends, recvs):
    finish(swap_copies(k, cur_ref, slot_ref, sends, recvs))
    axis = CUBE[k]
    slot_ref[k, lax.axis_index(axis)] = cur_ref[k]
    total = slot_ref[k, 0]
    for i in range(1, SIZES[axis]):
        total = total + slot_ref[k, i]
    cur_ref[k + 1] = total


def swap_scratch(width):
    n = len(CUBE)
    return [pltpu.VMEM((n + 1, SUB, width), F32), pltpu.VMEM((n, RING, SUB, width), F32),
            SEM((n, n)), SEM((n, n))]


def norm_body(ht_ref, w1_ref, xt_ref, xb_ref):
    h = ht_ref[...].astype(F32)
    inv_rms = lax.rsqrt(jnp.mean(h * h, axis=0, keepdims=True) + 1e-6)
    xt = h * inv_rms * jnp.broadcast_to(w1_ref[:, :1], h.shape)
    xt_ref[0] = xt
    xb_ref[...] = xt.T.astype(BF16)


def norm_rows(ht, w1):
    dim, tokens = ht.shape
    tb = tokens // 2
    return pl.pallas_call(
        norm_body,
        grid=(2,),
        in_specs=[block(1, dim, tb), block(None, dim, LANES)],
        out_specs=[block(0, 1, dim, tb), block(0, tb, dim)],
        out_shape=[f32(2, dim, tb), bf16(tokens, dim)],
        compiler_params=params(),
        cost_estimate=cost(10 * ht.size, 8 * ht.size),
        name="norm",
    )(ht, w1)


GAP = 2


def fwd_body(tb, early, late, x_ref, row_ref, mask_ref, e_ref, xt_ref,
             xg_ref, stat_ref, count_ref, z_ref, p_ref, lab_ref, pay_ref, ring_sem, half_sem, die_sem,
             stat_sem, own_sem, *swap):
    step = pl.program_id(0)
    tokens = x_ref.shape[0]
    dim, bv = e_ref.shape
    cut = halved(dim)
    spans = (pl.ds(0, cut), pl.ds(cut, dim - cut))
    core = lax.axis_index('core')
    across = peer(core=1)
    group = [peer(x=r, core=c) for r in range(1, RING) for c in PAIR]
    everyone = others('y') + others('z') + group + [across]
    ring = [send(xt_ref.at[core], xg_ref.at[2 * w, core], ring_sem.at[0, w], ring_sem.at[1, w],
                 peer(x=WAYS[w])) for w in PAIR]
    on = [send(xg_ref.at[2 * w, core, spans[w]], xg_ref.at[1, core, spans[w]],
               half_sem.at[0, w], half_sem.at[1, w], peer(x=WAYS[w])) for w in PAIR]
    over = [send(xg_ref.at[r, core], xg_ref.at[r, core], die_sem.at[0, r], die_sem.at[1, r],
                 across) for r in range(RING - 1)]

    @pl.when(step == 0)
    def _():
        cur_ref = swap[0]
        cur_ref[0] = jnp.full(cur_ref.shape[1:], jnp.sum(mask_ref[...].astype(F32)), F32)
        call(everyone)

    @pl.when(step == 0)
    def _():
        z_ref[...] = jnp.zeros_like(z_ref)
        p_ref[...] = jnp.zeros_like(p_ref)
        local = (row_ref[...] - core * (bv * pl.num_programs(0))).astype(F32)
        for k in range(tokens // LANES):
            lab_ref[lane_slice(k), :] = in_lanes(local[:, lane_slice(k)]).astype(jnp.int32)

    for k in range(len(CUBE) + 1):
        @pl.when(step == k * GAP + 1)
        def _(k=k):
            if not k:
                with jax.named_scope('f_meet'):
                    meet(everyone)
            if k:
                swap_sum(k - 1, *swap)
            if k < len(CUBE):
                start(swap_copies(k, *swap))
            else:
                count_ref[...] = swap[0][k]
            if not k:
                start(ring)

    @pl.when(step == early)
    def _():
        with jax.named_scope('f_ring'):
            finish(ring)
        start(on)
        start(over[::2])

    @pl.when(step == late)
    def _():
        with jax.named_scope('f_on'):
            finish(on)
        over[1].start()

    lane = lax.broadcasted_iota(jnp.int32, (tb, LANES), 1)

    def rows_part(i, carry):
        rows = pl.ds(pl.multiple_of(i * tb, tb), tb)
        z = dot_f32(x_ref[rows, :], e_ref[...], ((1,), (0,)))
        lab = lab_ref[rows, :] - step * bv
        zsum = z_ref[rows, :]
        psum = p_ref[rows, :]
        for j in range(bv // LANES):
            t = jnp.tanh(z[:, lane_slice(j)] * INV_CAP)
            zsum = zsum + jnp.exp2(t * CAP_LOG2E)
            psum = jnp.where(lab == lane + j * LANES, t, psum)
        z_ref[rows, :] = zsum
        p_ref[rows, :] = psum
        return carry

    lax.fori_loop(0, tokens // tb, rows_part, 0, unroll=True)

    @pl.when(step == pl.num_programs(0) - 1)
    def _():
        pay_ref[...] = jnp.concatenate(
            [jnp.sum(z_ref[...].T, axis=0, keepdims=True),
             jnp.sum(p_ref[...].T, axis=0, keepdims=True),
             jnp.where(mask_ref[...] > 0, row_ref[...], FAR).astype(F32)], axis=0)
        own = pltpu.make_async_copy(pay_ref, stat_ref.at[0, core], own_sem)
        own.start()
        copies = [send(pay_ref, stat_ref.at[(n + 1) // 2, core], stat_sem.at[0, n],
                       stat_sem.at[1, n], where) for n, where in enumerate([across] + group)]
        start(copies)
        with jax.named_scope('f_end'):
            finish(over)
            own.wait()
            finish(copies)


def forward(x, lab_row, mask_row, et, xt, bv=1024, tb=256):
    tokens, dim = x.shape
    vocab = et.shape[1]
    tb = min(tb, tokens)
    steps = vocab // bv
    after = len(CUBE) * GAP + 2
    early, late = max(after, steps * 5 // 8), max(after + 1, steps * 11 // 12)
    per_lane = pltpu.VMEM((tokens, LANES), F32)
    return pl.pallas_call(
        lambda *refs: fwd_body(tb, early, late, *refs),
        grid=(steps,),
        in_specs=[block(None, tokens, dim), block(None, 1, tokens), block(None, 1, tokens),
                  block(1, dim, bv), HBM],
        out_specs=[HBM, HBM, block(None, SUB, LANES)],
        out_shape=[f32(RING - 1, 2, dim, tokens // 2), f32(RING, 2, 3, tokens), f32(SUB, LANES)],
        scratch_shapes=[
            per_lane, per_lane, pltpu.VMEM((tokens, LANES), jnp.int32),
            pltpu.VMEM((3, tokens), F32),
            SEM((2, 2)), SEM((2, 2)), SEM((2, RING)), SEM((2, SUB)), SEM, *swap_scratch(LANES)],
        compiler_params=meeting(1),
        cost_estimate=cost(2 * x.size * vocab, 2 * et.size, 2 * tokens * vocab),
        name="fwd",
    )(x, lab_row, mask_row, et, xt)


def grad_tile(z, scale, lab, vid, inv_count):
    t = jnp.tanh(z * INV_CAP)
    p = jnp.exp2(t * CAP_LOG2E) * scale
    p = jnp.where(lab == vid, p - inv_count, p)
    return (p * (1.0 - t * t)).astype(BF16)


GATHERS = ('xyz', 'yzx', 'zxy')
STEPS = (' a', 'a A', 'A bc', 'b Bdf', 'Bc eC', 'df DF', 'e E', 'CDFE ')
LETTERS = 'abcdef'
ADD_LAG = (2, 1, 3)
TILE_LAG = (2, 2, 7)
LAST_LAG = (0, 0, 1)
WHEN = ((10, 11, 12, 14, 16, 18, 22, 31), (12, 14, 16, 19, 23, 27, 29, 35),
        (19, 21, 22, 26, 29, 31, 32, 35))
SIDES = (160, 176, 192)


def main_body(n_chunks, tb, rb, cnt_ref, stat_ref, ht_ref, w1_ref, own_ref, xg_ref, et_ref,
              ag_ref, dh_ref, sum_ref,
              xb_ref, xt_ref, scale_ref, lab_ref, pbuf,
              gx_ref, gin_ref, dw_ref, ebuf, rbuf, ga_ref, gb_ref, gc_ref, gd_ref, shard, tiles,
              part_in, tile_in, bpart_in, btile_in, psem,
              esem, fsem, gsem, own_sem, psend, precv, tsend, trecv,
              bpsend, bprecv, btsend, btrecv, agsend, agrecv, *swap):
    slabs, group_tokens, _ = xb_ref.shape
    dim, tokens = gx_ref.shape
    deep = slabs * LANES
    wide = rbuf.shape[1]
    blocks = group_tokens // tb
    row_blocks = tokens // rb
    cut = halved(dim)
    rest = dim - cut
    units = 8 * n_chunks
    row_units = et_ref.shape[1] // (wide * LANES)
    inv_count = 1.0 / jnp.maximum(cnt_ref[0:1, :], 1.0)
    vocab_off = lax.axis_index('core') * et_ref.shape[1]
    me = {axis: lax.axis_index(axis) for axis in AXES}
    lane = lax.broadcasted_iota(jnp.int32, (tb, LANES), 1)

    def shifted(q, da, db):
        odd = lax.rem(q // 4, 2)
        return peer(z=db + odd * (da - db), y=da + odd * (db - da))

    def tile_index(u, j):
        k = u // 8
        odd = lax.rem(k, 2)
        s = lax.rem(u, 8) // 2
        half = lax.rem(u, 2)
        db = lax.rem(2 + 3 * s + 3 * (s * (s - 1) // 2), RING)
        da = 2 + half - j * (1 + 2 * half)
        dz, dy = db + odd * (da - db), da + odd * (db - da)
        return ((k * RING + lax.rem(me['z'] + dz, RING)) * RING
                + lax.rem(me['y'] + dy, RING)) * SIZES['x'] + me['x']

    def fetch(u, j):
        cols = pl.ds(pl.multiple_of(tile_index(u, j) * LANES, LANES), LANES)
        slot = lax.rem(u, 2)
        return pltpu.make_async_copy(
            et_ref.at[:, cols], ebuf.at[slot, j, pl.ds(0, dim)], esem.at[slot, j])

    def fetch_wide(v, j):
        cols = pl.ds(pl.multiple_of((v * wide + j) * LANES, LANES), LANES)
        slot = lax.rem(v, 2)
        return pltpu.make_async_copy(
            et_ref.at[:, cols], rbuf.at[slot, j, pl.ds(0, dim)], fsem.at[slot, j])

    def parts(src, dst, sends, recvs, q, da, db):
        return (send(src.at[pl.ds(0, cut)], dst.at[0, pl.ds(0, cut)], sends.at[0], recvs.at[0],
                     shifted(q, da, db)),
                send(src.at[pl.ds(cut, rest)], dst.at[1, pl.ds(0, rest)], sends.at[1],
                     recvs.at[1], shifted(q, 3 * da, 3 * db)))

    def part_copies(q):
        return parts(tiles.at[q, 0], part_in.at[q], psend.at[q], precv.at[q], q, 1, 0)

    def bpart_copies(k):
        return parts(tiles.at[4 * k, 3], bpart_in.at[k], bpsend.at[k], bprecv.at[k], 4 * k, 0, 1)

    def tile_copies(q):
        return [send(tiles.at[q, 1 + w], tile_in.at[q, w], tsend.at[q, w], trecv.at[q, w],
                     shifted(q, WAYS[w], 0)) for w in PAIR]

    def btile_copies(k):
        return [send(tiles.at[4 * k + 1 + w, 3], btile_in.at[k, w], btsend.at[k, w],
                     btrecv.at[k, w], shifted(4 * k, 0, WAYS[w])) for w in PAIR]

    def add_parts(first, second, got):
        first[0:cut, :] += got[0, 0:cut, :]
        second[cut:dim, :] += got[1, 0:rest, :]

    def close_slab(q):
        with jax.named_scope('w_tile'):
            arrive(tile_copies(q))
        tiles[q, 3] = tiles[q, 3] + (tile_in[q, 0] + tile_in[q, 1])

    def close_chunk(k):
        close_slab(4 * k + 3)
        with jax.named_scope('w_btile'):
            arrive(btile_copies(k))
        shard[k] = tiles[4 * k + 3, 3] + (btile_in[k, 0] + btile_in[k, 1])

    def own_copy(k):
        return pltpu.make_async_copy(
            shard.at[k], ag_ref.at[k, me['z'], me['y'], me['x']], own_sem.at[k])

    def hops(k, letter):
        block = LETTERS.index(letter.lower())
        passed = int(letter.isupper())
        side = SIDES[min(k, 2)] * dim // 576 // SUB * SUB
        ranges = ((0, side), (side, dim - 2 * side), (dim - side, side))
        out = []
        for p, order in enumerate(GATHERS):
            phase = min(block, 2)
            axis = order[phase]
            if SIZES[axis] == 1 or (phase == 2 and block - 2 >= SIZES[order[1]]):
                continue
            for w in PAIR:
                at = dict(me)
                for done in order[:phase]:
                    at[done] = pl.ds(0, SIZES[done])
                if phase == 2:
                    at[order[1]] = lax.rem(me[order[1]] + block - 2, SIZES[order[1]])
                low, high = ranges[p]
                if passed:
                    at[axis] = lax.rem(me[axis] + RING - WAYS[w], RING)
                    mid = halved(high)
                    low, high = (low + mid, high - mid) if w else (low, mid)
                there = ag_ref.at[k, at['z'], at['y'], at['x'], pl.ds(low, high)]
                here = there if block + passed else shard.at[k, pl.ds(low, high)]
                sems = (k, p, block, passed, w)
                out.append(send(here, there, agsend.at[sems], agrecv.at[sems],
                                peer(**{axis: WAYS[w]})))
        return out

    def gather_step(k, n):
        if n == 0:
            close_chunk(k)
        waits, starts = STEPS[n].split(' ')
        for letter in waits:
            with jax.named_scope(f'w_g{n}{letter}'):
                arrive(hops(k, letter))
        if n == 0:
            own_copy(k).start()
        if n == 2:
            own_copy(k).wait()
        for letter in starts:
            start(hops(k, letter))

    def ticks(u, low, high):
        def every_other(first, count):
            def run(act):
                if first < high and first + 2 * count > low + 1:
                    @pl.when((u >= first) & (u < first + 2 * count) & (lax.rem(u + first, 2) == 0))
                    def _():
                        act((u - first) // 2)
            return run

        for k in range(n_chunks):
            added = 8 * k + ADD_LAG[min(k, 2)]
            closed = added + TILE_LAG[min(k, 2)]

            @every_other(added, RING)
            def _(s, k=k):
                q = 4 * k + s
                with jax.named_scope('w_part'):
                    arrive(part_copies(q))
                add_parts(tiles.at[q, 1], tiles.at[q, 2], part_in.at[q])
                start(tile_copies(q))

            @every_other(closed, RING - 1)
            def _(s, k=k):
                close_slab(4 * k + s)

                @pl.when(s == 0)
                def _():
                    start(bpart_copies(k))

            @every_other(closed + RING + LAST_LAG[min(k, 2)], 1)
            def _(s, k=k):
                with jax.named_scope('w_bpart'):
                    arrive(bpart_copies(k))
                add_parts(tiles.at[4 * k + 1, 3], tiles.at[4 * k + 2, 3], bpart_in.at[k])
                start(btile_copies(k))

        for k in range(n_chunks):
            for n, late in enumerate(WHEN[min(k, 2)]):
                due = 8 * k + late
                if low <= due < high:
                    @pl.when(u == due)
                    def _(k=k, n=n):
                        gather_step(k, n)

    if deep > dim:
        zeros = jnp.zeros((deep - dim, LANES), BF16)
        for slot in PAIR:
            for j in PAIR:
                ebuf[slot, j, dim:, :] = zeros
            for j in range(wide):
                rbuf[slot, j, dim:, :] = zeros
    start([fetch(0, j) for j in PAIR])

    half = tokens // 2
    pieces = 2 * group_tokens // tokens
    whole, tail = divmod(dim, LANES)

    def bring(i, ref):
        return pltpu.make_async_copy(ref, pbuf.at[lax.rem(i, 2)], psem.at[lax.rem(i, 2)])

    def bring_far(i):
        return bring(i, xg_ref.at[i // 2 - 1, lax.rem(i, 2)])

    def label_rows(r, cols):
        return (stat_ref[r, 0, 0:1, cols] + stat_ref[r, 1, 0:1, cols], stat_ref[r, 0, 2:3, cols])

    start([bring(i, own_ref.at[i]) for i in PAIR])
    partners = [where for axis in AXES for where in others(axis)]
    call(partners)

    def piece(i, carry):
        bring(i, own_ref.at[0]).wait()
        v = pbuf[lax.rem(i, 2)].astype(BF16)
        vt = v.T
        rows = pl.ds(pl.multiple_of(i * half, half), half)
        for k in range(whole):
            xb_ref[k, rows, :] = vt[:, lane_slice(k)]
        if tail:
            xb_ref[whole, rows, :] = jnp.concatenate(
                [vt[:, dim - tail:], jnp.zeros((half, LANES - tail), BF16)], axis=1)
        for k in range(half // LANES):
            xt_ref[i * (half // LANES) + k] = v[:, lane_slice(k)]

        @pl.when(i + 2 < pieces)
        def _():
            bring_far(i + 2).start()

        row_sum, label = label_rows(
            i // 2, pl.ds(pl.multiple_of(lax.rem(i, 2) * half, half), half))
        scale = jnp.where(label >= 0.0, 1.0, 0.0) / row_sum
        for k in range(half // LANES):
            at = pl.ds(pl.multiple_of(i * half + k * LANES, LANES), LANES)
            scale_ref[at, :] = in_lanes(scale[:, lane_slice(k)]) * inv_count
            lab_ref[at, :] = in_lanes(label[:, lane_slice(k)]).astype(jnp.int32)
        return carry

    with jax.named_scope('prep'):
        lax.fori_loop(0, pieces, piece, 0)
    meet(partners)
    row_sum, label = label_rows(0, slice(None))
    picked = (stat_ref[0, 0, 1:2, :] + stat_ref[0, 1, 1:2, :]) * SOFT_CAP
    loss_part = jnp.sum(jnp.where(label >= 0.0, jnp.log(row_sum) - picked, 0.0))

    def table_product(i, g_ref, half, store):
        n = tb // LANES
        x = jnp.concatenate([xt_ref[i * n + m] for m in range(n)], axis=1)
        g = jnp.concatenate([g_ref[0], g_ref[1]], axis=1)
        part = dot_f32(x, g, ((1,), (0,)))
        for j in PAIR:
            store(2 * half + j, part[:, lane_slice(j)])

    def close_unit(u):
        before = lax.rem(u + units, units)
        q = before // 2

        def add(t, part):
            tiles[q, t] += part

        table_product(blocks - 1, gb_ref, lax.rem(before, 2), add)

        @pl.when((u >= 0) & (lax.rem(before, 2) == 0))
        def _():
            start(part_copies(q))

        ticks(u, 0, units)

    def table_unit(u, carry):
        slot = lax.rem(u, 2)
        q = u // 2
        half = slot
        for j in PAIR:
            fetch(u, j).wait()

        @pl.when(u + 1 < units)
        def _():
            start([fetch(u + 1, j) for j in PAIR])

        bases = [tile_index(u, j) * LANES + vocab_off for j in PAIR]

        def grads(i, g_ref):
            rows = pl.ds(pl.multiple_of(i * tb, tb), tb)
            x = jnp.concatenate([xb_ref[n, rows, :] for n in range(slabs)], axis=1)
            e = jnp.concatenate([ebuf[slot, 0], ebuf[slot, 1]], axis=1)
            z = dot_f32(x, e, ((1,), (0,)))
            lab = lab_ref[rows, :]
            scale = scale_ref[rows, :]
            for j in PAIR:
                g_ref[j] = grad_tile(z[:, lane_slice(j)], scale, lab - bases[j], lane,
                                     inv_count)

        def product(i, g_ref, store):
            table_product(i, g_ref, half, store)

        def put(t, part):
            tiles[q, t] = part

        def add(t, part):
            tiles[q, t] += part

        grads(0, ga_ref)
        close_unit(u - 1)
        grads(1, gb_ref)
        product(0, ga_ref, put)

        def both(i, c):
            grads(2 * i, ga_ref)
            product(2 * i - 1, gb_ref, add)
            grads(2 * i + 1, gb_ref)
            product(2 * i, ga_ref, add)
            return c

        with jax.named_scope('t_comp'):
            lax.fori_loop(1, blocks // 2, both, 0)
        return carry

    gb_ref[...] = jnp.zeros_like(gb_ref)
    tiles[RING * n_chunks - 1] = jnp.zeros_like(tiles[0])
    lax.fori_loop(0, units, table_unit, 0)
    close_unit(units - 1)

    row_lane = lax.broadcasted_iota(jnp.int32, (rb, LANES), 1)
    start([fetch_wide(0, j) for j in range(wide)])
    gx_ref[...] = jnp.zeros_like(gx_ref)

    def row_unit(v, carry):
        slot = lax.rem(v, 2)
        for j in range(wide):
            fetch_wide(v, j).wait()

        @pl.when(v + 1 < row_units)
        def _():
            start([fetch_wide(v + 1, j) for j in range(wide)])

        base = v * wide * LANES + vocab_off

        def grads(i, g_ref):
            rows = pl.ds(pl.multiple_of(i * rb, rb), rb)
            x = jnp.concatenate([xb_ref[n, rows, :] for n in range(slabs)], axis=1)
            e = jnp.concatenate([rbuf[slot, j] for j in range(wide)], axis=1)
            z = dot_f32(x, e, ((1,), (0,)))
            lab = lab_ref[rows, :] - base
            scale = scale_ref[rows, :]
            for j in range(wide):
                g_ref[:, lane_slice(j)] = grad_tile(
                    z[:, lane_slice(j)], scale, lab, row_lane + j * LANES, inv_count)

        def product(i, g_ref):
            rows = pl.ds(pl.multiple_of(i * rb, rb), rb)
            e = jnp.concatenate([rbuf[slot, j, 0:dim, :] for j in range(wide)], axis=1)
            gx_ref[:, rows] += dot_f32(e, g_ref[...], ((1,), (1,)))

        grads(0, gc_ref)
        grads(1, gd_ref)
        product(0, gc_ref)

        def both(i, c):
            grads(2 * i, gc_ref)
            product(2 * i - 1, gd_ref)
            grads(2 * i + 1, gd_ref)
            product(2 * i, gc_ref)
            return c

        with jax.named_scope('r_comp'):
            lax.fori_loop(1, row_blocks // 2, both, 0)
        product(row_blocks - 1, gd_ref)
        ticks(v + units, units, units + row_units)
        return carry

    lax.fori_loop(0, row_units, row_unit, 0)

    if SIZES['core'] > 1:
        swap_rows = send(gx_ref, gin_ref, gsem.at[0], gsem.at[1], peer(core=1))
        swap_rows.start()
        with jax.named_scope('w_rows'):
            swap_rows.wait()
    else:
        gin_ref[...] = jnp.zeros_like(gin_ref)
    dw_ref[...] = jnp.zeros_like(dw_ref)

    def norm_back(i, carry):
        cols = pl.ds(pl.multiple_of(i * rb, rb), rb)
        h = ht_ref[:, cols].astype(F32)
        inv_rms = lax.rsqrt(jnp.mean(h * h, axis=0, keepdims=True) + 1e-6)
        n = h * inv_rms
        g = gx_ref[:, cols] + gin_ref[:, cols]
        gn = g * n
        part = dw_ref[...]
        for j in range(rb // LANES):
            part = part + gn[:, lane_slice(j)]
        dw_ref[...] = part
        w1 = jnp.broadcast_to(w1_ref[:, :1], h.shape)
        inner = jnp.mean(gn * w1, axis=0, keepdims=True)
        dh_ref[:, cols] = ((g * w1 - n * inner) * inv_rms).astype(BF16)
        return carry

    with jax.named_scope('n_back'):
        lax.fori_loop(0, tokens // rb, norm_back, 0)
    cur_ref = swap[0]
    cur_ref[0] = jnp.zeros_like(cur_ref[0])
    cur_ref[0, 0:1, 0:dim] = jnp.sum(dw_ref[...].T, axis=0, keepdims=True)
    cur_ref[0, 1:2, 0:LANES] = loss_part * inv_count
    for k in range(len(CUBE)):
        start(swap_copies(k, *swap))
        with jax.named_scope('w_swap'):
            swap_sum(k, *swap)
    sum_ref[...] = cur_ref[len(CUBE)]
    for k in range(n_chunks):
        for n, late in enumerate(WHEN[min(k, 2)]):
            if 8 * k + late >= units + row_units:
                gather_step(k, n)

    def sent(q, carry):
        for copy in (*part_copies(q), *tile_copies(q)):
            copy.wait_send()
        return carry

    lax.fori_loop(0, 4 * n_chunks, sent, 0)

    for k in range(n_chunks):
        for copy in (*bpart_copies(k), *btile_copies(k)):
            copy.wait_send()
        for letter in LETTERS + LETTERS.upper():
            for copy in hops(k, letter):
                copy.wait_send()


def backward(count, stat, ht, w1, xt_own, xg, et, tb=1024, rb=512, wide=8):
    dim, tokens = ht.shape
    vocab = et.shape[1]
    slabs = -(-dim // LANES)
    group_tokens = SIZES['x'] * tokens
    cube = tuple(SIZES[axis] for axis in AXES[:3])
    n_chunks = vocab // (LANES * cube[0] * cube[1] * cube[2])
    tb, rb = min(tb, group_tokens // 4), min(rb, tokens // 2)
    part = dim - halved(dim)
    q = RING * n_chunks
    tile = (dim, LANES)
    held = (slabs * LANES, LANES)

    def vmem(dtype, *shape):
        return pltpu.VMEM(shape, dtype)

    return pl.pallas_call(
        lambda *refs: main_body(n_chunks, tb, rb, *refs),
        in_specs=[VMEM] * 4 + [HBM] * 3,
        out_specs=[HBM, VMEM, VMEM],
        out_shape=[f32(n_chunks, *cube, *tile), bf16(dim, tokens), f32(SUB, slabs * LANES)],
        scratch_shapes=[
            vmem(BF16, slabs, group_tokens, LANES), vmem(BF16, group_tokens // LANES, *tile),
            vmem(F32, group_tokens, LANES), vmem(jnp.int32, group_tokens, LANES),
            vmem(F32, 2, dim, tokens // 2),
            vmem(F32, dim, tokens), vmem(F32, dim, tokens), vmem(F32, *tile),
            vmem(BF16, 2, 2, *held), vmem(BF16, 2, wide, *held),
            *[vmem(BF16, 2, tb, LANES)] * 2, *[vmem(BF16, rb, wide * LANES)] * 2,
            vmem(F32, n_chunks, *tile), vmem(F32, q, RING, *tile),
            vmem(F32, q, 2, part, LANES), vmem(F32, q, 2, *tile),
            vmem(F32, n_chunks, 2, part, LANES), vmem(F32, n_chunks, 2, *tile),
            SEM((2,)), SEM((2, 2)), SEM((2, wide)), SEM((2,)), SEM((n_chunks,)),
            *[SEM((q, 2))] * 4,
            *[SEM((n_chunks, 2))] * 4,
            *[SEM((n_chunks, len(GATHERS), len(LETTERS), 2, 2))] * 2,
            *swap_scratch(slabs * LANES),
        ],
        compiler_params=meeting(2),
        cost_estimate=cost(16 * ht.size * vocab, 4 * et.size),
        name="backward",
    )(count, stat, ht, w1, xt_own, xg, et)


def place_body(rows, deep, src_ref, out_ref, buf, in_sem, out_sem):
    n_chunks, n_dev, dim, _ = src_ref.shape
    per = dim // rows
    pieces = n_chunks * per
    wide = n_dev * LANES

    def rows_of(i):
        return pl.ds(pl.multiple_of(lax.rem(i, per) * rows, rows), rows)

    def write(i, sem):
        slot = lax.rem(i, deep)
        cols = pl.ds(pl.multiple_of(i // per * wide, wide), wide)
        return pltpu.make_async_copy(buf.at[slot], out_ref.at[rows_of(i), cols], sem.at[slot])

    def piece(i, carry):
        slot = lax.rem(i, deep)

        @pl.when(i < pieces)
        def _():
            @pl.when(i >= deep)
            def _():
                write(i - deep, out_sem).wait()

            for k in range(n_dev):
                pltpu.make_async_copy(src_ref.at[i // per, k, rows_of(i)],
                                      buf.at[slot, :, lane_slice(k)], in_sem.at[slot]).start()

        j = i - deep // 2

        @pl.when(j >= 0)
        def _():
            write(j, in_sem).wait()
            write(j, out_sem).start()
        return carry

    lax.fori_loop(0, pieces + deep // 2, piece, 0)
    lax.fori_loop(max(pieces - deep, 0), pieces, lambda i, c: (write(i, out_sem).wait(), c)[1], 0)


def place(gathered, rows=48, deep=12):
    n_chunks, n_dev, dim, _ = gathered.shape
    return pl.pallas_call(
        lambda *refs: place_body(rows, deep, *refs),
        in_specs=[HBM],
        out_specs=HBM,
        out_shape=f32(dim, n_chunks * n_dev * LANES),
        scratch_shapes=[pltpu.VMEM((deep, rows, n_dev * LANES), F32), SEM((deep,)), SEM((deep,))],
        compiler_params=params(),
        cost_estimate=cost(gathered.size, 8 * gathered.size),
        name="place",
    )(gathered)


def solution(mesh):
    grid_mesh = Mesh(mesh.devices.reshape(RING, RING, RING, 2), AXES)
    dp = AXES[:3]

    def local_step(hidden, norm_w, embed_table, labels, loss_mask):
        batch_rows, seq_len, dim = hidden.shape
        vocab = embed_table.shape[0]
        tokens = batch_rows * seq_len
        et = embed_table.T
        ht = hidden.reshape(tokens, dim).T
        w1 = jnp.broadcast_to((1.0 + norm_w.astype(F32))[:, None], (dim, LANES))
        mask_row = loss_mask.reshape(1, tokens)
        lab_row = labels.reshape(1, tokens)
        xt_own, xb_own = norm_rows(ht, w1)
        xg, stat, count = forward(xb_own, lab_row, mask_row, et, xt_own)
        gathered, dht, sums = backward(count, stat, ht, w1, xt_own, xg, et)
        table = place(gathered.reshape(-1, RING ** 3, dim, LANES))
        return (sums[1, 0], dht.T.reshape(batch_rows, seq_len, dim),
                sums[0, :dim], table.T)

    return jax.shard_map(
        local_step, mesh=grid_mesh,
        in_specs=(P(dp, None, None), P(None), P('core', None), P(dp, None), P(dp, None)),
        out_specs=(P(), P(dp, None, None), P(None), P('core', None)), check_vma=False)
```

```python
import jax
import jax.numpy as jnp
from jax import lax
from jax.experimental import pallas as pl
from jax.experimental.pallas import tpu as pltpu
from jax.sharding import Mesh, PartitionSpec as P

SOFT_CAP = 30.0
INV_CAP = 1.0 / SOFT_CAP
CAP_LOG2E = SOFT_CAP * 1.4426950408889634
LANES = 128
SUB = 8
RING = 4
WAYS = (1, RING - 1)
PAIR = range(2)
VMEM_LIMIT = 62 * 1024 * 1024
F32 = jnp.float32
BF16 = jnp.bfloat16
FAR = -(2 ** 22)
MESH_ID = pl.DeviceIdType.MESH
AXES = ('z', 'y', 'x', 'core')
CUBE = ('x', 'y', 'z')
SIZES = {'z': RING, 'y': RING, 'x': RING, 'core': 2}
SEM = pltpu.SemaphoreType.DMA
HBM = pl.BlockSpec(memory_space=pl.ANY)
SMEM = pl.BlockSpec(memory_space=pltpu.SMEM)
VMEM = pl.BlockSpec(memory_space=pltpu.VMEM)


def dot_f32(a, b, dims):
    return lax.dot_general(a, b, (dims, ((), ())), preferred_element_type=F32)


def f32(*shape):
    return jax.ShapeDtypeStruct(shape, F32)


def bf16(*shape):
    return jax.ShapeDtypeStruct(shape, BF16)


def block(axis, *shape):
    return pl.BlockSpec(shape, lambda i: tuple(i if n == axis else 0 for n in range(len(shape))))


def cost(flops, moved, exps=0):
    return pl.CostEstimate(flops=flops, bytes_accessed=moved, transcendentals=exps)


def params(**kw):
    return pltpu.CompilerParams(vmem_limit_bytes=VMEM_LIMIT, **kw)


def meeting(ident):
    return params(collective_id=ident, has_side_effects=True)


def lane_slice(j):
    return slice(j * LANES, (j + 1) * LANES)


def in_lanes(row):
    return jnp.broadcast_to(row, (LANES, LANES)).T


def halved(n):
    return n // (2 * SUB) * SUB


def peer(**shift):
    place = []
    for axis in AXES:
        here = lax.axis_index(axis)
        if axis in shift:
            here = lax.rem(here + shift[axis], SIZES[axis])
        place.append(here)
    return tuple(place)


def send(src, dst, send_sem, recv_sem, where):
    return pltpu.make_async_remote_copy(
        src, dst, send_sem, recv_sem, device_id=where, device_id_type=MESH_ID)


def start(copies):
    for copy in copies:
        copy.start()


def finish(copies):
    for copy in copies:
        copy.wait()


def arrive(copies):
    for copy in copies:
        copy.wait_recv()


def call(peers):
    for where in peers:
        pl.semaphore_signal(pltpu.get_barrier_semaphore(), inc=1, device_id=where,
                            device_id_type=MESH_ID)


def meet(peers):
    pl.semaphore_wait(pltpu.get_barrier_semaphore(), len(peers))


def others(axis):
    return [peer(**{axis: r}) for r in range(1, SIZES[axis])]


def swap_copies(order, k, cur_ref, slot_ref, sends, recvs):
    axis = order[k]
    return [send(cur_ref.at[k], slot_ref.at[k, lax.axis_index(axis)], sends.at[k, n],
                 recvs.at[k, n], where) for n, where in enumerate(others(axis))]


def swap_sum(order, k, cur_ref, slot_ref, sends, recvs):
    finish(swap_copies(order, k, cur_ref, slot_ref, sends, recvs))
    axis = order[k]
    slot_ref[k, lax.axis_index(axis)] = cur_ref[k]
    total = slot_ref[k, 0]
    for i in range(1, SIZES[axis]):
        total = total + slot_ref[k, i]
    cur_ref[k + 1] = total


def swap_scratch(width):
    n = len(CUBE)
    return [pltpu.VMEM((n + 1, SUB, width), F32), pltpu.VMEM((n, RING, SUB, width), F32),
            SEM((n, n)), SEM((n, n))]


def norm_body(ht_ref, w1_ref, xt_ref, xb_ref):
    h = ht_ref[...].astype(F32)
    inv_rms = lax.rsqrt(jnp.mean(h * h, axis=0, keepdims=True) + 1e-6)
    xt = h * inv_rms * jnp.broadcast_to(w1_ref[:, :1], h.shape)
    xt_ref[0] = xt
    xb_ref[...] = xt.T.astype(BF16)


def norm_rows(ht, w1):
    dim, tokens = ht.shape
    tb = tokens // 2
    return pl.pallas_call(
        norm_body,
        grid=(2,),
        in_specs=[block(1, dim, tb), block(None, dim, LANES)],
        out_specs=[block(0, 1, dim, tb), block(0, tb, dim)],
        out_shape=[f32(2, dim, tb), bf16(tokens, dim)],
        compiler_params=params(),
        cost_estimate=cost(10 * ht.size, 8 * ht.size),
        name="norm",
    )(ht, w1)


GAP = 2


def fwd_body(tb, early, late, x_ref, row_ref, mask_ref, e_ref, xt_ref,
             xg_ref, stat_ref, count_ref, z_ref, p_ref, lab_ref, pay_ref, ring_sem, half_sem, die_sem,
             stat_sem, own_sem, *swap):
    step = pl.program_id(0)
    tokens = x_ref.shape[0]
    dim, bv = e_ref.shape
    cut = halved(dim)
    spans = (pl.ds(0, cut), pl.ds(cut, dim - cut))
    core = lax.axis_index('core')
    across = peer(core=1)
    group = [peer(x=r, core=c) for r in range(1, RING) for c in PAIR]
    everyone = others('y') + others('z') + group + [across]
    ring = [send(xt_ref.at[core], xg_ref.at[2 * w, core], ring_sem.at[0, w], ring_sem.at[1, w],
                 peer(x=WAYS[w])) for w in PAIR]
    on = [send(xg_ref.at[2 * w, core, spans[w]], xg_ref.at[1, core, spans[w]],
               half_sem.at[0, w], half_sem.at[1, w], peer(x=WAYS[w])) for w in PAIR]
    over = [send(xg_ref.at[r, core], xg_ref.at[r, core], die_sem.at[0, r], die_sem.at[1, r],
                 across) for r in range(RING - 1)]

    @pl.when(step == 0)
    def _():
        cur_ref = swap[0]
        cur_ref[0] = jnp.full(cur_ref.shape[1:], jnp.sum(mask_ref[...].astype(F32)), F32)
        call(everyone)

    @pl.when(step == 0)
    def _():
        z_ref[...] = jnp.zeros_like(z_ref)
        p_ref[...] = jnp.zeros_like(p_ref)
        local = (row_ref[...] - core * (bv * pl.num_programs(0))).astype(F32)
        for k in range(tokens // LANES):
            lab_ref[lane_slice(k), :] = in_lanes(local[:, lane_slice(k)]).astype(jnp.int32)

    for k in range(len(CUBE) + 1):
        @pl.when(step == k * GAP + 1)
        def _(k=k):
            if not k:
                meet(everyone)
            if k:
                swap_sum(CUBE, k - 1, *swap)
            if k < len(CUBE):
                start(swap_copies(CUBE, k, *swap))
            else:
                count_ref[...] = swap[0][k]
            if not k:
                start(ring)

    @pl.when(step == early)
    def _():
        finish(ring)
        start(on)
        start(over[::2])

    @pl.when(step == late)
    def _():
        finish(on)
        over[1].start()

    lane = lax.broadcasted_iota(jnp.int32, (tb, LANES), 1)

    def rows_part(i, carry):
        rows = pl.ds(pl.multiple_of(i * tb, tb), tb)
        z = dot_f32(x_ref[rows, :], e_ref[...], ((1,), (0,)))
        lab = lab_ref[rows, :] - step * bv
        zsum = z_ref[rows, :]
        psum = p_ref[rows, :]
        for j in range(bv // LANES):
            t = jnp.tanh(z[:, lane_slice(j)] * INV_CAP)
            zsum = zsum + jnp.exp2(t * CAP_LOG2E)
            psum = jnp.where(lab == lane + j * LANES, t, psum)
        z_ref[rows, :] = zsum
        p_ref[rows, :] = psum
        return carry

    lax.fori_loop(0, tokens // tb, rows_part, 0, unroll=True)

    @pl.when(step == pl.num_programs(0) - 1)
    def _():
        pay_ref[...] = jnp.concatenate(
            [jnp.sum(z_ref[...].T, axis=0, keepdims=True),
             jnp.sum(p_ref[...].T, axis=0, keepdims=True),
             jnp.where(mask_ref[...] > 0, row_ref[...], FAR).astype(F32)], axis=0)
        own = pltpu.make_async_copy(pay_ref, stat_ref.at[0, core], own_sem)
        own.start()
        copies = [send(pay_ref, stat_ref.at[(n + 1) // 2, core], stat_sem.at[0, n],
                       stat_sem.at[1, n], where) for n, where in enumerate([across] + group)]
        start(copies)
        finish(over)
        own.wait()
        finish(copies)


def forward(x, lab_row, mask_row, et, xt, bv=1024, tb=256):
    tokens, dim = x.shape
    vocab = et.shape[1]
    tb = min(tb, tokens)
    steps = vocab // bv
    after = len(CUBE) * GAP + 2
    early, late = max(after, steps * 5 // 8), max(after + 1, steps * 11 // 12)
    per_lane = pltpu.VMEM((tokens, LANES), F32)
    return pl.pallas_call(
        lambda *refs: fwd_body(tb, early, late, *refs),
        grid=(steps,),
        in_specs=[block(None, tokens, dim), block(None, 1, tokens), block(None, 1, tokens),
                  block(1, dim, bv), HBM],
        out_specs=[HBM, HBM, block(None, SUB, LANES)],
        out_shape=[f32(RING - 1, 2, dim, tokens // 2), f32(RING, 2, 3, tokens), f32(SUB, LANES)],
        scratch_shapes=[
            per_lane, per_lane, pltpu.VMEM((tokens, LANES), jnp.int32),
            pltpu.VMEM((3, tokens), F32),
            SEM((2, 2)), SEM((2, 2)), SEM((2, RING)), SEM((2, SUB)), SEM, *swap_scratch(LANES)],
        compiler_params=meeting(1),
        cost_estimate=cost(2 * x.size * vocab, 2 * et.size, 2 * tokens * vocab),
        name="fwd",
    )(x, lab_row, mask_row, et, xt)


def grad_tile(z, scale, lab, vid, inv_count):
    t = jnp.tanh(z * INV_CAP)
    p = jnp.exp2(t * CAP_LOG2E) * scale
    p = jnp.where(lab == vid, p - inv_count, p)
    return (p * (1.0 - t * t)).astype(BF16)


GATHERS = ('xyz', 'yzx', 'zxy')
STEPS = (' a', 'a A', 'A bc', 'b Bdf', 'Bc eC', 'df DF', 'e E', 'CDFE ')
LETTERS = 'abcdef'
ADD_LAG = (2, 3, 5)
TILE_LAG = (2, 3, 2)
LAST_LAG = (0, 0, 1)
WHEN = ((10, 12, 13, 16, 19, 22, 23, 26), (14, 15, 17, 20, 24, 25, 31, 42),
        (14, 17, 20, 21, 26, 29, 35, 38))
SIDES = (144, 176, 192)


def main_body(n_chunks, tb, rb, cnt_ref, stat_ref, ht_ref, w1_ref, own_ref, xg_ref, et_ref,
              ag_ref, dh_ref, sum_ref,
              xb_ref, xt_ref, scale_ref, lab_ref, pbuf,
              gx_ref, gin_ref, dw_ref, ebuf, rbuf, ga_ref, gb_ref, gc_ref, gd_ref, shard, tiles,
              part_in, tile_in, bpart_in, btile_in, psem,
              esem, fsem, gsem, own_sem, psend, precv, tsend, trecv,
              bpsend, bprecv, btsend, btrecv, agsend, agrecv, *swap):
    slabs, group_tokens, _ = xb_ref.shape
    dim, tokens = gx_ref.shape
    deep = slabs * LANES
    wide = rbuf.shape[1]
    blocks = group_tokens // tb
    row_blocks = tokens // rb
    cut = halved(dim)
    rest = dim - cut
    units = 8 * n_chunks
    row_units = et_ref.shape[1] // (wide * LANES)
    inv_count = 1.0 / jnp.maximum(cnt_ref[0:1, :], 1.0)
    vocab_off = lax.axis_index('core') * et_ref.shape[1]
    me = {axis: lax.axis_index(axis) for axis in AXES}
    lane = lax.broadcasted_iota(jnp.int32, (tb, LANES), 1)

    def shifted(q, da, db):
        odd = lax.rem(q // 4, 2)
        return peer(z=db + odd * (da - db), y=da + odd * (db - da))

    def tile_index(u, j):
        k = u // 8
        odd = lax.rem(k, 2)
        s = lax.rem(u, 8) // 2
        half = lax.rem(u, 2)
        db = lax.rem(2 + 3 * s + 3 * (s * (s - 1) // 2), RING)
        da = 2 + half - j * (1 + 2 * half)
        dz, dy = db + odd * (da - db), da + odd * (db - da)
        return ((k * RING + lax.rem(me['z'] + dz, RING)) * RING
                + lax.rem(me['y'] + dy, RING)) * SIZES['x'] + me['x']

    def fetch(u, j):
        cols = pl.ds(pl.multiple_of(tile_index(u, j) * LANES, LANES), LANES)
        slot = lax.rem(u, 2)
        return pltpu.make_async_copy(
            et_ref.at[:, cols], ebuf.at[slot, j, pl.ds(0, dim)], esem.at[slot, j])

    def fetch_wide(v, j):
        cols = pl.ds(pl.multiple_of((v * wide + j) * LANES, LANES), LANES)
        slot = lax.rem(v, 2)
        return pltpu.make_async_copy(
            et_ref.at[:, cols], rbuf.at[slot, j, pl.ds(0, dim)], fsem.at[slot, j])

    def parts(src, dst, sends, recvs, q, da, db):
        return (send(src.at[pl.ds(0, cut)], dst.at[0, pl.ds(0, cut)], sends.at[0], recvs.at[0],
                     shifted(q, da, db)),
                send(src.at[pl.ds(cut, rest)], dst.at[1, pl.ds(0, rest)], sends.at[1],
                     recvs.at[1], shifted(q, 3 * da, 3 * db)))

    def part_copies(q):
        return parts(tiles.at[q, 0], part_in.at[q], psend.at[q], precv.at[q], q, 1, 0)

    def bpart_copies(k):
        return parts(tiles.at[4 * k, 3], bpart_in.at[k], bpsend.at[k], bprecv.at[k], 4 * k, 0, 1)

    def tile_copies(q):
        return [send(tiles.at[q, 1 + w], tile_in.at[q, w], tsend.at[q, w], trecv.at[q, w],
                     shifted(q, WAYS[w], 0)) for w in PAIR]

    def btile_copies(k):
        return [send(tiles.at[4 * k + 1 + w, 3], btile_in.at[k, w], btsend.at[k, w],
                     btrecv.at[k, w], shifted(4 * k, 0, WAYS[w])) for w in PAIR]

    def add_parts(first, second, got):
        first[0:cut, :] += got[0, 0:cut, :]
        second[cut:dim, :] += got[1, 0:rest, :]

    def close_slab(q):
        arrive(tile_copies(q))
        tiles[q, 3] = tiles[q, 3] + (tile_in[q, 0] + tile_in[q, 1])

    def close_chunk(k):
        close_slab(4 * k + 3)
        arrive(btile_copies(k))
        shard[k] = tiles[4 * k + 3, 3] + (btile_in[k, 0] + btile_in[k, 1])

    def own_copy(k):
        return pltpu.make_async_copy(
            shard.at[k], ag_ref.at[k, me['z'], me['y'], me['x']], own_sem.at[k])

    def hops(k, letter):
        block = LETTERS.index(letter.lower())
        passed = int(letter.isupper())
        side = SIDES[min(k, 2)] * dim // 576 // SUB * SUB
        ranges = ((0, side), (side, dim - 2 * side), (dim - side, side))
        out = []
        for p, order in enumerate(GATHERS):
            phase = min(block, 2)
            axis = order[phase]
            if SIZES[axis] == 1 or (phase == 2 and block - 2 >= SIZES[order[1]]):
                continue
            for w in PAIR:
                at = dict(me)
                for done in order[:phase]:
                    at[done] = pl.ds(0, SIZES[done])
                if phase == 2:
                    at[order[1]] = lax.rem(me[order[1]] + block - 2, SIZES[order[1]])
                low, high = ranges[p]
                if passed:
                    at[axis] = lax.rem(me[axis] + RING - WAYS[w], RING)
                    mid = halved(high)
                    low, high = (low + mid, high - mid) if w else (low, mid)
                there = ag_ref.at[k, at['z'], at['y'], at['x'], pl.ds(low, high)]
                here = there if block + passed else shard.at[k, pl.ds(low, high)]
                sems = (k, p, block, passed, w)
                out.append(send(here, there, agsend.at[sems], agrecv.at[sems],
                                peer(**{axis: WAYS[w]})))
        return out

    def gather_step(k, n):
        if n == 0:
            close_chunk(k)
        waits, starts = STEPS[n].split(' ')
        for letter in waits:
            arrive(hops(k, letter))
        if n == 0:
            own_copy(k).start()
        if n == 2:
            own_copy(k).wait()
        for letter in starts:
            start(hops(k, letter))

    def ticks(u, low, high):
        def every_other(first, count):
            def run(act):
                if first < high and first + 2 * count > low + 1:
                    @pl.when((u >= first) & (u < first + 2 * count) & (lax.rem(u + first, 2) == 0))
                    def _():
                        act((u - first) // 2)
            return run

        for k in range(n_chunks):
            added = 8 * k + ADD_LAG[min(k, 2)]
            closed = added + TILE_LAG[min(k, 2)]

            @every_other(added, RING)
            def _(s, k=k):
                q = 4 * k + s
                arrive(part_copies(q))
                add_parts(tiles.at[q, 1], tiles.at[q, 2], part_in.at[q])
                start(tile_copies(q))

            @every_other(closed, RING - 1)
            def _(s, k=k):
                close_slab(4 * k + s)

                @pl.when(s == 0)
                def _():
                    start(bpart_copies(k))

            @every_other(closed + RING + LAST_LAG[min(k, 2)], 1)
            def _(s, k=k):
                arrive(bpart_copies(k))
                add_parts(tiles.at[4 * k + 1, 3], tiles.at[4 * k + 2, 3], bpart_in.at[k])
                start(btile_copies(k))

        for k in range(n_chunks):
            for n, late in enumerate(WHEN[min(k, 2)]):
                due = 8 * k + late
                if low <= due < high:
                    @pl.when(u == due)
                    def _(k=k, n=n):
                        gather_step(k, n)

    if deep > dim:
        zeros = jnp.zeros((deep - dim, LANES), BF16)
        for slot in PAIR:
            for j in PAIR:
                ebuf[slot, j, dim:, :] = zeros
            for j in range(wide):
                rbuf[slot, j, dim:, :] = zeros
    start([fetch(0, j) for j in PAIR])

    half = tokens // 2
    pieces = 2 * group_tokens // tokens
    ahead = pbuf.shape[0]
    whole, tail = divmod(dim, LANES)

    def bring(i, ref):
        slot = lax.rem(i, ahead)
        return pltpu.make_async_copy(ref, pbuf.at[slot], psem.at[slot])

    def bring_far(i):
        return bring(i, xg_ref.at[i // 2 - 1, lax.rem(i, 2)])

    def label_rows(r, cols):
        return (stat_ref[r, 0, 0:1, cols] + stat_ref[r, 1, 0:1, cols], stat_ref[r, 0, 2:3, cols])

    start([bring(i, own_ref.at[i]) for i in PAIR])
    start([bring_far(i) for i in range(2, min(ahead, pieces))])
    partners = [where for axis in AXES for where in others(axis)]
    call(partners)

    def piece(i, carry):
        bring(i, own_ref.at[0]).wait()
        v = pbuf[lax.rem(i, ahead)].astype(BF16)
        vt = v.T
        rows = pl.ds(pl.multiple_of(i * half, half), half)
        for k in range(whole):
            xb_ref[k, rows, :] = vt[:, lane_slice(k)]
        if tail:
            xb_ref[whole, rows, :] = jnp.concatenate(
                [vt[:, dim - tail:], jnp.zeros((half, LANES - tail), BF16)], axis=1)
        for k in range(half // LANES):
            xt_ref[i * (half // LANES) + k] = v[:, lane_slice(k)]

        @pl.when(i + ahead < pieces)
        def _():
            bring_far(i + ahead).start()

        row_sum, label = label_rows(
            i // 2, pl.ds(pl.multiple_of(lax.rem(i, 2) * half, half), half))
        scale = jnp.where(label >= 0.0, 1.0, 0.0) / row_sum
        for k in range(half // LANES):
            at = pl.ds(pl.multiple_of(i * half + k * LANES, LANES), LANES)
            scale_ref[at, :] = in_lanes(scale[:, lane_slice(k)]) * inv_count
            lab_ref[at, :] = in_lanes(label[:, lane_slice(k)]).astype(jnp.int32)
        return carry

    lax.fori_loop(0, pieces, piece, 0)
    meet(partners)
    row_sum, label = label_rows(0, slice(None))
    picked = (stat_ref[0, 0, 1:2, :] + stat_ref[0, 1, 1:2, :]) * SOFT_CAP
    loss_part = jnp.sum(jnp.where(label >= 0.0, jnp.log(row_sum) - picked, 0.0))

    def table_product(i, g_ref, half, store):
        n = tb // LANES
        x = jnp.concatenate([xt_ref[i * n + m] for m in range(n)], axis=1)
        g = jnp.concatenate([g_ref[0], g_ref[1]], axis=1)
        part = dot_f32(x, g, ((1,), (0,)))
        for j in PAIR:
            store(2 * half + j, part[:, lane_slice(j)])

    def close_unit(u):
        before = lax.rem(u + units, units)
        q = before // 2

        def add(t, part):
            tiles[q, t] += part

        table_product(blocks - 1, gb_ref, lax.rem(before, 2), add)

        @pl.when((u >= 0) & (lax.rem(before, 2) == 0))
        def _():
            start(part_copies(q))

        ticks(u, 0, units)

    def table_unit(u, carry):
        slot = lax.rem(u, 2)
        q = u // 2
        half = slot
        for j in PAIR:
            fetch(u, j).wait()

        @pl.when(u + 1 < units)
        def _():
            start([fetch(u + 1, j) for j in PAIR])

        bases = [tile_index(u, j) * LANES + vocab_off for j in PAIR]

        def grads(i, g_ref):
            rows = pl.ds(pl.multiple_of(i * tb, tb), tb)
            x = jnp.concatenate([xb_ref[n, rows, :] for n in range(slabs)], axis=1)
            e = jnp.concatenate([ebuf[slot, 0], ebuf[slot, 1]], axis=1)
            z = dot_f32(x, e, ((1,), (0,)))
            lab = lab_ref[rows, :]
            scale = scale_ref[rows, :]
            for j in PAIR:
                g_ref[j] = grad_tile(z[:, lane_slice(j)], scale, lab - bases[j], lane,
                                     inv_count)

        def product(i, g_ref, store):
            table_product(i, g_ref, half, store)

        def put(t, part):
            tiles[q, t] = part

        def add(t, part):
            tiles[q, t] += part

        grads(0, ga_ref)
        close_unit(u - 1)
        grads(1, gb_ref)
        product(0, ga_ref, put)

        def both(i, c):
            grads(2 * i, ga_ref)
            product(2 * i - 1, gb_ref, add)
            grads(2 * i + 1, gb_ref)
            product(2 * i, ga_ref, add)
            return c

        lax.fori_loop(1, blocks // 2, both, 0)
        return carry

    gb_ref[...] = jnp.zeros_like(gb_ref)
    tiles[RING * n_chunks - 1] = jnp.zeros_like(tiles[0])
    lax.fori_loop(0, units, table_unit, 0)
    close_unit(units - 1)

    row_lane = lax.broadcasted_iota(jnp.int32, (rb, LANES), 1)
    start([fetch_wide(0, j) for j in range(wide)])
    gx_ref[...] = jnp.zeros_like(gx_ref)

    def row_unit(v, carry):
        slot = lax.rem(v, 2)
        for j in range(wide):
            fetch_wide(v, j).wait()

        @pl.when(v + 1 < row_units)
        def _():
            start([fetch_wide(v + 1, j) for j in range(wide)])

        base = v * wide * LANES + vocab_off

        def grads(i, g_ref):
            rows = pl.ds(pl.multiple_of(i * rb, rb), rb)
            x = jnp.concatenate([xb_ref[n, rows, :] for n in range(slabs)], axis=1)
            e = jnp.concatenate([rbuf[slot, j] for j in range(wide)], axis=1)
            z = dot_f32(x, e, ((1,), (0,)))
            lab = lab_ref[rows, :] - base
            scale = scale_ref[rows, :]
            for j in range(wide):
                g_ref[:, lane_slice(j)] = grad_tile(
                    z[:, lane_slice(j)], scale, lab, row_lane + j * LANES, inv_count)

        def product(i, g_ref):
            rows = pl.ds(pl.multiple_of(i * rb, rb), rb)
            e = jnp.concatenate([rbuf[slot, j, 0:dim, :] for j in range(wide)], axis=1)
            gx_ref[:, rows] += dot_f32(e, g_ref[...], ((1,), (1,)))

        grads(0, gc_ref)
        grads(1, gd_ref)
        product(0, gc_ref)

        def both(i, c):
            grads(2 * i, gc_ref)
            product(2 * i - 1, gd_ref)
            grads(2 * i + 1, gd_ref)
            product(2 * i, gc_ref)
            return c

        lax.fori_loop(1, row_blocks // 2, both, 0)
        product(row_blocks - 1, gd_ref)
        ticks(v + units, units, units + row_units)
        return carry

    lax.fori_loop(0, row_units, row_unit, 0)

    def late_steps(steps):
        for n in steps:
            for k in range(n_chunks):
                if 8 * k + WHEN[min(k, 2)][n] >= units + row_units:
                    gather_step(k, n)

    final = len(STEPS) - 1
    if SIZES['core'] > 1:
        swap_rows = send(gx_ref, gin_ref, gsem.at[0], gsem.at[1], peer(core=1))
        swap_rows.start()
        late_steps(range(final))
        swap_rows.wait()
    else:
        late_steps(range(final))
        gin_ref[...] = jnp.zeros_like(gin_ref)
    dw_ref[...] = jnp.zeros_like(dw_ref)

    def norm_back(i, carry):
        cols = pl.ds(pl.multiple_of(i * rb, rb), rb)
        h = ht_ref[:, cols].astype(F32)
        inv_rms = lax.rsqrt(jnp.mean(h * h, axis=0, keepdims=True) + 1e-6)
        n = h * inv_rms
        g = gx_ref[:, cols] + gin_ref[:, cols]
        gn = g * n
        part = dw_ref[...]
        for j in range(rb // LANES):
            part = part + gn[:, lane_slice(j)]
        dw_ref[...] = part
        w1 = jnp.broadcast_to(w1_ref[:, :1], h.shape)
        inner = jnp.mean(gn * w1, axis=0, keepdims=True)
        dh_ref[:, cols] = ((g * w1 - n * inner) * inv_rms).astype(BF16)
        return carry

    lax.fori_loop(0, tokens // rb, norm_back, 0)
    cur_ref = swap[0]
    cur_ref[0] = jnp.zeros_like(cur_ref[0])
    cur_ref[0, 0:1, 0:dim] = jnp.sum(dw_ref[...].T, axis=0, keepdims=True)
    cur_ref[0, 1:2, 0:LANES] = loss_part * inv_count
    for k in range(len(CUBE)):
        start(swap_copies(AXES, k, *swap))
        swap_sum(AXES, k, *swap)
    sum_ref[...] = cur_ref[len(CUBE)]
    late_steps([final])

    def sent(q, carry):
        for copy in (*part_copies(q), *tile_copies(q)):
            copy.wait_send()
        return carry

    lax.fori_loop(0, 4 * n_chunks, sent, 0)

    for k in range(n_chunks):
        for copy in (*bpart_copies(k), *btile_copies(k)):
            copy.wait_send()
        for letter in LETTERS + LETTERS.upper():
            for copy in hops(k, letter):
                copy.wait_send()


def backward(count, stat, ht, w1, xt_own, xg, et, tb=1024, rb=512, wide=8):
    dim, tokens = ht.shape
    vocab = et.shape[1]
    slabs = -(-dim // LANES)
    group_tokens = SIZES['x'] * tokens
    cube = tuple(SIZES[axis] for axis in AXES[:3])
    n_chunks = vocab // (LANES * cube[0] * cube[1] * cube[2])
    tb, rb = min(tb, group_tokens // 4), min(rb, tokens // 2)
    part = dim - halved(dim)
    q = RING * n_chunks
    tile = (dim, LANES)
    held = (slabs * LANES, LANES)

    def vmem(dtype, *shape):
        return pltpu.VMEM(shape, dtype)

    return pl.pallas_call(
        lambda *refs: main_body(n_chunks, tb, rb, *refs),
        in_specs=[VMEM] * 4 + [HBM] * 3,
        out_specs=[HBM, VMEM, VMEM],
        out_shape=[f32(n_chunks, *cube, *tile), bf16(dim, tokens), f32(SUB, slabs * LANES)],
        scratch_shapes=[
            vmem(BF16, slabs, group_tokens, LANES), vmem(BF16, group_tokens // LANES, *tile),
            vmem(F32, group_tokens, LANES), vmem(jnp.int32, group_tokens, LANES),
            vmem(F32, RING, dim, tokens // 2),
            vmem(F32, dim, tokens), vmem(F32, dim, tokens), vmem(F32, *tile),
            vmem(BF16, 2, 2, *held), vmem(BF16, 2, wide, *held),
            *[vmem(BF16, 2, tb, LANES)] * 2, *[vmem(BF16, rb, wide * LANES)] * 2,
            vmem(F32, n_chunks, *tile), vmem(F32, q, RING, *tile),
            vmem(F32, q, 2, part, LANES), vmem(F32, q, 2, *tile),
            vmem(F32, n_chunks, 2, part, LANES), vmem(F32, n_chunks, 2, *tile),
            SEM((RING,)), SEM((2, 2)), SEM((2, wide)), SEM((2,)), SEM((n_chunks,)),
            *[SEM((q, 2))] * 4,
            *[SEM((n_chunks, 2))] * 4,
            *[SEM((n_chunks, len(GATHERS), len(LETTERS), 2, 2))] * 2,
            *swap_scratch(slabs * LANES),
        ],
        compiler_params=meeting(2),
        cost_estimate=cost(16 * ht.size * vocab, 4 * et.size),
        name="backward",
    )(count, stat, ht, w1, xt_own, xg, et)


def place_body(rows, deep, src_ref, out_ref, buf, in_sem, out_sem):
    n_chunks, n_dev, dim, _ = src_ref.shape
    per = dim // rows
    pieces = n_chunks * per

    def source(i):
        return src_ref.at[i // per, :, pl.ds(lax.rem(i, per) * rows, rows)]

    def read(i):
        slot = lax.rem(i, deep)
        return pltpu.make_async_copy(source(i), buf.at[slot], in_sem.at[slot])

    def written(i):
        slot = lax.rem(i, deep)
        return pltpu.make_async_copy(buf.at[slot], source(i), out_sem.at[slot])

    def piece(i, carry):
        @pl.when(i < pieces)
        def _():
            @pl.when(i >= deep)
            def _():
                written(i - deep).wait()

            read(i).start()

        j = i - deep // 2

        @pl.when(j >= 0)
        def _():
            read(j).wait()
            slot = lax.rem(j, deep)
            at = pl.ds(pl.multiple_of(lax.rem(j, per) * rows, rows), rows)
            for k in range(n_dev):
                cols = pl.ds(pl.multiple_of(((j // per) * n_dev + k) * LANES, LANES), LANES)
                pltpu.make_async_copy(buf.at[slot, k], out_ref.at[at, cols],
                                      out_sem.at[slot]).start()
        return carry

    lax.fori_loop(0, pieces + deep // 2, piece, 0)
    lax.fori_loop(max(pieces - deep, 0), pieces, lambda i, c: (written(i).wait(), c)[1], 0)


def place(gathered, rows=48, deep=12):
    n_chunks, n_dev, dim, _ = gathered.shape
    return pl.pallas_call(
        lambda *refs: place_body(rows, deep, *refs),
        in_specs=[HBM],
        out_specs=HBM,
        out_shape=f32(dim, n_chunks * n_dev * LANES),
        scratch_shapes=[pltpu.VMEM((deep, n_dev, rows, LANES), F32), SEM((deep,)), SEM((deep,))],
        compiler_params=params(),
        cost_estimate=cost(gathered.size, 8 * gathered.size),
        name="place",
    )(gathered)


def solution(mesh):
    grid_mesh = Mesh(mesh.devices.reshape(RING, RING, RING, 2), AXES)
    dp = AXES[:3]

    def local_step(hidden, norm_w, embed_table, labels, loss_mask):
        batch_rows, seq_len, dim = hidden.shape
        vocab = embed_table.shape[0]
        tokens = batch_rows * seq_len
        et = embed_table.T
        ht = hidden.reshape(tokens, dim).T
        w1 = jnp.broadcast_to((1.0 + norm_w.astype(F32))[:, None], (dim, LANES))
        mask_row = loss_mask.reshape(1, tokens)
        lab_row = labels.reshape(1, tokens)
        xt_own, xb_own = norm_rows(ht, w1)
        xg, stat, count = forward(xb_own, lab_row, mask_row, et, xt_own)
        gathered, dht, sums = backward(count, stat, ht, w1, xt_own, xg, et)
        table = place(gathered.reshape(-1, RING ** 3, dim, LANES))
        return (sums[1, 0], dht.T.reshape(batch_rows, seq_len, dim),
                sums[0, :dim], table.T)

    return jax.shard_map(
        local_step, mesh=grid_mesh,
        in_specs=(P(dp, None, None), P(None), P('core', None), P(dp, None), P(dp, None)),
        out_specs=(P(), P(dp, None, None), P(None), P('core', None)), check_vma=False)
```
